32 devices in a mesh: groups: 2 (over x), seq: 8 (over z, y), section: 2 (over core).
Axes of the slice: x: 2, y: 2, z: 4, core: 2. Of those that a mesh axis runs over, the one named last changes fastest.
Arguments:
- latent_cache: bfloat16 [2, 8, 32768, 576], P('section', 'groups', 'seq'), parts along dimension 1, may hold values from -6 to 6
- index_keys: bfloat16 [2, 8, 32768, 128], P('section', 'groups', 'seq'), parts along dimension 1, may hold values from -6 to 6
- latent_query: bfloat16 [2, 8, 128, 576], P('section', 'groups', 'seq'), parts along dimension 1, may hold values from -54 to 54
- index_query: bfloat16 [2, 8, 64, 128], P('section', 'groups', 'seq'), parts along dimension 1, may hold values from -6 to 6
- index_weight: bfloat16 [2, 8, 64], P('section', 'groups', 'seq'), parts along dimension 1, may hold values from -0.75 to 0.75
- value_up_weight: bfloat16 [2, 128, 512, 128], P('section', 'seq'), may hold values from -0.25 to 0.25
- selected: int32 [2, 8, 2, 32], P('section', 'groups'), parts along dimension 1, may hold values from 0 to 511, as said below
- lengths: int32 [8], P('groups'), parts along dimension 0, may hold values from 16384 to 32767, as said below
Outputs:
- index_scores: float32 [2, 8, 32768], P('section', 'groups', 'seq'), parts along dimension 1
- head_out: bfloat16 [2, 8, 128, 128], P('section', 'groups', 'seq'), parts along dimension 1
The draws below stay inside these ranges and needn't reach their ends.
There are 2 independent parts, one for each index of `groups`. The reference program is written for one: setup_inputs(seed, part) draws one part's arguments, and reference() takes and returns one part's arrays. A program takes and returns all parts, laid end to end along the dimension named above; an argument that names none is the same for every part. Nothing has to cross between parts.
Inputs may be any that keep to these rules, and one draw needn't show every extreme that they name: `lengths`: never one more than a multiple of 64. `selected`: for each layer, row and head group, 32 distinct block numbers, each block starting before the row's length; the block holding the row's last live token is always among them.
All inputs are finite; a program needn't handle non-finite values.
Results may differ from the reference program's by a relative error of at most 0.0048.
Values may be sent and summed in bfloat16 or wider, within the bound.
A program may use at most 128 MiB of HBM per device.

```python
import jax
import jax.numpy as jnp
from jax import lax

ATTENTION_HEADS = 128
LATENT_WIDTH = 512
ROTARY_WIDTH = 64
VALUE_WIDTH = 128
IDX_HEADS = 64
IDX_DIM = 128
BLOCK = 64
HEAD_GROUPS = 2
DECODE_ROWS = 4
CTX_DEV = 4096
CONTEXT_POSITIONS = 32768
LAYER_COUNT = 2
NSEL = 32


def base_lengths(key):
    drawn = jax.random.randint(jax.random.fold_in(key, 11), (DECODE_ROWS,), CONTEXT_POSITIONS // 2, CONTEXT_POSITIONS)
    drawn = jnp.where(drawn % BLOCK == 1, drawn + 1, drawn)
    longest = jax.random.randint(jax.random.fold_in(key, 13), (), 0, DECODE_ROWS)
    row_ids = jnp.arange(DECODE_ROWS, dtype=jnp.int32)
    return jnp.where(row_ids == longest, CONTEXT_POSITIONS - 1, drawn).astype(jnp.int32)


def draw_lengths(key, part):
    return base_lengths(key)


def draw_selected(key, part):
    row_lengths = base_lengths(key)
    count = CONTEXT_POSITIONS // BLOCK
    blocks = jnp.arange(count, dtype=jnp.int32)
    last_block = (row_lengths - 1) // BLOCK
    raw = jax.random.randint(jax.random.fold_in(key, 12), (LAYER_COUNT, DECODE_ROWS, HEAD_GROUPS, count), 0, 2 ** 17)
    ranked = raw * 4096 + blocks
    ranked = jnp.where(blocks[None, None, None, :] <= last_block[None, :, None, None], ranked, -1)
    ranked = jnp.where(blocks[None, None, None, :] == last_block[None, :, None, None], 2 ** 30, ranked)
    return lax.top_k(ranked, NSEL)[1].astype(jnp.int32)


def leading_keys(key):
    width = LATENT_WIDTH + ROTARY_WIDTH
    signs = jax.random.bernoulli(jax.random.fold_in(key, 23), 0.5, (LAYER_COUNT, DECODE_ROWS, width))
    return jnp.where(signs, jnp.float32(1.5), jnp.float32(-1.5))


def latent_values(key):
    width = LATENT_WIDTH + ROTARY_WIDTH
    array_shape = (LAYER_COUNT, DECODE_ROWS, CONTEXT_POSITIONS, width)
    values = jnp.clip(jax.random.normal(jax.random.fold_in(key, 21), array_shape, jnp.float32), -6.0, 6.0)
    row_lengths = base_lengths(key)
    row_ids = jnp.arange(DECODE_ROWS)
    leading = leading_keys(key)
    spread = 0.015 * width ** 0.5
    random_noise = jax.random.normal(jax.random.fold_in(key, 22), (LAYER_COUNT, DECODE_ROWS, width), jnp.float32)
    values = values.at[:, row_ids, row_lengths - 1].set(leading)
    values = values.at[:, row_ids, row_lengths - 2].set(jnp.clip(leading + spread * random_noise, -6.0, 6.0))
    return values


def draw_latent_cache(key, part):
    return latent_values(key).astype(jnp.bfloat16)


def draw_latent_query(key, part):
    width = LATENT_WIDTH + ROTARY_WIDTH
    array_shape = (LAYER_COUNT, DECODE_ROWS, ATTENTION_HEADS, width)
    values = 1.5 * jnp.clip(jax.random.normal(jax.random.fold_in(key, 31), array_shape, jnp.float32), -6.0, 6.0)
    leading = leading_keys(key)
    head_ids = jnp.arange(ATTENTION_HEADS)
    target = jnp.array([120.0, 180.0, 260.0, 340.0], jnp.float32)[head_ids // 8 % 4]
    factor = target / (2.25 * width * (VALUE_WIDTH + ROTARY_WIDTH) ** (-0.5))
    planted = factor[None, None, :, None] * leading[:, :, None, :]
    aligned = (head_ids % 8 == 0)[None, None, :, None]
    values = jnp.where(aligned, planted, values)
    return values.astype(jnp.bfloat16)


def level_of(stream_key, extent, cuts, low, top_value):
    level = 1.0
    for position, parts in cuts:
        heights = jax.random.uniform(jax.random.fold_in(jax.random.fold_in(stream_key, 6), position), (parts,), jnp.float32, low / len(cuts), top_value / len(cuts))
        level = level * jnp.repeat(jnp.exp(heights), extent[position] // parts).reshape((-1,) + (1,) * (len(extent) - 1 - position))
    return level


def normal_values(key, shape, scale, reach, split=(), held_as=jnp.bfloat16):
    values = scale * jax.random.normal(key, shape, jnp.float32)
    if split:
        values = values * level_of(key, shape, split, -0.22, 0.18)
    return jnp.clip(values, -reach, reach).astype(held_as)


def setup_inputs(seed: int = 0, part: int = 0) -> dict:
    splits = jax.random.split(jax.random.key(seed), 9)
    part_keys = jax.random.split(jax.random.fold_in(splits[8], part), 9)
    return {
        "latent_cache": draw_latent_cache(jax.random.fold_in(jax.random.fold_in(splits[8], part), 71), part),
        "index_keys": normal_values(part_keys[1], (LAYER_COUNT, DECODE_ROWS, CONTEXT_POSITIONS, IDX_DIM), 1.0, 6.0, ((0, 2), (2, 8))),
        "latent_query": draw_latent_query(jax.random.fold_in(jax.random.fold_in(splits[8], part), 71), part),
        "index_query": normal_values(part_keys[3], (LAYER_COUNT, DECODE_ROWS, IDX_HEADS, IDX_DIM), 1.0, 6.0, ((0, 2), (2, 8))),
        "index_weight": normal_values(part_keys[4], (LAYER_COUNT, DECODE_ROWS, IDX_HEADS), 0.125, 0.75, ((0, 2), (2, 8))),
        "value_up_weight": normal_values(splits[5], (LAYER_COUNT, ATTENTION_HEADS, LATENT_WIDTH, VALUE_WIDTH), LATENT_WIDTH ** -0.5, 0.25, ((0, 2), (1, 8))),
        "selected": draw_selected(jax.random.fold_in(jax.random.fold_in(splits[8], part), 71), part),
        "lengths": draw_lengths(jax.random.fold_in(jax.random.fold_in(splits[8], part), 71), part),
    }


def reference(latent_cache, index_keys, latent_query, index_query, index_weight, value_up_weight, selected, lengths):
    scale = (VALUE_WIDTH + ROTARY_WIDTH) ** -0.5
    positions = jnp.arange(CONTEXT_POSITIONS, dtype=jnp.int32)
    live_mask = positions[None, :] < lengths[:, None]
    group_wise = ATTENTION_HEADS // HEAD_GROUPS
    spans = CONTEXT_POSITIONS // CTX_DEV
    score_list = []
    head_list = []
    for layer_index in range(LAYER_COUNT):
        index_dots = jnp.einsum("bhd,btd->bht", index_query[layer_index].astype(jnp.float32), index_keys[layer_index].astype(jnp.float32))
        weighted = jax.nn.relu(index_dots * IDX_DIM ** -0.5) * index_weight[layer_index].astype(jnp.float32)[:, :, None]
        score_list.append(jnp.where(live_mask, jnp.sum(weighted, axis=1), jnp.float32(0.0)))

        def one_row(packed):
            latent_rows, query_matrix, chosen, row_length = packed
            tokens = (chosen[:, :, None] * BLOCK + jnp.arange(BLOCK, dtype=jnp.int32)[None, None, :]).reshape(HEAD_GROUPS, NSEL * BLOCK).astype(jnp.int32)
            picked_blocks = latent_rows[tokens].astype(jnp.float32)
            group_split = query_matrix.reshape(HEAD_GROUPS, group_wise, LATENT_WIDTH + ROTARY_WIDTH).astype(jnp.float32)
            scores = jnp.einsum("ghd,gkd->ghk", group_split, picked_blocks) * scale
            usable = (tokens < row_length)[:, None, :]
            masked = jnp.where(usable, scores, jnp.float32(-1e30))
            shard = (tokens // CTX_DEV).astype(jnp.int32)
            onehot = shard[:, None, :, None] == jnp.arange(spans, dtype=jnp.int32)[None, None, None, :]
            shard_max = jnp.max(jnp.where(onehot, masked[..., None], jnp.float32(-1e30)), axis=2)
            local_max = jnp.take_along_axis(shard_max, jnp.broadcast_to(shard[:, None, :], masked.shape).astype(jnp.int32), axis=2)
            row_max = jnp.max(shard_max, axis=2, keepdims=True)
            local_weights = jnp.where(usable, jnp.exp(masked - local_max), jnp.float32(0.0))
            factor = jnp.where(usable, jnp.exp(local_max - row_max), jnp.float32(0.0))
            total_per_row = jnp.sum(local_weights * factor, axis=2)
            rounded_values = local_weights.astype(jnp.bfloat16).astype(jnp.float32) * factor
            summed_values = jnp.einsum("qyj,qjp->qyp", rounded_values, picked_blocks[:, :, :LATENT_WIDTH])
            return (summed_values / total_per_row[:, :, None]).astype(jnp.bfloat16).reshape(ATTENTION_HEADS, LATENT_WIDTH)

        attended = lax.map(one_row, (latent_cache[layer_index], latent_query[layer_index], selected[layer_index], lengths))
        projected = jnp.einsum("bhc,hcv->bhv", attended.astype(jnp.float32), value_up_weight[layer_index].astype(jnp.float32))
        head_list.append(projected.astype(jnp.bfloat16))
    return jnp.stack(score_list), jnp.stack(head_list)
```

```python
import functools

import jax
import jax.numpy as jnp
from jax import lax
from jax.experimental import pallas as pl
from jax.experimental.pallas import tpu as pltpu
from jax.sharding import PartitionSpec as P

LATENT_WIDTH = 512
ROTARY_WIDTH = 64
VALUE_WIDTH = 128
IDX_DIM = 128
BLOCK = 64
HEAD_GROUPS = 2
NEG = -1e30
LOG2E = 1.4426950408889634
FIRST = 8
MORE = 4
LANES = 128
PACKED = LATENT_WIDTH + LANES
MIB = 1024 * 1024
MESH = pl.DeviceIdType.MESH


class Line:
    def __init__(self, n):
        self.half = n // 2
        self.me = lax.axis_index("seq")
        self.z = lax.div(self.me, 2)
        self.y = lax.rem(self.me, 2)
        self.partner = self.me + 1 - 2 * self.y
        self.order = sorted(range(1, self.half), key=lambda k: (-k.bit_length(), k))

    def step(self, k, sign):
        if self.half & (self.half - 1):
            return lax.rem(self.z + sign * k + self.half, self.half)
        out = self.z
        for j in range(k.bit_length()):
            if k >> j & 1:
                bit = lax.rem(lax.div(self.z, 1 << j), 2)
                out = out + (1 - 2 * bit) * (1 << j)
        return out

    def to(self, k):
        return self.step(k, 1)

    def frm(self, k):
        return self.step(k, -1)

    def device(self, z):
        return 2 * z + self.y

    def greet(self):
        barrier = pltpu.get_barrier_semaphore()
        peers = [self.partner] + [self.device(self.to(k)) for k in self.order]
        for peer in peers:
            pl.semaphore_signal(
                barrier, inc=1, device_id={"seq": peer}, device_id_type=MESH
            )
        return lambda: pl.semaphore_wait(barrier, self.half)


def push(peer, src, dst, send_sem, recv_sem):
    return pltpu.make_async_remote_copy(
        src_ref=src,
        dst_ref=dst,
        send_sem=send_sem,
        recv_sem=recv_sem,
        device_id={"seq": peer},
        device_id_type=MESH,
    )


def gather_kernel(
    n, lq, iq, iw, sel, keys, weight, gq, giw, kbuf, wbuf, table,
    lqs, iqs, sels, load_sem, zsend, zrecv, ysend, yrecv,
):
    line = Line(n)
    me = line.me
    rows, heads, width = lqs.shape
    held = iw.shape[1]
    entered = line.greet()
    loads = [
        pltpu.make_async_copy(lq, lqs, load_sem.at[0]),
        pltpu.make_async_copy(iq, iqs, load_sem.at[1]),
        pltpu.make_async_copy(iw, giw.at[me], load_sem.at[2]),
        pltpu.make_async_copy(sel, sels, load_sem.at[3]),
        pltpu.make_async_copy(keys, kbuf, load_sem.at[4]),
        pltpu.make_async_copy(weight, wbuf, load_sem.at[5]),
    ]
    for copy in loads:
        copy.start()
    for copy in loads[:3]:
        copy.wait()

    lane = lax.broadcasted_iota(jnp.int32, (iqs.shape[1], LANES), 1)
    row = lax.broadcasted_iota(jnp.int32, (iqs.shape[1], LANES), 0)
    for b in range(rows):
        mine = iqs[b].astype(jnp.float32)
        turned = pltpu.roll(mine, LANES // 2, 1)
        if heads == 2 * iqs.shape[1]:
            spare = jnp.concatenate([turned, mine], axis=0)
        else:
            spare = jnp.where(row < held, turned, pltpu.roll(mine, held, 0))
        gq[me, b, :, 0:LATENT_WIDTH] = lqs[b, :, 0:LATENT_WIDTH]
        gq[me, b, :, LATENT_WIDTH:width] = lqs[b, :, LATENT_WIDTH:width]
        spare = spare.astype(jnp.bfloat16)
        gq[me, b, :, width:PACKED] = spare[:, width - LATENT_WIDTH :]
    entered()

    def pieces(owner):
        return [gq.at[owner, b] for b in range(rows)] + [giw.at[owner]]

    across, along, onward = [], {}, {}
    for r, ref in enumerate(pieces(me)):
        across.append(push(line.partner, ref, ref, ysend.at[0, r], yrecv.at[0, r]))
        for k in line.order:
            along[k, r] = push(
                line.device(line.to(k)), ref, ref, zsend.at[k, r], zrecv.at[k, r]
            )
    for k in line.order:
        for r, ref in enumerate(pieces(line.device(line.frm(k)))):
            onward[k, r] = push(line.partner, ref, ref, ysend.at[k, r], yrecv.at[k, r])
    for r in range(rows, -1, -1):
        for k in line.order:
            along[k, r].start()
        across[r].start()

    loads[3].wait()
    here = keys.shape[1] // BLOCK
    first = me * here
    chosen = sels[...]
    spots = lax.broadcasted_iota(jnp.int32, table.shape, 2)
    kept = jnp.full(table.shape, -1, jnp.int32)
    count = jnp.zeros(table.shape, jnp.int32)
    for i in range(sels.shape[2]):
        block = jnp.broadcast_to(chosen[:, :, i : i + 1], table.shape)
        mine = (block >= first) & (block < first + here)
        kept = jnp.where(mine & (spots == count), block, kept)
        count = count + jnp.where(mine, 1, 0)
    table[...] = jnp.where(spots == LANES - 1, count, kept)

    for r in range(rows, -1, -1):
        for k in line.order:
            along[k, r].wait_recv()
            onward[k, r].start()
    loads[4].wait()
    loads[5].wait()
    for r in range(rows, -1, -1):
        across[r].wait_recv()
        for k in line.order:
            onward[k, r].wait_recv()
    for r in range(rows, -1, -1):
        across[r].wait_send()
        for k in line.order:
            along[k, r].wait_send()
            onward[k, r].wait_send()


def local_kernel(table, lens, gq, cache, own, sent, own_lse, sent_lse, buf, sems):
    me = lax.axis_index("seq")
    side = lax.rem(me, 2)
    rows, width, span = cache.shape
    here = span // BLOCK
    first = me * here
    pairs = rows * HEAD_GROUPS

    def count_of(b, g):
        return table[b, g, LANES - 1]

    def block_copy(b, g, block, slot):
        rg = b * HEAD_GROUPS + g
        start = pl.multiple_of((block - first) // 2 * LANES, LANES)
        dest = pl.multiple_of(slot * LANES, LANES)
        return pltpu.make_async_copy(
            cache.at[b, :, pl.ds(start, LANES)],
            buf.at[rg, :, pl.ds(dest, LANES)],
            sems.at[rg, slot],
        )

    @pl.loop(0, pairs)
    def _(rg):
        b, g = rg // HEAD_GROUPS, rg % HEAD_GROUPS

        @pl.loop(0, count_of(b, g))
        def _(slot):
            block_copy(b, g, table[b, g, slot], slot).start()

    @pl.loop(0, pairs)
    def _(rg):
        count = count_of(rg // HEAD_GROUPS, rg % HEAD_GROUPS)
        extra = jnp.maximum(count - FIRST, 0)
        room = FIRST + (extra + MORE - 1) // MORE * MORE

        @pl.loop(count, room)
        def _(slot):
            dest = pl.multiple_of(slot * LANES, LANES)
            buf[rg, :, pl.ds(dest, LANES)] = jnp.zeros((width, LANES), jnp.bfloat16)

    heads = gq.shape[2]
    per_group = gq.shape[0] // HEAD_GROUPS
    wide = per_group * heads
    scale = (VALUE_WIDTH + ROTARY_WIDTH) ** (-0.5) * LOG2E
    lane = lax.broadcasted_iota(jnp.int32, (1, LANES), 1)
    spot = lax.broadcasted_iota(jnp.int32, (per_group // 2, heads, LANES), 2)

    def scores(b, g, query, base, slots):
        rg = b * HEAD_GROUPS + g
        count = count_of(b, g)
        bias = []
        for j in range(slots):
            slot = base + j
            block = table[b, g, slot]
            begin = block % 2 * BLOCK
            live = jnp.minimum(BLOCK, lens[b] - block * BLOCK)
            end = jnp.where(slot < count, begin + live, 0)
            bias.append(jnp.where((lane >= begin) & (lane < end), 0.0, NEG))
        bias = jnp.concatenate(bias, axis=1)
        start = base * LANES
        if not isinstance(start, int):
            start = pl.multiple_of(start, MORE * LANES)
        window = pl.ds(start, slots * LANES)
        s = jnp.dot(query, buf[rg, :, window], preferred_element_type=jnp.float32)
        return s * scale + bias, window

    def mix(b, g, p, window):
        return lax.dot_general(
            p.astype(jnp.bfloat16),
            buf[b * HEAD_GROUPS + g, :LATENT_WIDTH, window],
            (((1,), (1,)), ((), ())),
            preferred_element_type=jnp.float32,
        )

    @pl.loop(0, rows)
    def _(b):
        for g in range(HEAD_GROUPS):

            @pl.loop(0, count_of(b, g))
            def _(slot, g=g):
                block_copy(b, g, first, slot).wait()

        queries, state = [], []
        for g in range(HEAD_GROUPS):
            query = gq[pl.ds(g * per_group, per_group), b]
            if heads % 16:
                query = query.astype(jnp.float32)
            query = query.reshape(wide, PACKED)[:, :width].astype(jnp.bfloat16)
            queries.append(query)
        firsts = [scores(b, g, queries[g], 0, FIRST) for g in range(HEAD_GROUPS)]
        for g, (s, window) in enumerate(firsts):
            top = jnp.max(s, axis=1, keepdims=True)
            p = jnp.exp2(s - top)
            state.append((top, jnp.sum(p, axis=1, keepdims=True), mix(b, g, p, window)))

        for g in range(HEAD_GROUPS):

            def more(c, carry, g=g):
                top, total, acc = carry
                s, window = scores(b, g, queries[g], FIRST + c * MORE, MORE)
                new = jnp.maximum(top, jnp.max(s, axis=1, keepdims=True))
                p = jnp.exp2(s - new)
                keep = jnp.exp2(top - new)
                total = total * keep + jnp.sum(p, axis=1, keepdims=True)
                return new, total, acc * keep + mix(b, g, p, window)

            extra = jnp.maximum(count_of(b, g) - FIRST, 0)
            top, total, acc = lax.fori_loop(0, (extra + MORE - 1) // MORE, more, state[g])
            acc = (acc / total).reshape(per_group, heads, LATENT_WIDTH)
            lse = jnp.broadcast_to(top + jnp.log2(total), (wide, LANES))
            lse = lse.reshape(per_group, heads, LANES)
            acc = acc.reshape(per_group // 2, 2, heads, LATENT_WIDTH)
            lse = lse.reshape(per_group // 2, 2, heads, LANES)
            here_z = pl.ds(g * per_group // 2, per_group // 2)
            even = side == 0
            own[here_z, b] = jnp.where(even, acc[:, 0], acc[:, 1])
            sent[here_z, b] = jnp.where(even, acc[:, 1], acc[:, 0]).astype(jnp.bfloat16)
            own_lse[here_z] = jnp.where(
                spot == b, jnp.where(even, lse[:, 0], lse[:, 1]), own_lse[here_z]
            )
            sent_lse[here_z] = jnp.where(
                spot == b, jnp.where(even, lse[:, 1], lse[:, 0]), sent_lse[here_z]
            )


def exchange_kernel(
    n, lens, own, sent, own_lse, sent_lse, gq, giw, kbuf, attended, scores,
    kept, from_pair, pair_lse, joint, joint_lse, from_line, line_lse,
    ysend, yrecv, zsend, zrecv,
):
    line = Line(n)
    half, me = line.half, line.me
    _, rows, heads, latent = own.shape
    entered = line.greet()
    entered()

    ring = line.order + [0]
    across, along = {}, {}
    for k in ring:
        z = line.to(k)
        refs = [(sent_lse.at[z], pair_lse.at[z])]
        refs += [(sent.at[z, b], from_pair.at[z, b]) for b in range(rows)]
        for r, (src, dst) in enumerate(refs):
            across[k, r] = push(line.partner, src, dst, ysend.at[k, r], yrecv.at[k, r])
            across[k, r].start()

    span = kbuf.shape[1]
    tile = min(512, span)
    lane = lax.broadcasted_iota(jnp.int32, (1, tile), 1)
    held = giw.shape[2]
    group = 8
    diagonal = (
        lax.broadcasted_iota(jnp.int32, (n * group, held), 0) % group
        == lax.broadcasted_iota(jnp.int32, (n * group, held), 1)
    )
    low = lax.broadcasted_iota(jnp.int32, (n * group, LANES), 1) < LANES // 2

    def index_row(b):
        packed = gq[:, b, :, LATENT_WIDTH:PACKED].astype(jnp.float32)
        if heads == 2 * group:
            left = packed[:, :group].reshape(n * group, LANES)
            right = packed[:, group:].reshape(n * group, LANES)
        else:
            left = packed.reshape(n * group, LANES)
            right = pltpu.roll(left, n * group - held, 0)
        query = jnp.where(low, pltpu.roll(left, LANES // 2, 1), right)
        query = query.astype(jnp.bfloat16)
        weight = giw[:, b : b + 1].astype(jnp.float32)
        weight = jnp.broadcast_to(weight, (n, group, held)).reshape(n * group, held)
        weight = jnp.sum(jnp.where(diagonal, weight, 0.0), axis=1, keepdims=True)
        weight = jnp.broadcast_to(weight * IDX_DIM ** (-0.5), (n * group, LANES))
        length = lens[b]

        def step(c, carry):
            start = pl.multiple_of(c * tile, tile)
            dots = lax.dot_general(
                query,
                kbuf[b, pl.ds(start, tile), :],
                (((1,), (1,)), ((), ())),
                preferred_element_type=jnp.float32,
            )
            pieces = []
            for j in range(tile // LANES):
                part = jnp.maximum(dots[:, j * LANES : (j + 1) * LANES], 0.0) * weight
                pieces.append(jnp.sum(part, axis=0, keepdims=True))
            total = jnp.concatenate(pieces, axis=1)
            live = me * span + c * tile + lane < length
            scores[b : b + 1, pl.ds(start, tile)] = jnp.where(live, total, 0.0)
            return carry

        lax.fori_loop(0, span // tile, step, 0)

    def weigh(parts):
        best = functools.reduce(jnp.maximum, parts)
        grown = [jnp.exp2(part - best) for part in parts]
        whole = functools.reduce(jnp.add, grown)
        return [part / whole for part in grown], best + jnp.log2(whole)

    early = rows // 2
    for b in range(early):
        index_row(b)

    for k in ring:
        z = line.to(k)
        across[k, 0].wait_recv()
        (mine, theirs), lse = weigh([own_lse[z], pair_lse[z]])
        if k:
            joint_lse[z] = lse
            target = line.device(z)
            along[k, 0] = push(
                target, joint_lse.at[z], line_lse.at[line.z], zsend.at[k, 0], zrecv.at[k, 0]
            )
        else:
            line_lse[z] = lse
        for b in range(rows):
            across[k, b + 1].wait_recv()
            value = mine[:, b : b + 1] * own[z, b]
            value += theirs[:, b : b + 1] * from_pair[z, b].astype(jnp.float32)
            if k:
                joint[z, b] = value.astype(jnp.bfloat16)
                along[k, b + 1] = push(
                    target, joint.at[z, b], from_line.at[line.z, b],
                    zsend.at[k, b + 1], zrecv.at[k, b + 1],
                )
            else:
                kept[b] = value
        if k:
            for r in range(rows + 1):
                along[k, r].start()

    for b in range(early, rows):
        index_row(b)

    for k in line.order:
        along[k, 0].wait_recv()
    spans = [line.z] + [line.frm(k) for k in line.order]
    factors, _ = weigh([line_lse[z] for z in spans])
    for b in range(rows):
        for k in line.order:
            along[k, b + 1].wait_recv()
        value = factors[0][:, b : b + 1] * kept[b]
        for z, factor in zip(spans[1:], factors[1:]):
            value += factor[:, b : b + 1] * from_line[z, b].astype(jnp.float32)
        attended[b] = value.astype(attended.dtype)
    for copy in list(across.values()) + list(along.values()):
        copy.wait_send()


def project_kernel(attended, weight, scores, out, scores_out, sem):
    copy = pltpu.make_async_copy(scores, scores_out, sem.at[0])
    copy.start()
    rows, heads, latent = attended.shape
    flat = attended[...]
    if heads % 16:
        flat = flat.astype(jnp.float32)
    flat = flat.reshape(rows * heads, latent).astype(jnp.bfloat16)
    which = lax.broadcasted_iota(jnp.int32, (rows * heads, 1), 0) % heads
    y = jnp.zeros((rows * heads, weight.shape[2]), jnp.float32)
    for h in range(heads):
        part = jnp.dot(flat, weight[h], preferred_element_type=jnp.float32)
        y = jnp.where(which == h, part, y)
    out[...] = y.reshape(rows, heads, weight.shape[2]).astype(out.dtype)
    copy.wait()


def on_device(
    n,
    latent_cache,
    index_keys,
    latent_query,
    index_query,
    index_weight,
    value_up_weight,
    selected,
    lengths,
):
    cache, keys, lq = latent_cache[0], index_keys[0], latent_query[0]
    iq, iw, weight, sel = index_query[0], index_weight[0], value_up_weight[0], selected[0]
    rows, span, width = cache.shape
    heads = lq.shape[1]
    half = n // 2
    extra = -iq.shape[1] % 8
    if extra:
        iq = jnp.pad(iq, ((0, 0), (0, extra), (0, 0)))
    vmem = pl.BlockSpec(memory_space=pltpu.VMEM)
    smem = pl.BlockSpec(memory_space=pltpu.SMEM)
    hbm = pl.BlockSpec(memory_space=pl.ANY)
    dma = pltpu.SemaphoreType.DMA

    def far(x):
        return pltpu.with_memory_space_constraint(x, pltpu.HBM)

    def near(x):
        return pltpu.with_memory_space_constraint(x, pltpu.VMEM)

    gq, giw, kbuf, wbuf, table = pl.pallas_call(
        functools.partial(gather_kernel, n),
        out_shape=(
            pltpu.VMEM((n, rows, heads, PACKED), lq.dtype),
            pltpu.VMEM((n,) + iw.shape, iw.dtype),
            pltpu.VMEM(keys.shape, keys.dtype),
            pltpu.VMEM(weight.shape, weight.dtype),
            pltpu.VMEM((rows, HEAD_GROUPS, LANES), jnp.int32),
        ),
        in_specs=[hbm] * 6,
        out_specs=(vmem,) * 5,
        scratch_shapes=[
            pltpu.VMEM(lq.shape, lq.dtype),
            pltpu.VMEM(iq.shape, iq.dtype),
            pltpu.VMEM(sel.shape, sel.dtype),
            dma((6,)),
            dma((half, rows + 1)), dma((half, rows + 1)),
            dma((half, rows + 1)), dma((half, rows + 1)),
        ],
        compiler_params=pltpu.CompilerParams(
            collective_id=0, has_side_effects=True, vmem_limit_bytes=16 * MIB
        ),
        name="gather",
    )(far(lq), far(iq), far(iw), far(sel), far(keys), far(weight))

    pairs = rows * HEAD_GROUPS
    nsel = sel.shape[2]
    room = FIRST + -(-max(nsel - FIRST, 0) // MORE) * MORE
    own, sent, own_lse, sent_lse = pl.pallas_call(
        local_kernel,
        out_shape=(
            pltpu.VMEM((half, rows, heads, LATENT_WIDTH), jnp.float32),
            pltpu.VMEM((half, rows, heads, LATENT_WIDTH), jnp.bfloat16),
            pltpu.VMEM((half, heads, LANES), jnp.float32),
            pltpu.VMEM((half, heads, LANES), jnp.float32),
        ),
        in_specs=[smem, smem, vmem, hbm],
        out_specs=(vmem,) * 4,
        scratch_shapes=[
            pltpu.VMEM((pairs, width, room * LANES), cache.dtype),
            dma((pairs, nsel)),
        ],
        compiler_params=pltpu.CompilerParams(vmem_limit_bytes=44 * MIB),
        name="local",
    )(table, lengths, near(gq), far(jnp.swapaxes(cache, 1, 2)))

    steps = (half, rows + 1)
    attended, scores = pl.pallas_call(
        functools.partial(exchange_kernel, n),
        out_shape=(
            pltpu.VMEM((rows, heads, LATENT_WIDTH), jnp.bfloat16),
            pltpu.VMEM((rows, span), jnp.float32),
        ),
        in_specs=[smem] + [vmem] * 7,
        out_specs=(vmem, vmem),
        scratch_shapes=[
            pltpu.VMEM((rows, heads, LATENT_WIDTH), jnp.float32),
            pltpu.VMEM(sent.shape, sent.dtype),
            pltpu.VMEM(sent_lse.shape, sent_lse.dtype),
            pltpu.VMEM(sent.shape, sent.dtype),
            pltpu.VMEM(sent_lse.shape, sent_lse.dtype),
            pltpu.VMEM(sent.shape, sent.dtype),
            pltpu.VMEM(sent_lse.shape, sent_lse.dtype),
            dma(steps), dma(steps), dma(steps), dma(steps),
        ],
        compiler_params=pltpu.CompilerParams(
            collective_id=1, has_side_effects=True, vmem_limit_bytes=16 * MIB
        ),
        name="exchange",
    )(
        lengths, near(own), near(sent), near(own_lse), near(sent_lse),
        near(gq), near(giw), near(kbuf),
    )

    head_out, index_scores = pl.pallas_call(
        project_kernel,
        out_shape=(
            jax.ShapeDtypeStruct((rows, heads, weight.shape[2]), jnp.bfloat16),
            jax.ShapeDtypeStruct((rows, span), jnp.float32),
        ),
        in_specs=[vmem, vmem, vmem],
        out_specs=(vmem, hbm),
        scratch_shapes=[dma((1,))],
        compiler_params=pltpu.CompilerParams(vmem_limit_bytes=16 * MIB),
        name="project",
    )(near(attended), near(wbuf), near(scores))
    return (index_scores[None], head_out[None])


def solution(mesh):
    return jax.shard_map(
        functools.partial(on_device, mesh.shape["seq"]),
        mesh=mesh,
        in_specs=(
            P("section", "groups", "seq", None),
            P("section", "groups", "seq", None),
            P("section", "groups", "seq", None),
            P("section", "groups", "seq", None),
            P("section", "groups", "seq"),
            P("section", "seq", None, None),
            P("section", "groups", None, None),
            P("groups"),
        ),
        out_specs=(P("section", "groups", "seq"), P("section", "groups", "seq", None)),
        check_vma=False,
    )
```

```python
import functools

import jax
import jax.numpy as jnp
from jax import lax
from jax.experimental import pallas as pl
from jax.experimental.pallas import tpu as pltpu
from jax.sharding import PartitionSpec as P

LATENT_WIDTH = 512
ROTARY_WIDTH = 64
VALUE_WIDTH = 128
IDX_DIM = 128
BLOCK = 64
HEAD_GROUPS = 2
NEG = -1e30
LOG2E = 1.4426950408889634
FIRST = 4
MORE = 2
STRIP = 256
LANES = 128
PACKED = LATENT_WIDTH + LANES
MIB = 1024 * 1024
MESH = pl.DeviceIdType.MESH


class Line:
    def __init__(self, n):
        self.half = n // 2
        self.me = lax.axis_index("seq")
        self.z = lax.div(self.me, 2)
        self.y = lax.rem(self.me, 2)
        self.partner = self.me + 1 - 2 * self.y
        self.order = sorted(range(1, self.half), key=lambda k: (-k.bit_length(), k))

    def step(self, k, sign):
        if self.half & (self.half - 1):
            return lax.rem(self.z + sign * k + self.half, self.half)
        out = self.z
        for j in range(k.bit_length()):
            if k >> j & 1:
                bit = lax.rem(lax.div(self.z, 1 << j), 2)
                out = out + (1 - 2 * bit) * (1 << j)
        return out

    def to(self, k):
        return self.step(k, 1)

    def frm(self, k):
        return self.step(k, -1)

    def device(self, z):
        return 2 * z + self.y

    def greet(self):
        barrier = pltpu.get_barrier_semaphore()
        peers = [self.partner] + [self.device(self.to(k)) for k in self.order]
        for peer in peers:
            pl.semaphore_signal(
                barrier, inc=1, device_id={"seq": peer}, device_id_type=MESH
            )
        return lambda: pl.semaphore_wait(barrier, self.half)


def push(peer, src, dst, send_sem, recv_sem):
    return pltpu.make_async_remote_copy(
        src_ref=src,
        dst_ref=dst,
        send_sem=send_sem,
        recv_sem=recv_sem,
        device_id={"seq": peer},
        device_id_type=MESH,
    )


def gather_kernel(
    n, lq, iq, iw, sel, cache, keys, weight, gq, giw, cbuf, kbuf, wbuf, table,
    lqs, iqs, sels, load_sem, zsend, zrecv, ysend, yrecv,
):
    line = Line(n)
    me = line.me
    rows, heads, width = lqs.shape
    held = iw.shape[1]
    entered = line.greet()
    loads = [
        pltpu.make_async_copy(lq, lqs, load_sem.at[0]),
        pltpu.make_async_copy(iq, iqs, load_sem.at[1]),
        pltpu.make_async_copy(iw, giw.at[me], load_sem.at[2]),
        pltpu.make_async_copy(sel, sels, load_sem.at[3]),
        pltpu.make_async_copy(keys, kbuf, load_sem.at[4]),
        pltpu.make_async_copy(weight, wbuf, load_sem.at[5]),
    ]
    strips = cbuf.shape[1]
    for b in range(rows):
        for j in range(strips):
            loads.append(
                pltpu.make_async_copy(
                    cache.at[b, :, pl.ds(j * STRIP, STRIP)],
                    cbuf.at[b, j],
                    load_sem.at[6 + b * strips + j],
                )
            )
    for copy in loads[:4] + loads[6:] + loads[4:6]:
        copy.start()
    for copy in loads[:3]:
        copy.wait()

    lane = lax.broadcasted_iota(jnp.int32, (iqs.shape[1], LANES), 1)
    row = lax.broadcasted_iota(jnp.int32, (iqs.shape[1], LANES), 0)
    for b in range(rows):
        mine = iqs[b].astype(jnp.float32)
        turned = pltpu.roll(mine, LANES // 2, 1)
        if heads == 2 * iqs.shape[1]:
            spare = jnp.concatenate([turned, mine], axis=0)
        else:
            spare = jnp.where(row < held, turned, pltpu.roll(mine, held, 0))
        gq[me, b, :, 0:LATENT_WIDTH] = lqs[b, :, 0:LATENT_WIDTH]
        gq[me, b, :, LATENT_WIDTH:width] = lqs[b, :, LATENT_WIDTH:width]
        spare = spare.astype(jnp.bfloat16)
        gq[me, b, :, width:PACKED] = spare[:, width - LATENT_WIDTH :]
    entered()

    def pieces(owner):
        return [gq.at[owner, b] for b in range(rows)] + [giw.at[owner]]

    across, along, onward = [], {}, {}
    for r, ref in enumerate(pieces(me)):
        across.append(push(line.partner, ref, ref, ysend.at[0, r], yrecv.at[0, r]))
        for k in line.order:
            along[k, r] = push(
                line.device(line.to(k)), ref, ref, zsend.at[k, r], zrecv.at[k, r]
            )
    for k in line.order:
        for r, ref in enumerate(pieces(line.device(line.frm(k)))):
            onward[k, r] = push(line.partner, ref, ref, ysend.at[k, r], yrecv.at[k, r])
    for r in range(rows, -1, -1):
        for k in line.order:
            along[k, r].start()
        across[r].start()

    loads[3].wait()
    here = keys.shape[1] // BLOCK
    first = me * here
    chosen = sels[...]
    spots = lax.broadcasted_iota(jnp.int32, table.shape, 2)
    kept = jnp.zeros(table.shape, jnp.int32)
    counts = [jnp.zeros(table.shape, jnp.int32)] * 2
    nsel = (LANES - 2) // 2
    for i in range(sels.shape[2]):
        block = jnp.broadcast_to(chosen[:, :, i : i + 1], table.shape)
        mine = (block >= first) & (block < first + here)
        odd = block & 1
        for part in range(2):
            take = mine & (odd == part)
            kept = jnp.where(take & (spots == part * nsel + counts[part]), block, kept)
            counts[part] = counts[part] + jnp.where(take, 1, 0)
    kept = jnp.where(spots == LANES - 2, counts[0], kept)
    table[...] = jnp.where(spots == LANES - 1, counts[1], kept)

    for r in range(rows, -1, -1):
        for k in line.order:
            along[k, r].wait_recv()
            onward[k, r].start()
    for copy in loads[4:]:
        copy.wait()
    for r in range(rows, -1, -1):
        across[r].wait_recv()
        for k in line.order:
            onward[k, r].wait_recv()
    for r in range(rows, -1, -1):
        across[r].wait_send()
        for k in line.order:
            along[k, r].wait_send()
            onward[k, r].wait_send()


def local_kernel(table, lens, gq, cache, own, sent, own_lse, sent_lse):
    me = lax.axis_index("seq")
    side = lax.rem(me, 2)
    rows, strips, width, _ = cache.shape
    first = me * (strips * STRIP // BLOCK)
    per_strip = STRIP // LANES
    nsel = (LANES - 2) // 2

    def count_of(b, g, part):
        return table[b, g, LANES - 2 + part]

    heads = gq.shape[2]
    per_group = gq.shape[0] // HEAD_GROUPS
    wide = per_group * heads
    scale = (VALUE_WIDTH + ROTARY_WIDTH) ** (-0.5) * LOG2E
    lane = lax.broadcasted_iota(jnp.int32, (1, LANES), 1)
    spot = lax.broadcasted_iota(jnp.int32, (per_group // 2, heads, LANES), 2)

    def latents(b, g, j):
        tiles, ends = [], []
        for part in range(2):
            held = j < count_of(b, g, part)
            block = table[b, g, part * nsel + j]
            tile = jnp.where(held, (block - first) // 2, 0)
            start = pl.multiple_of(tile % per_strip * LANES, LANES)
            tiles.append(cache[b, tile // per_strip, :, pl.ds(start, LANES)])
            live = jnp.minimum(BLOCK, lens[b] - block * BLOCK)
            ends.append(part * BLOCK + jnp.where(held, live, 0))
        usable = (lane < ends[0]) | ((lane >= BLOCK) & (lane < ends[1]))
        low, high = tiles
        both = jnp.concatenate([low[:, :BLOCK], high[:, BLOCK:]], axis=1)
        return both, jnp.where(usable, 0.0, NEG)

    def chunk(b, g, query, base, tiles):
        parts = [latents(b, g, base + j) for j in range(tiles)]
        keys = jnp.concatenate([part for part, _ in parts], axis=1)
        bias = jnp.concatenate([part for _, part in parts], axis=1)
        s = jnp.dot(query, keys, preferred_element_type=jnp.float32)
        return s * scale + bias, keys

    def mix(p, keys):
        return lax.dot_general(
            p.astype(jnp.bfloat16),
            keys[:LATENT_WIDTH],
            (((1,), (1,)), ((), ())),
            preferred_element_type=jnp.float32,
        )

    @pl.loop(0, rows)
    def _(b):
        queries, state = [], []
        for g in range(HEAD_GROUPS):
            query = gq[pl.ds(g * per_group, per_group), b]
            if heads % 16:
                query = query.astype(jnp.float32)
            query = query.reshape(wide, PACKED)[:, :width].astype(jnp.bfloat16)
            queries.append(query)
        firsts = [chunk(b, g, queries[g], 0, FIRST) for g in range(HEAD_GROUPS)]
        for g, (s, keys) in enumerate(firsts):
            top = jnp.max(s, axis=1, keepdims=True)
            p = jnp.exp2(s - top)
            state.append((top, jnp.sum(p, axis=1, keepdims=True), mix(p, keys)))

        for g in range(HEAD_GROUPS):

            def more(c, carry, g=g):
                top, total, acc = carry
                s, keys = chunk(b, g, queries[g], FIRST + c * MORE, MORE)
                new = jnp.maximum(top, jnp.max(s, axis=1, keepdims=True))
                p = jnp.exp2(s - new)
                keep = jnp.exp2(top - new)
                total = total * keep + jnp.sum(p, axis=1, keepdims=True)
                return new, total, acc * keep + mix(p, keys)

            extra = jnp.maximum(count_of(b, g, 0), count_of(b, g, 1)) - FIRST
            steps = (jnp.maximum(extra, 0) + MORE - 1) // MORE
            top, total, acc = lax.fori_loop(0, steps, more, state[g])
            acc = (acc * (1.0 / total)).reshape(per_group // 2, 2, heads, LATENT_WIDTH)
            lse = jnp.broadcast_to(top + jnp.log2(total), (wide, LANES))
            lse = lse.reshape(per_group // 2, 2, heads, LANES)
            here_z = pl.ds(g * per_group // 2, per_group // 2)
            even = side == 0
            own[here_z, b] = jnp.where(even, acc[:, 0], acc[:, 1])
            sent[here_z, b] = jnp.where(even, acc[:, 1], acc[:, 0]).astype(jnp.bfloat16)
            own_lse[here_z] = jnp.where(
                spot == b, jnp.where(even, lse[:, 0], lse[:, 1]), own_lse[here_z]
            )
            sent_lse[here_z] = jnp.where(
                spot == b, jnp.where(even, lse[:, 1], lse[:, 0]), sent_lse[here_z]
            )


def exchange_kernel(
    n, lens, own, sent, own_lse, sent_lse, gq, giw, kbuf, attended, scores,
    kept, from_pair, pair_lse, joint, joint_lse, from_line, line_lse,
    ysend, yrecv, zsend, zrecv,
):
    line = Line(n)
    half, me = line.half, line.me
    _, rows, heads, latent = own.shape
    entered = line.greet()
    entered()

    ring = line.order + [0]
    across, along = {}, {}
    for k in ring:
        z = line.to(k)
        refs = [(sent_lse.at[z], pair_lse.at[z])]
        refs += [(sent.at[z, b], from_pair.at[z, b]) for b in range(rows)]
        for r, (src, dst) in enumerate(refs):
            across[k, r] = push(line.partner, src, dst, ysend.at[k, r], yrecv.at[k, r])
            across[k, r].start()

    span = kbuf.shape[1]
    tile = min(512, span)
    lane = lax.broadcasted_iota(jnp.int32, (1, tile), 1)
    held = giw.shape[2]
    group = 8
    diagonal = (
        lax.broadcasted_iota(jnp.int32, (n * group, held), 0) % group
        == lax.broadcasted_iota(jnp.int32, (n * group, held), 1)
    )
    low = lax.broadcasted_iota(jnp.int32, (n * group, LANES), 1) < LANES // 2

    def index_row(b):
        packed = gq[:, b, :, LATENT_WIDTH:PACKED].astype(jnp.float32)
        if heads == 2 * group:
            left = packed[:, :group].reshape(n * group, LANES)
            right = packed[:, group:].reshape(n * group, LANES)
        else:
            left = packed.reshape(n * group, LANES)
            right = pltpu.roll(left, n * group - held, 0)
        query = jnp.where(low, pltpu.roll(left, LANES // 2, 1), right)
        query = query.astype(jnp.bfloat16)
        weight = giw[:, b : b + 1].astype(jnp.float32)
        weight = jnp.broadcast_to(weight, (n, group, held)).reshape(n * group, held)
        weight = jnp.sum(jnp.where(diagonal, weight, 0.0), axis=1, keepdims=True)
        weight = jnp.broadcast_to(weight * IDX_DIM ** (-0.5), (n * group, LANES))
        length = lens[b]

        def step(c, carry):
            start = pl.multiple_of(c * tile, tile)
            dots = lax.dot_general(
                query,
                kbuf[b, pl.ds(start, tile), :],
                (((1,), (1,)), ((), ())),
                preferred_element_type=jnp.float32,
            )
            pieces = []
            for j in range(tile // LANES):
                part = jnp.maximum(dots[:, j * LANES : (j + 1) * LANES], 0.0) * weight
                pieces.append(jnp.sum(part, axis=0, keepdims=True))
            total = jnp.concatenate(pieces, axis=1)
            live = me * span + c * tile + lane < length
            scores[b : b + 1, pl.ds(start, tile)] = jnp.where(live, total, 0.0)
            return carry

        lax.fori_loop(0, span // tile, step, 0)

    def weigh(parts):
        best = functools.reduce(jnp.maximum, parts)
        grown = [jnp.exp2(part - best) for part in parts]
        whole = functools.reduce(jnp.add, grown)
        return [part / whole for part in grown], best + jnp.log2(whole)

    early = rows // 2
    for b in range(early):
        index_row(b)

    for k in ring:
        z = line.to(k)
        across[k, 0].wait_recv()
        (mine, theirs), lse = weigh([own_lse[z], pair_lse[z]])
        if k:
            joint_lse[z] = lse
            target = line.device(z)
            along[k, 0] = push(
                target, joint_lse.at[z], line_lse.at[line.z], zsend.at[k, 0], zrecv.at[k, 0]
            )
        else:
            line_lse[z] = lse
        for b in range(rows):
            across[k, b + 1].wait_recv()
            value = mine[:, b : b + 1] * own[z, b]
            value += theirs[:, b : b + 1] * from_pair[z, b].astype(jnp.float32)
            if k:
                joint[z, b] = value.astype(jnp.bfloat16)
                along[k, b + 1] = push(
                    target, joint.at[z, b], from_line.at[line.z, b],
                    zsend.at[k, b + 1], zrecv.at[k, b + 1],
                )
            else:
                kept[b] = value
        if k:
            for r in range(rows + 1):
                along[k, r].start()

    for b in range(early, rows):
        index_row(b)

    for k in line.order:
        along[k, 0].wait_recv()
    spans = [line.z] + [line.frm(k) for k in line.order]
    factors, _ = weigh([line_lse[z] for z in spans])
    for b in range(rows):
        for k in line.order:
            along[k, b + 1].wait_recv()
        value = factors[0][:, b : b + 1] * kept[b]
        for z, factor in zip(spans[1:], factors[1:]):
            value += factor[:, b : b + 1] * from_line[z, b].astype(jnp.float32)
        attended[b] = value.astype(attended.dtype)
    for copy in list(across.values()) + list(along.values()):
        copy.wait_send()


def project_kernel(attended, weight, scores, out, scores_out, sem):
    copy = pltpu.make_async_copy(scores, scores_out, sem.at[0])
    copy.start()
    rows, heads, latent = attended.shape
    flat = attended[...]
    if heads % 16:
        flat = flat.astype(jnp.float32)
    flat = flat.reshape(rows * heads, latent).astype(jnp.bfloat16)
    which = lax.broadcasted_iota(jnp.int32, (rows * heads, 1), 0) % heads
    y = jnp.zeros((rows * heads, weight.shape[2]), jnp.float32)
    for h in range(heads):
        part = jnp.dot(flat, weight[h], preferred_element_type=jnp.float32)
        y = jnp.where(which == h, part, y)
    out[...] = y.reshape(rows, heads, weight.shape[2]).astype(out.dtype)
    copy.wait()


def on_device(
    n,
    latent_cache,
    index_keys,
    latent_query,
    index_query,
    index_weight,
    value_up_weight,
    selected,
    lengths,
):
    cache, keys, lq = latent_cache[0], index_keys[0], latent_query[0]
    iq, iw, weight, sel = index_query[0], index_weight[0], value_up_weight[0], selected[0]
    rows, span, width = cache.shape
    heads = lq.shape[1]
    half = n // 2
    extra = -iq.shape[1] % 8
    if extra:
        iq = jnp.pad(iq, ((0, 0), (0, extra), (0, 0)))
    vmem = pl.BlockSpec(memory_space=pltpu.VMEM)
    smem = pl.BlockSpec(memory_space=pltpu.SMEM)
    hbm = pl.BlockSpec(memory_space=pl.ANY)
    dma = pltpu.SemaphoreType.DMA

    def far(x):
        return pltpu.with_memory_space_constraint(x, pltpu.HBM)

    def near(x):
        return pltpu.with_memory_space_constraint(x, pltpu.VMEM)

    gq, giw, cbuf, kbuf, wbuf, table = pl.pallas_call(
        functools.partial(gather_kernel, n),
        out_shape=(
            pltpu.VMEM((n, rows, heads, PACKED), lq.dtype),
            pltpu.VMEM((n,) + iw.shape, iw.dtype),
            pltpu.VMEM((rows, span // STRIP, width, STRIP), cache.dtype),
            pltpu.VMEM(keys.shape, keys.dtype),
            pltpu.VMEM(weight.shape, weight.dtype),
            pltpu.VMEM((rows, HEAD_GROUPS, LANES), jnp.int32),
        ),
        in_specs=[hbm] * 7,
        out_specs=(vmem,) * 6,
        scratch_shapes=[
            pltpu.VMEM(lq.shape, lq.dtype),
            pltpu.VMEM(iq.shape, iq.dtype),
            pltpu.VMEM(sel.shape, sel.dtype),
            dma((6 + rows * (span // STRIP),)),
            dma((half, rows + 1)), dma((half, rows + 1)),
            dma((half, rows + 1)), dma((half, rows + 1)),
        ],
        compiler_params=pltpu.CompilerParams(
            collective_id=0, has_side_effects=True, vmem_limit_bytes=16 * MIB
        ),
        name="gather",
    )(
        far(lq), far(iq), far(iw), far(sel), far(jnp.swapaxes(cache, 1, 2)),
        far(keys), far(weight),
    )

    own, sent, own_lse, sent_lse = pl.pallas_call(
        local_kernel,
        out_shape=(
            pltpu.VMEM((half, rows, heads, LATENT_WIDTH), jnp.float32),
            pltpu.VMEM((half, rows, heads, LATENT_WIDTH), jnp.bfloat16),
            pltpu.VMEM((half, heads, LANES), jnp.float32),
            pltpu.VMEM((half, heads, LANES), jnp.float32),
        ),
        in_specs=[smem, smem, vmem, vmem],
        out_specs=(vmem,) * 4,
        compiler_params=pltpu.CompilerParams(vmem_limit_bytes=16 * MIB),
        name="local",
    )(table, lengths, near(gq), near(cbuf))

    steps = (half, rows + 1)
    attended, scores = pl.pallas_call(
        functools.partial(exchange_kernel, n),
        out_shape=(
            pltpu.VMEM((rows, heads, LATENT_WIDTH), jnp.bfloat16),
            pltpu.VMEM((rows, span), jnp.float32),
        ),
        in_specs=[smem] + [vmem] * 7,
        out_specs=(vmem, vmem),
        scratch_shapes=[
            pltpu.VMEM((rows, heads, LATENT_WIDTH), jnp.float32),
            pltpu.VMEM(sent.shape, sent.dtype),
            pltpu.VMEM(sent_lse.shape, sent_lse.dtype),
            pltpu.VMEM(sent.shape, sent.dtype),
            pltpu.VMEM(sent_lse.shape, sent_lse.dtype),
            pltpu.VMEM(sent.shape, sent.dtype),
            pltpu.VMEM(sent_lse.shape, sent_lse.dtype),
            dma(steps), dma(steps), dma(steps), dma(steps),
        ],
        compiler_params=pltpu.CompilerParams(
            collective_id=1, has_side_effects=True, vmem_limit_bytes=16 * MIB
        ),
        name="exchange",
    )(
        lengths, near(own), near(sent), near(own_lse), near(sent_lse),
        near(gq), near(giw), near(kbuf),
    )

    head_out, index_scores = pl.pallas_call(
        project_kernel,
        out_shape=(
            jax.ShapeDtypeStruct((rows, heads, weight.shape[2]), jnp.bfloat16),
            jax.ShapeDtypeStruct((rows, span), jnp.float32),
        ),
        in_specs=[vmem, vmem, vmem],
        out_specs=(vmem, hbm),
        scratch_shapes=[dma((1,))],
        compiler_params=pltpu.CompilerParams(vmem_limit_bytes=16 * MIB),
        name="project",
    )(near(attended), near(wbuf), near(scores))
    return (index_scores[None], head_out[None])


def solution(mesh):
    return jax.shard_map(
        functools.partial(on_device, mesh.shape["seq"]),
        mesh=mesh,
        in_specs=(
            P("section", "groups", "seq", None),
            P("section", "groups", "seq", None),
            P("section", "groups", "seq", None),
            P("section", "groups", "seq", None),
            P("section", "groups", "seq"),
            P("section", "seq", None, None),
            P("section", "groups", None, None),
            P("groups"),
        ),
        out_specs=(P("section", "groups", "seq"), P("section", "groups", "seq", None)),
        check_vma=False,
    )
```

```python
import functools

import jax
import jax.numpy as jnp
from jax import lax
from jax.experimental import pallas as pl
from jax.experimental.pallas import tpu as pltpu
from jax.sharding import PartitionSpec as P

LATENT_WIDTH = 512
ROTARY_WIDTH = 64
VALUE_WIDTH = 128
IDX_DIM = 128
BLOCK = 64
HEAD_GROUPS = 2
NEG = -1e30
LOG2E = 1.4426950408889634
FIRST = 4
MORE = 2
STRIP = 256
LANES = 128
PACKED = LATENT_WIDTH + LANES
MIB = 1024 * 1024
MESH = pl.DeviceIdType.MESH


class Line:
    def __init__(self, n):
        self.half = n // 2
        self.me = lax.axis_index("seq")
        self.z = lax.div(self.me, 2)
        self.y = lax.rem(self.me, 2)
        self.partner = self.me + 1 - 2 * self.y
        self.order = sorted(range(1, self.half), key=lambda k: (-k.bit_length(), k))

    def step(self, k, sign):
        if self.half & (self.half - 1):
            return lax.rem(self.z + sign * k + self.half, self.half)
        out = self.z
        for j in range(k.bit_length()):
            if k >> j & 1:
                bit = lax.rem(lax.div(self.z, 1 << j), 2)
                out = out + (1 - 2 * bit) * (1 << j)
        return out

    def to(self, k):
        return self.step(k, 1)

    def frm(self, k):
        return self.step(k, -1)

    def device(self, z):
        return 2 * z + self.y

    def opposite(self, z):
        return 2 * z + 1 - self.y

    def greet(self):
        barrier = pltpu.get_barrier_semaphore()
        n = 2 * self.half
        for k in range(1, n):
            peer = lax.rem(self.me + k, n)
            pl.semaphore_signal(
                barrier, inc=1, device_id={"seq": peer}, device_id_type=MESH
            )
        return lambda: pl.semaphore_wait(barrier, n - 1)


def push(peer, src, dst, send_sem, recv_sem):
    return pltpu.make_async_remote_copy(
        src_ref=src,
        dst_ref=dst,
        send_sem=send_sem,
        recv_sem=recv_sem,
        device_id={"seq": peer},
        device_id_type=MESH,
    )


def gather_kernel(
    n, lq, iq, iw, sel, cache, keys, weight, gq, giw, cbuf, kbuf, wbuf, table,
    lqs, iqs, sels, load_sem, zsend, zrecv, ysend, yrecv, dsend, drecv,
):
    line = Line(n)
    me = line.me
    rows, heads, width = lqs.shape
    held = iw.shape[1]
    entered = line.greet()
    loads = [
        pltpu.make_async_copy(lq, lqs, load_sem.at[0]),
        pltpu.make_async_copy(iq, iqs, load_sem.at[1]),
        pltpu.make_async_copy(iw, giw.at[me], load_sem.at[2]),
        pltpu.make_async_copy(sel, sels, load_sem.at[3]),
        pltpu.make_async_copy(keys, kbuf, load_sem.at[4]),
        pltpu.make_async_copy(weight, wbuf, load_sem.at[5]),
    ]
    strips = cbuf.shape[1]
    for b in range(rows):
        for j in range(strips):
            loads.append(
                pltpu.make_async_copy(
                    cache.at[b, :, pl.ds(j * STRIP, STRIP)],
                    cbuf.at[b, j],
                    load_sem.at[6 + b * strips + j],
                )
            )
    for copy in loads[:4] + loads[6:] + loads[4:6]:
        copy.start()
    for copy in loads[:3]:
        copy.wait()

    lane = lax.broadcasted_iota(jnp.int32, (iqs.shape[1], LANES), 1)
    row = lax.broadcasted_iota(jnp.int32, (iqs.shape[1], LANES), 0)
    for b in range(rows):
        mine = iqs[b].astype(jnp.float32)
        turned = pltpu.roll(mine, LANES // 2, 1)
        if heads == 2 * iqs.shape[1]:
            spare = jnp.concatenate([turned, mine], axis=0)
        else:
            spare = jnp.where(row < held, turned, pltpu.roll(mine, held, 0))
        gq[me, b, :, 0:LATENT_WIDTH] = lqs[b, :, 0:LATENT_WIDTH]
        gq[me, b, :, LATENT_WIDTH:width] = lqs[b, :, LATENT_WIDTH:width]
        spare = spare.astype(jnp.bfloat16)
        gq[me, b, :, width:PACKED] = spare[:, width - LATENT_WIDTH :]
    entered()

    def pieces(owner):
        return [gq.at[owner, b] for b in range(rows)] + [giw.at[owner]]

    across, along, onward, slant = [], {}, {}, {}
    for r, ref in enumerate(pieces(me)):
        across.append(push(line.partner, ref, ref, ysend.at[0, r], yrecv.at[0, r]))
        for k in line.order:
            along[k, r] = push(
                line.device(line.to(k)), ref, ref, zsend.at[k, r], zrecv.at[k, r]
            )
    for k in line.order:
        ref = pieces(me)[0]
        slant[k] = push(line.opposite(line.to(k)), ref, ref, dsend.at[k], drecv.at[k])
        for r, ref in enumerate(pieces(line.device(line.frm(k)))):
            if r == 0:
                continue
            onward[k, r] = push(line.partner, ref, ref, ysend.at[k, r], yrecv.at[k, r])
    for r in range(rows, -1, -1):
        for k in line.order:
            along[k, r].start()
            if r == 0:
                slant[k].start()
        across[r].start()

    loads[3].wait()
    here = keys.shape[1] // BLOCK
    first = me * here
    chosen = sels[...]
    spots = lax.broadcasted_iota(jnp.int32, table.shape, 2)
    kept = jnp.zeros(table.shape, jnp.int32)
    counts = [jnp.zeros(table.shape, jnp.int32)] * 2
    nsel = (LANES - 2) // 2
    for i in range(sels.shape[2]):
        block = jnp.broadcast_to(chosen[:, :, i : i + 1], table.shape)
        mine = (block >= first) & (block < first + here)
        odd = block & 1
        for part in range(2):
            take = mine & (odd == part)
            kept = jnp.where(take & (spots == part * nsel + counts[part]), block, kept)
            counts[part] = counts[part] + jnp.where(take, 1, 0)
    kept = jnp.where(spots == LANES - 2, counts[0], kept)
    table[...] = jnp.where(spots == LANES - 1, counts[1], kept)

    for r in range(rows, 0, -1):
        for k in line.order:
            along[k, r].wait_recv()
            onward[k, r].start()
    for copy in loads[4:]:
        copy.wait()
    direct = [along[k, 0] for k in line.order] + list(slant.values())
    for copy in direct + across + list(onward.values()):
        copy.wait_recv()
    for copy in across + list(along.values()) + list(onward.values()) + list(slant.values()):
        copy.wait_send()


def local_kernel(table, lens, gq, cache, own, own_first, sent, lse_out):
    me = lax.axis_index("seq")
    side = lax.rem(me, 2)
    rows, strips, width, _ = cache.shape
    first = me * (strips * STRIP // BLOCK)
    per_strip = STRIP // LANES
    nsel = (LANES - 2) // 2

    def count_of(b, g, part):
        return table[b, g, LANES - 2 + part]

    heads = gq.shape[2]
    per_group = gq.shape[0] // HEAD_GROUPS
    wide = per_group * heads
    scale = (VALUE_WIDTH + ROTARY_WIDTH) ** (-0.5) * LOG2E
    lane = lax.broadcasted_iota(jnp.int32, (1, LANES), 1)
    head = lax.broadcasted_iota(jnp.int32, (wide, LANES), 0)
    spot = lax.broadcasted_iota(jnp.int32, (wide, LANES), 1)

    def latents(b, g, j):
        tiles, ends = [], []
        for part in range(2):
            held = j < count_of(b, g, part)
            block = table[b, g, part * nsel + j]
            tile = jnp.where(held, (block - first) // 2, 0)
            start = pl.multiple_of(tile % per_strip * LANES, LANES)
            tiles.append(cache[b, tile // per_strip, :, pl.ds(start, LANES)])
            live = jnp.minimum(BLOCK, lens[b] - block * BLOCK)
            ends.append(part * BLOCK + jnp.where(held, live, 0))
        usable = (lane < ends[0]) | ((lane >= BLOCK) & (lane < ends[1]))
        low, high = tiles
        both = jnp.concatenate([low[:, :BLOCK], high[:, BLOCK:]], axis=1)
        return both, jnp.where(usable, 0.0, NEG)

    def chunk(b, g, query, base, tiles):
        parts = [latents(b, g, base + j) for j in range(tiles)]
        keys = jnp.concatenate([part for part, _ in parts], axis=1)
        bias = jnp.concatenate([part for _, part in parts], axis=1)
        s = jnp.dot(query, keys, preferred_element_type=jnp.float32)
        return s * scale + bias, keys

    def mix(p, keys):
        return lax.dot_general(
            p.astype(jnp.bfloat16),
            keys[:LATENT_WIDTH],
            (((1,), (1,)), ((), ())),
            preferred_element_type=jnp.float32,
        )

    @pl.loop(0, rows)
    def _(b):
        queries, state = [], []
        for g in range(HEAD_GROUPS):
            query = gq[pl.ds(g * per_group, per_group), b]
            if heads % 16:
                query = query.astype(jnp.float32)
            query = query.reshape(wide, PACKED)[:, :width].astype(jnp.bfloat16)
            queries.append(query)
        firsts = [chunk(b, g, queries[g], 0, FIRST) for g in range(HEAD_GROUPS)]
        for g, (s, keys) in enumerate(firsts):
            top = jnp.max(s, axis=1, keepdims=True)
            p = jnp.exp2(s - top)
            state.append((top, jnp.sum(p, axis=1, keepdims=True), mix(p, keys)))

        def more(c, carry):
            after = []
            chunks = [
                chunk(b, g, queries[g], FIRST + c * MORE, MORE) for g in range(HEAD_GROUPS)
            ]
            for (s, keys), (top, total, acc) in zip(chunks, carry):
                new = jnp.maximum(top, jnp.max(s, axis=1, keepdims=True))
                p = jnp.exp2(s - new)
                keep = jnp.exp2(top - new)
                total = total * keep + jnp.sum(p, axis=1, keepdims=True)
                after.append((new, total, acc * keep + mix(p, keys)))
            return after

        extra = functools.reduce(
            jnp.maximum,
            [count_of(b, g, part) for g in range(HEAD_GROUPS) for part in range(2)],
        )
        extra = jnp.maximum(extra - FIRST, 0)
        state = lax.fori_loop(0, (extra + MORE - 1) // MORE, more, state)
        lses = jnp.zeros((1, LANES), jnp.float32)
        for g, (top, total, acc) in enumerate(state):
            acc = (acc * (1.0 / total)).reshape(per_group // 2, 2, heads, LATENT_WIDTH)
            lse = jnp.broadcast_to(top + jnp.log2(total), (wide, LANES))
            lse = jnp.where(spot == head + g * wide, lse, 0.0)
            lses += jnp.sum(lse, axis=0, keepdims=True)
            here_z = pl.ds(g * per_group // 2, per_group // 2)
            even = side == 0
            mine = jnp.where(even, acc[:, 0], acc[:, 1])
            own[here_z, b] = mine
            sent[here_z, b] = jnp.where(even, acc[:, 1], acc[:, 0]).astype(jnp.bfloat16)

            @pl.when(b == 0)
            def _(mine=mine, here_z=here_z):
                own_first[here_z] = mine.astype(jnp.bfloat16)

        lse_out[pl.ds(b, 1)] = lses


def exchange_kernel(
    n, lens, own, own_first, sent, lse, gq, giw, kbuf, attended, scores,
    kept, from_pair, joint, from_line, firsts, lses, share, share_first,
    ysend, yrecv, zsend, zrecv, fsend, frecv, lsend, lrecv,
):
    line = Line(n)
    half, me = line.half, line.me
    _, rows, heads, latent = own.shape
    entered = line.greet()
    entered()

    ring = line.order + [0]
    across, along, first, told = {}, {}, {}, {}
    for k in range(1, n):
        told[k] = push(
            lax.rem(me + k, n), lse, lses.at[me], lsend.at[k], lrecv.at[k]
        )
        told[k].start()
    for k in ring:
        z = line.to(k)
        for b in range(1, rows):
            across[k, b] = push(
                line.partner, sent.at[z, b], from_pair.at[z, b], ysend.at[k, b], yrecv.at[k, b]
            )
            across[k, b].start()
        peers = [(1, line.opposite(z), sent.at[z, 0])]
        if k:
            peers.append((0, line.device(z), own_first.at[z]))
        for side, peer, src in peers:
            first[k, side] = push(
                peer, src, firsts.at[me], fsend.at[k, side], frecv.at[k, side]
            )
            first[k, side].start()

    span = kbuf.shape[1]
    tile = min(512, span)
    lane = lax.broadcasted_iota(jnp.int32, (1, tile), 1)
    held = giw.shape[2]
    group = 8
    diagonal = (
        lax.broadcasted_iota(jnp.int32, (n * group, held), 0) % group
        == lax.broadcasted_iota(jnp.int32, (n * group, held), 1)
    )
    low = lax.broadcasted_iota(jnp.int32, (n * group, LANES), 1) < LANES // 2

    def index_row(b):
        packed = gq[:, b, :, LATENT_WIDTH:PACKED].astype(jnp.float32)
        if heads == 2 * group:
            left = packed[:, :group].reshape(n * group, LANES)
            right = packed[:, group:].reshape(n * group, LANES)
        else:
            left = packed.reshape(n * group, LANES)
            right = pltpu.roll(left, n * group - held, 0)
        query = jnp.where(low, pltpu.roll(left, LANES // 2, 1), right)
        query = query.astype(jnp.bfloat16)
        weight = giw[:, b : b + 1].astype(jnp.float32)
        weight = jnp.broadcast_to(weight, (n, group, held)).reshape(n * group, held)
        weight = jnp.sum(jnp.where(diagonal, weight, 0.0), axis=1, keepdims=True)
        weight = jnp.broadcast_to(weight * IDX_DIM ** (-0.5), (n * group, LANES))
        length = lens[b]

        def step(c, carry):
            start = pl.multiple_of(c * tile, tile)
            dots = lax.dot_general(
                query,
                kbuf[b, pl.ds(start, tile), :],
                (((1,), (1,)), ((), ())),
                preferred_element_type=jnp.float32,
            )
            pieces = []
            for j in range(tile // LANES):
                part = jnp.maximum(dots[:, j * LANES : (j + 1) * LANES], 0.0) * weight
                pieces.append(jnp.sum(part, axis=0, keepdims=True))
            total = jnp.concatenate(pieces, axis=1)
            live = me * span + c * tile + lane < length
            scores[b : b + 1, pl.ds(start, tile)] = jnp.where(live, total, 0.0)
            return carry

        lax.fori_loop(0, span // tile, step, 0)

    early = rows // 2
    for b in range(early):
        index_row(b)

    for copy in told.values():
        copy.wait_recv()
    lses[me] = lse[...]
    table = [lses[s] for s in range(n)]
    best = functools.reduce(jnp.maximum, table)
    whole = functools.reduce(jnp.add, [jnp.exp2(part - best) for part in table])
    best = best + jnp.log2(whole)
    both = [jnp.exp2(lse[...] - best), jnp.exp2(lses[line.partner] - best)]
    share[...] = jnp.transpose(jnp.concatenate(both, axis=0))
    share_first[...] = jnp.transpose(
        jnp.concatenate([jnp.exp2(part[0:1] - best[0:1]) for part in table], axis=0)
    )

    for k in ring:
        z = line.to(k)
        target = line.device(z)
        part = share[pl.ds(pl.multiple_of(target * heads, heads), heads)]
        for b in range(1, rows):
            across[k, b].wait_recv()
            value = part[:, b : b + 1] * own[z, b]
            value += part[:, rows + b : rows + b + 1] * from_pair[z, b].astype(jnp.float32)
            if k:
                joint[z, b] = value.astype(jnp.bfloat16)
                along[k, b] = push(
                    target, joint.at[z, b], from_line.at[line.z, b],
                    zsend.at[k, b], zrecv.at[k, b],
                )
            else:
                kept[b] = value
        if k:
            for b in range(1, rows):
                along[k, b].start()

    for b in range(early, rows):
        index_row(b)

    for copy in first.values():
        copy.wait_recv()
    firsts[me] = jnp.zeros((heads, latent), firsts.dtype)
    part = share_first[pl.ds(pl.multiple_of(me * heads, heads), heads)]
    mine = share[pl.ds(pl.multiple_of(me * heads, heads), heads)]
    value = mine[:, 0:1] * own[line.z, 0]
    for s in range(n):
        value += part[:, s : s + 1] * firsts[s].astype(jnp.float32)
    attended[0] = value.astype(attended.dtype)
    for b in range(1, rows):
        value = kept[b]
        for k in line.order:
            along[k, b].wait_recv()
            value += from_line[line.frm(k), b].astype(jnp.float32)
        attended[b] = value.astype(attended.dtype)
    copies = [across, along, first, told]
    for copy in [copy for group in copies for copy in group.values()]:
        copy.wait_send()


def project_kernel(attended, weight, scores, out, scores_out, sem):
    copy = pltpu.make_async_copy(scores, scores_out, sem.at[0])
    copy.start()
    rows, heads, latent = attended.shape
    flat = attended[...]
    if heads % 16:
        flat = flat.astype(jnp.float32)
    flat = flat.reshape(rows * heads, latent).astype(jnp.bfloat16)
    which = lax.broadcasted_iota(jnp.int32, (rows * heads, 1), 0) % heads
    y = jnp.zeros((rows * heads, weight.shape[2]), jnp.float32)
    for h in range(heads):
        part = jnp.dot(flat, weight[h], preferred_element_type=jnp.float32)
        y = jnp.where(which == h, part, y)
    out[...] = y.reshape(rows, heads, weight.shape[2]).astype(out.dtype)
    copy.wait()


def on_device(
    n,
    latent_cache,
    index_keys,
    latent_query,
    index_query,
    index_weight,
    value_up_weight,
    selected,
    lengths,
):
    cache, keys, lq = latent_cache[0], index_keys[0], latent_query[0]
    iq, iw, weight, sel = index_query[0], index_weight[0], value_up_weight[0], selected[0]
    rows, span, width = cache.shape
    heads = lq.shape[1]
    half = n // 2
    extra = -iq.shape[1] % 8
    if extra:
        iq = jnp.pad(iq, ((0, 0), (0, extra), (0, 0)))
    vmem = pl.BlockSpec(memory_space=pltpu.VMEM)
    smem = pl.BlockSpec(memory_space=pltpu.SMEM)
    hbm = pl.BlockSpec(memory_space=pl.ANY)
    dma = pltpu.SemaphoreType.DMA

    def far(x):
        return pltpu.with_memory_space_constraint(x, pltpu.HBM)

    def near(x):
        return pltpu.with_memory_space_constraint(x, pltpu.VMEM)

    gq, giw, cbuf, kbuf, wbuf, table = pl.pallas_call(
        functools.partial(gather_kernel, n),
        out_shape=(
            pltpu.VMEM((n, rows, heads, PACKED), lq.dtype),
            pltpu.VMEM((n,) + iw.shape, iw.dtype),
            pltpu.VMEM((rows, span // STRIP, width, STRIP), cache.dtype),
            pltpu.VMEM(keys.shape, keys.dtype),
            pltpu.VMEM(weight.shape, weight.dtype),
            pltpu.VMEM((rows, HEAD_GROUPS, LANES), jnp.int32),
        ),
        in_specs=[hbm] * 7,
        out_specs=(vmem,) * 6,
        scratch_shapes=[
            pltpu.VMEM(lq.shape, lq.dtype),
            pltpu.VMEM(iq.shape, iq.dtype),
            pltpu.VMEM(sel.shape, sel.dtype),
            dma((6 + rows * (span // STRIP),)),
            dma((half, rows + 1)), dma((half, rows + 1)),
            dma((half, rows + 1)), dma((half, rows + 1)),
            dma((half,)), dma((half,)),
        ],
        compiler_params=pltpu.CompilerParams(
            collective_id=0, has_side_effects=True, vmem_limit_bytes=16 * MIB
        ),
        name="gather",
    )(
        far(lq), far(iq), far(iw), far(sel), far(jnp.swapaxes(cache, 1, 2)),
        far(keys), far(weight),
    )

    own, own_first, sent, lse = pl.pallas_call(
        local_kernel,
        out_shape=(
            pltpu.VMEM((half, rows, heads, LATENT_WIDTH), jnp.float32),
            pltpu.VMEM((half, heads, LATENT_WIDTH), jnp.bfloat16),
            pltpu.VMEM((half, rows, heads, LATENT_WIDTH), jnp.bfloat16),
            pltpu.VMEM((rows, n * heads), jnp.float32),
        ),
        in_specs=[smem, smem, vmem, vmem],
        out_specs=(vmem,) * 4,
        compiler_params=pltpu.CompilerParams(vmem_limit_bytes=16 * MIB),
        name="local",
    )(table, lengths, near(gq), near(cbuf))

    attended, scores = pl.pallas_call(
        functools.partial(exchange_kernel, n),
        out_shape=(
            pltpu.VMEM((rows, heads, LATENT_WIDTH), jnp.bfloat16),
            pltpu.VMEM((rows, span), jnp.float32),
        ),
        in_specs=[smem] + [vmem] * 7,
        out_specs=(vmem, vmem),
        scratch_shapes=[
            pltpu.VMEM((rows, heads, LATENT_WIDTH), jnp.float32),
            pltpu.VMEM(sent.shape, sent.dtype),
            pltpu.VMEM(sent.shape, sent.dtype),
            pltpu.VMEM(sent.shape, sent.dtype),
            pltpu.VMEM((n, heads, LATENT_WIDTH), sent.dtype),
            pltpu.VMEM((n,) + lse.shape, lse.dtype),
            pltpu.VMEM((n * heads, 2 * rows), jnp.float32),
            pltpu.VMEM((n * heads, n), jnp.float32),
            dma((half, rows)), dma((half, rows)), dma((half, rows)), dma((half, rows)),
            dma((half, 2)), dma((half, 2)), dma((n,)), dma((n,)),
        ],
        compiler_params=pltpu.CompilerParams(
            collective_id=1, has_side_effects=True, vmem_limit_bytes=16 * MIB
        ),
        name="exchange",
    )(
        lengths, near(own), near(own_first), near(sent), near(lse),
        near(gq), near(giw), near(kbuf),
    )

    head_out, index_scores = pl.pallas_call(
        project_kernel,
        out_shape=(
            jax.ShapeDtypeStruct((rows, heads, weight.shape[2]), jnp.bfloat16),
            jax.ShapeDtypeStruct((rows, span), jnp.float32),
        ),
        in_specs=[vmem, vmem, vmem],
        out_specs=(vmem, hbm),
        scratch_shapes=[dma((1,))],
        compiler_params=pltpu.CompilerParams(vmem_limit_bytes=16 * MIB),
        name="project",
    )(near(attended), near(wbuf), near(scores))
    return (index_scores[None], head_out[None])


def solution(mesh):
    return jax.shard_map(
        functools.partial(on_device, mesh.shape["seq"]),
        mesh=mesh,
        in_specs=(
            P("section", "groups", "seq", None),
            P("section", "groups", "seq", None),
            P("section", "groups", "seq", None),
            P("section", "groups", "seq", None),
            P("section", "groups", "seq"),
            P("section", "seq", None, None),
            P("section", "groups", None, None),
            P("groups"),
        ),
        out_specs=(P("section", "groups", "seq"), P("section", "groups", "seq", None)),
        check_vma=False,
    )
```

```python
import functools

import jax
import jax.numpy as jnp
from jax import lax
from jax.experimental import pallas as pl
from jax.experimental.pallas import tpu as pltpu
from jax.sharding import PartitionSpec as P

LATENT_WIDTH = 512
ROTARY_WIDTH = 64
VALUE_WIDTH = 128
IDX_DIM = 128
BLOCK = 64
HEAD_GROUPS = 2
NEG = -1e30
LOG2E = 1.4426950408889634
FIRST = 4
MORE = 2
STRIP = 128
EARLY = 2
SLOTS = 62
LANES = 128
PACKED = LATENT_WIDTH + LANES
MIB = 1024 * 1024
MESH = pl.DeviceIdType.MESH


class Line:
    def __init__(self, n):
        self.half = n // 2
        self.me = lax.axis_index("seq")
        self.z = lax.div(self.me, 2)
        self.y = lax.rem(self.me, 2)
        self.partner = self.me + 1 - 2 * self.y
        self.order = list(range(1, self.half))
        self.far = sorted(self.order, key=lambda k: (-k.bit_length(), k))

    def step(self, k, sign):
        if self.half & (self.half - 1):
            return lax.rem(self.z + sign * k + self.half, self.half)
        out = self.z
        for j in range(k.bit_length()):
            if k >> j & 1:
                bit = lax.rem(lax.div(self.z, 1 << j), 2)
                out = out + (1 - 2 * bit) * (1 << j)
        return out

    def to(self, k):
        return self.step(k, 1)

    def frm(self, k):
        return self.step(k, -1)

    def device(self, z):
        return 2 * z + self.y

    def opposite(self, z):
        return 2 * z + 1 - self.y

    def greet(self):
        barrier = pltpu.get_barrier_semaphore()
        n = 2 * self.half
        for k in range(1, n):
            peer = lax.rem(self.me + k, n)
            pl.semaphore_signal(
                barrier, inc=1, device_id={"seq": peer}, device_id_type=MESH
            )
        return lambda: pl.semaphore_wait(barrier, n - 1)


def push(peer, src, dst, send_sem, recv_sem):
    return pltpu.make_async_remote_copy(
        src_ref=src,
        dst_ref=dst,
        send_sem=send_sem,
        recv_sem=recv_sem,
        device_id={"seq": peer},
        device_id_type=MESH,
    )


def index_row(n, b, gq, giw, kbuf, length, store):
    me = lax.axis_index("seq")
    heads, held, span = gq.shape[2], giw.shape[2], kbuf.shape[1]
    tile = min(512, span)
    group = 8
    lane = lax.broadcasted_iota(jnp.int32, (1, tile), 1)
    diagonal = (
        lax.broadcasted_iota(jnp.int32, (n * group, held), 0) % group
        == lax.broadcasted_iota(jnp.int32, (n * group, held), 1)
    )
    low = lax.broadcasted_iota(jnp.int32, (n * group, LANES), 1) < LANES // 2
    packed = gq[:, b, :, LATENT_WIDTH:PACKED].astype(jnp.float32)
    if heads == 2 * group:
        left = packed[:, :group].reshape(n * group, LANES)
        right = packed[:, group:].reshape(n * group, LANES)
    else:
        left = packed.reshape(n * group, LANES)
        right = pltpu.roll(left, n * group - held, 0)
    query = jnp.where(low, pltpu.roll(left, LANES // 2, 1), right)
    query = query.astype(jnp.bfloat16)
    weight = giw[:, b : b + 1].astype(jnp.float32)
    weight = jnp.broadcast_to(weight, (n, group, held)).reshape(n * group, held)
    weight = jnp.sum(jnp.where(diagonal, weight, 0.0), axis=1, keepdims=True)
    weight = jnp.broadcast_to(weight * IDX_DIM ** (-0.5), (n * group, LANES))

    def step(c, carry):
        start = pl.multiple_of(c * tile, tile)
        dots = lax.dot_general(
            query,
            kbuf[b, pl.ds(start, tile), :],
            (((1,), (1,)), ((), ())),
            preferred_element_type=jnp.float32,
        )
        pieces = []
        for j in range(tile // LANES):
            part = jnp.maximum(dots[:, j * LANES : (j + 1) * LANES], 0.0) * weight
            pieces.append(jnp.sum(part, axis=0, keepdims=True))
        total = jnp.concatenate(pieces, axis=1)
        live = me * span + c * tile + lane < length
        store(pl.ds(start, tile), jnp.where(live, total, 0.0))
        return carry

    lax.fori_loop(0, span // tile, step, 0)


def gather_kernel(
    n, lq, iq, iw, sel, lens, cache, keys, weight, gq, giw, cbuf, kbuf, wbuf, table, scores,
    lqs, iqs, sels, ends, load_sem, zsend, zrecv, ysend, yrecv,
):
    line = Line(n)
    me = line.me
    rows, heads, width = lqs.shape
    held = iw.shape[1]
    loads = [
        pltpu.make_async_copy(lq, lqs, load_sem.at[0]),
        pltpu.make_async_copy(iq, iqs, load_sem.at[1]),
        pltpu.make_async_copy(iw, giw.at[me], load_sem.at[2]),
        pltpu.make_async_copy(sel, sels, load_sem.at[3]),
        pltpu.make_async_copy(lens, ends, load_sem.at[4]),
        pltpu.make_async_copy(keys, kbuf, load_sem.at[5]),
        pltpu.make_async_copy(weight, wbuf, load_sem.at[6]),
    ]
    strips = cbuf.shape[1]
    for b in range(rows):
        for j in range(strips):
            loads.append(
                pltpu.make_async_copy(
                    cache.at[b, :, pl.ds(j * STRIP, STRIP)],
                    cbuf.at[b, j],
                    load_sem.at[7 + b * strips + j],
                )
            )
    for copy in loads[:5]:
        copy.start()
    entered = line.greet()
    for copy in loads[:3]:
        copy.wait()

    lane = lax.broadcasted_iota(jnp.int32, (iqs.shape[1], LANES), 1)
    row = lax.broadcasted_iota(jnp.int32, (iqs.shape[1], LANES), 0)
    for b in range(rows):
        mine = iqs[b].astype(jnp.float32)
        turned = pltpu.roll(mine, LANES // 2, 1)
        if heads == 2 * iqs.shape[1]:
            spare = jnp.concatenate([turned, mine], axis=0)
        else:
            spare = jnp.where(row < held, turned, pltpu.roll(mine, held, 0))
        gq[me, b, :, 0:LATENT_WIDTH] = lqs[b, :, 0:LATENT_WIDTH]
        gq[me, b, :, LATENT_WIDTH:width] = lqs[b, :, LATENT_WIDTH:width]
        spare = spare.astype(jnp.bfloat16)
        gq[me, b, :, width:PACKED] = spare[:, width - LATENT_WIDTH :]
    entered()

    def piece(owner, r):
        return gq.at[owner, r] if r < rows else giw.at[owner]

    relayed = (0,) if line.half == 4 else ()
    turns = [0, rows] + list(range(1, rows))
    across, along, onward, relay = {}, {}, {}, {}
    for r in turns:
        ref = piece(me, r)
        across[r] = push(line.partner, ref, ref, ysend.at[0, r], yrecv.at[0, r])
        for k in line.order:
            ref = piece(me, r)
            if r in relayed and k == 3:
                ref = piece(line.device(line.frm(2)), r)
                target = line.device(line.to(1))
            else:
                target = line.device(line.to(k))
            along[k, r] = push(target, ref, ref, zsend.at[k, r], zrecv.at[k, r])
            ref = piece(line.device(line.frm(k)), r)
            onward[k, r] = push(line.partner, ref, ref, ysend.at[k, r], yrecv.at[k, r])
    for r in turns:
        across[r].start()
    for r in turns:
        for k in line.order:
            if not (r in relayed and k == 3):
                along[k, r].start()
    for copy in loads[5:]:
        copy.start()

    for copy in loads[3:5]:
        copy.wait()
    first = me * (keys.shape[1] // BLOCK)
    here = keys.shape[1] // BLOCK
    chosen = sels[...]
    spots = lax.broadcasted_iota(jnp.int32, table.shape, 2)
    which = lax.broadcasted_iota(jnp.int32, table.shape, 0)
    kept = jnp.zeros(table.shape, jnp.int32)
    counts = [jnp.zeros(table.shape, jnp.int32)] * 2
    for i in range(sels.shape[2]):
        block = jnp.broadcast_to(chosen[:, :, i : i + 1], table.shape)
        mine = (block >= first) & (block < first + here)
        odd = block & 1
        for part in range(2):
            take = mine & (odd == part)
            kept = jnp.where(take & (spots == part * SLOTS + counts[part]), block, kept)
            counts[part] = counts[part] + jnp.where(take, 1, 0)
    for b in range(rows):
        kept = jnp.where((spots == LANES - 3) & (which == b), ends[b], kept)
    kept = jnp.where(spots == LANES - 2, counts[0], kept)
    table[...] = jnp.where(spots == LANES - 1, counts[1], kept)

    for r in turns:
        for k in line.order:
            if not (r in relayed and k == 3):
                along[k, r].wait_recv()
                onward[k, r].start()
                if r in relayed and k == 2:
                    along[3, r].start()
    for r in relayed:
        along[3, r].wait_recv()
        onward[3, r].start()

    def complete(r):
        across[r].wait_recv()
        for k in line.order:
            onward[k, r].wait_recv()

    loads[5].wait()
    complete(rows)
    for b in range(rows):
        complete(b)
        if b < EARLY:

            def store(window, value, b=b):
                scores[b : b + 1, window] = value

            index_row(n, b, gq, giw, kbuf, ends[b], store)
    for copy in loads[6:]:
        copy.wait()
    for group in (across, along, onward):
        for copy in group.values():
            copy.wait_send()


def tiles_of(table, cache, b, g, base, tiles):
    rows, strips, width, strip = cache.shape
    first = lax.axis_index("seq") * (strips * strip // BLOCK)
    lane = lax.broadcasted_iota(jnp.int32, (1, LANES), 1)
    keys, bias = [], []
    for j in range(tiles):
        halves, ends = [], []
        for part in range(2):
            held = base + j < table[b, g, LANES - 2 + part]
            block = table[b, g, part * SLOTS + base + j]
            tile = jnp.where(held, (block - first) // 2, 0)
            halves.append(cache[b, tile])
            live = jnp.minimum(BLOCK, table[b, g, LANES - 3] - block * BLOCK)
            ends.append(part * BLOCK + jnp.where(held, live, 0))
        usable = (lane < ends[0]) | ((lane >= BLOCK) & (lane < ends[1]))
        low, high = halves
        keys.append(jnp.concatenate([low[:, :BLOCK], high[:, BLOCK:]], axis=1))
        bias.append(jnp.where(usable, 0.0, NEG))
    return jnp.concatenate(keys, axis=1), jnp.concatenate(bias, axis=1)


def query_of(gq, b, g, width):
    n, _, heads, _ = gq.shape
    per_group = n // HEAD_GROUPS
    query = gq[pl.ds(g * per_group, per_group), b]
    if heads % 16:
        query = query.astype(jnp.float32)
    return query.reshape(per_group * heads, PACKED)[:, :width].astype(jnp.bfloat16)


def scores_of(query, keys, bias):
    scale = (VALUE_WIDTH + ROTARY_WIDTH) ** (-0.5) * LOG2E
    return jnp.dot(query, keys, preferred_element_type=jnp.float32) * scale + bias


def absorb(state, s, keys):
    top, total, acc = state
    new = jnp.maximum(top, jnp.max(s, axis=1, keepdims=True))
    p = jnp.exp2(s - new)
    keep = jnp.exp2(top - new)
    mixed = lax.dot_general(
        p.astype(jnp.bfloat16),
        keys[:LATENT_WIDTH],
        (((1,), (1,)), ((), ())),
        preferred_element_type=jnp.float32,
    )
    return new, total * keep + jnp.sum(p, axis=1, keepdims=True), acc * keep + mixed


def surplus_kernel(table, gq, cache, accs, norms):
    rows, _, width, _ = cache.shape
    wide = accs.shape[1]
    lane = lax.broadcasted_iota(jnp.int32, (1, LANES), 1)

    @pl.loop(0, rows)
    def _(b):
        for g in range(HEAD_GROUPS):
            tiles = jnp.maximum(table[b, g, LANES - 2], table[b, g, LANES - 1])
            steps = (jnp.maximum(tiles - FIRST, 0) + MORE - 1) // MORE

            def more(c, state, g=g):
                keys, bias = tiles_of(table, cache, b, g, FIRST + c * MORE, MORE)
                return absorb(state, scores_of(query_of(gq, b, g, width), keys, bias), keys)

            start = (
                jnp.full((wide, 1), NEG, jnp.float32),
                jnp.zeros((wide, 1), jnp.float32),
                jnp.zeros((wide, LATENT_WIDTH), jnp.float32),
            )
            top, total, acc = lax.fori_loop(0, steps, more, start)
            accs[b * HEAD_GROUPS + g] = acc
            norms[b * HEAD_GROUPS + g] = jnp.where(lane == 0, top, total)


def attend_kernel(
    n, slots, gq, giw, cache, kbuf, accs, norms, scores_in, attended, scores,
    table, own, sent, from_pair, joint, from_line, lse, lses, share,
    slot_sem, ysend, yrecv, zsend, zrecv, lsend, lrecv,
):
    line = Line(n)
    half, me = line.half, line.me
    _, rows, heads, latent = own.shape
    width = cache.shape[2]
    per_group = n // HEAD_GROUPS
    wide = per_group * heads
    fetch = pltpu.make_async_copy(slots, table, slot_sem.at[0])
    fetch.start()
    entered = line.greet()
    fetch.wait()
    even = line.y == 0
    head = lax.broadcasted_iota(jnp.int32, (wide, LANES), 0)
    spot = lax.broadcasted_iota(jnp.int32, (wide, LANES), 1)
    ring = line.far + [0]

    def told(k, b):
        return push(
            lax.rem(me + k, n), lse.at[b], lses.at[me, b], lsend.at[k, b], lrecv.at[k, b]
        )

    def across(k, b):
        z = line.to(k)
        return push(
            line.partner, sent.at[z, b], from_pair.at[z, b], ysend.at[k, b], yrecv.at[k, b]
        )

    def along(k, b):
        z = line.to(k)
        return push(
            line.device(z), joint.at[z, b], from_line.at[line.z, b],
            zsend.at[k, b], zrecv.at[k, b],
        )

    @pl.loop(0, rows)
    def _(b):
        loaded = []
        for g in range(HEAD_GROUPS):
            keys, bias = tiles_of(table, cache, b, g, 0, FIRST)
            loaded.append((scores_of(query_of(gq, b, g, width), keys, bias), keys))
        lses_now = jnp.zeros((1, LANES), jnp.float32)
        for g, (s, keys) in enumerate(loaded):
            norm = norms[b * HEAD_GROUPS + g]
            state = (norm[:, 0:1], norm[:, 1:2], accs[b * HEAD_GROUPS + g])
            top, total, acc = absorb(state, s, keys)
            acc = (acc * (1.0 / total)).reshape(per_group // 2, 2, heads, latent)
            part = jnp.broadcast_to(top + jnp.log2(total), (wide, LANES))
            part = jnp.where(spot == head + g * wide, part, 0.0)
            lses_now += jnp.sum(part, axis=0, keepdims=True)
            here_z = pl.ds(g * per_group // 2, per_group // 2)
            own[here_z, b] = jnp.where(even, acc[:, 0], acc[:, 1])
            sent[here_z, b] = jnp.where(even, acc[:, 1], acc[:, 0]).astype(jnp.bfloat16)
        lse[b] = lses_now
        lses[me, b] = lses_now

        @pl.when(b == 0)
        def _():
            entered()

        for k in range(1, n):
            told(k, b).start()
        for k in ring:
            across(k, b).start()

    @pl.loop(0, rows)
    def _(b):
        for k in range(1, n):
            told(k, b).wait_recv()
        parts = [lses[s, b] for s in range(n)]
        best = functools.reduce(jnp.maximum, parts)
        whole = functools.reduce(jnp.add, [jnp.exp2(part - best) for part in parts])
        best = best + jnp.log2(whole)
        both = [jnp.exp2(lses[me, b] - best), jnp.exp2(lses[line.partner, b] - best)]
        share[...] = jnp.transpose(jnp.concatenate(both * 4, axis=0))
        for k in ring:
            z = line.to(k)
            target = line.device(z)
            part = share[pl.ds(pl.multiple_of(target * heads, heads), heads)]
            across(k, b).wait_recv()
            value = part[:, 0:1] * own[z, b]
            value += part[:, 1:2] * from_pair[z, b].astype(jnp.float32)
            if k:
                joint[z, b] = value.astype(jnp.bfloat16)
            else:
                own[z, b] = value
        for k in line.far:
            along(k, b).start()

    scores[0:EARLY] = scores_in[...]
    for b in range(EARLY, rows):

        def store(window, value, b=b):
            scores[b : b + 1, window] = value

        index_row(n, b, gq, giw, kbuf, table[b, 0, LANES - 3], store)

    @pl.loop(0, rows)
    def _(b):
        value = own[line.z, b]
        for k in line.far:
            along(k, b).wait_recv()
            value += from_line[line.frm(k), b].astype(jnp.float32)
        attended[b] = value.astype(attended.dtype)

    @pl.loop(0, rows)
    def _(b):
        for k in range(1, n):
            told(k, b).wait_send()
        for k in ring:
            across(k, b).wait_send()
        for k in line.far:
            along(k, b).wait_send()


def project_kernel(attended, weight, scores, out, scores_out, sem):
    copy = pltpu.make_async_copy(scores, scores_out, sem.at[0])
    copy.start()
    rows, heads, latent = attended.shape
    flat = attended[...]
    if heads % 16:
        flat = flat.astype(jnp.float32)
    flat = flat.reshape(rows * heads, latent).astype(jnp.bfloat16)
    which = lax.broadcasted_iota(jnp.int32, (rows * heads, 1), 0) % heads
    y = jnp.zeros((rows * heads, weight.shape[2]), jnp.float32)
    for h in range(heads):
        part = jnp.dot(flat, weight[h], preferred_element_type=jnp.float32)
        y = jnp.where(which == h, part, y)
    out[...] = y.reshape(rows, heads, weight.shape[2]).astype(out.dtype)
    copy.wait()


def on_device(
    n,
    latent_cache,
    index_keys,
    latent_query,
    index_query,
    index_weight,
    value_up_weight,
    selected,
    lengths,
):
    cache, keys, lq = latent_cache[0], index_keys[0], latent_query[0]
    iq, iw, weight, sel = index_query[0], index_weight[0], value_up_weight[0], selected[0]
    rows, span, width = cache.shape
    heads = lq.shape[1]
    half = n // 2
    extra = -iq.shape[1] % 8
    if extra:
        iq = jnp.pad(iq, ((0, 0), (0, extra), (0, 0)))
    vmem = pl.BlockSpec(memory_space=pltpu.VMEM)
    smem = pl.BlockSpec(memory_space=pltpu.SMEM)
    hbm = pl.BlockSpec(memory_space=pl.ANY)
    dma = pltpu.SemaphoreType.DMA

    def far(x):
        return pltpu.with_memory_space_constraint(x, pltpu.HBM)

    def near(x):
        return pltpu.with_memory_space_constraint(x, pltpu.VMEM)

    params = functools.partial(pltpu.CompilerParams, vmem_limit_bytes=16 * MIB)
    gq, giw, cbuf, kbuf, wbuf, table, scores = pl.pallas_call(
        functools.partial(gather_kernel, n),
        out_shape=(
            pltpu.VMEM((n, rows, heads, PACKED), lq.dtype),
            pltpu.VMEM((n,) + iw.shape, iw.dtype),
            pltpu.VMEM((rows, span // STRIP, width, STRIP), cache.dtype),
            pltpu.VMEM(keys.shape, keys.dtype),
            pltpu.VMEM(weight.shape, weight.dtype),
            pltpu.VMEM((rows, HEAD_GROUPS, LANES), jnp.int32),
            pltpu.VMEM((EARLY, span), jnp.float32),
        ),
        in_specs=[hbm] * 8,
        out_specs=(vmem,) * 7,
        scratch_shapes=[
            pltpu.VMEM(lq.shape, lq.dtype),
            pltpu.VMEM(iq.shape, iq.dtype),
            pltpu.VMEM(sel.shape, sel.dtype),
            pltpu.SMEM(lengths.shape, lengths.dtype),
            dma((7 + rows * (span // STRIP),)),
            dma((half, rows + 1)), dma((half, rows + 1)),
            dma((half, rows + 1)), dma((half, rows + 1)),
        ],
        compiler_params=params(collective_id=0, has_side_effects=True),
        name="gather",
    )(
        far(lq), far(iq), far(iw), far(sel), far(lengths),
        far(jnp.swapaxes(cache, 1, 2)), far(keys), far(weight),
    )

    pairs = rows * HEAD_GROUPS
    wide = n // HEAD_GROUPS * heads
    accs, norms = pl.pallas_call(
        surplus_kernel,
        out_shape=(
            pltpu.VMEM((pairs, wide, LATENT_WIDTH), jnp.float32),
            pltpu.VMEM((pairs, wide, LANES), jnp.float32),
        ),
        in_specs=[smem, vmem, vmem],
        out_specs=(vmem,) * 2,
        compiler_params=params(),
        name="surplus",
    )(table, near(gq), near(cbuf))

    parts = (half, rows, heads, LATENT_WIDTH)
    attended, scores = pl.pallas_call(
        functools.partial(attend_kernel, n),
        out_shape=(
            pltpu.VMEM((rows, heads, LATENT_WIDTH), jnp.bfloat16),
            pltpu.VMEM((rows, span), jnp.float32),
        ),
        in_specs=[vmem] * 8,
        out_specs=(vmem, vmem),
        scratch_shapes=[
            pltpu.SMEM(table.shape, table.dtype),
            pltpu.VMEM(parts, jnp.float32),
            pltpu.VMEM(parts, jnp.bfloat16),
            pltpu.VMEM(parts, jnp.bfloat16),
            pltpu.VMEM(parts, jnp.bfloat16),
            pltpu.VMEM(parts, jnp.bfloat16),
            pltpu.VMEM((rows, 1, n * heads), jnp.float32),
            pltpu.VMEM((n, rows, 1, n * heads), jnp.float32),
            pltpu.VMEM((n * heads, 8), jnp.float32),
            dma((1,)),
            dma((half, rows)), dma((half, rows)), dma((half, rows)), dma((half, rows)),
            dma((n, rows)), dma((n, rows)),
        ],
        compiler_params=params(collective_id=1, has_side_effects=True),
        name="attend",
    )(
        near(table), near(gq), near(giw), near(cbuf), near(kbuf),
        near(accs), near(norms), near(scores),
    )

    head_out, index_scores = pl.pallas_call(
        project_kernel,
        out_shape=(
            jax.ShapeDtypeStruct((rows, heads, weight.shape[2]), jnp.bfloat16),
            jax.ShapeDtypeStruct((rows, span), jnp.float32),
        ),
        in_specs=[vmem, vmem, vmem],
        out_specs=(vmem, hbm),
        scratch_shapes=[dma((1,))],
        compiler_params=pltpu.CompilerParams(vmem_limit_bytes=16 * MIB),
        name="project",
    )(near(attended), near(wbuf), near(scores))
    return (index_scores[None], head_out[None])


def solution(mesh):
    return jax.shard_map(
        functools.partial(on_device, mesh.shape["seq"]),
        mesh=mesh,
        in_specs=(
            P("section", "groups", "seq", None),
            P("section", "groups", "seq", None),
            P("section", "groups", "seq", None),
            P("section", "groups", "seq", None),
            P("section", "groups", "seq"),
            P("section", "seq", None, None),
            P("section", "groups", None, None),
            P("groups"),
        ),
        out_specs=(P("section", "groups", "seq"), P("section", "groups", "seq", None)),
        check_vma=False,
    )
```

```python
import functools

import jax
import jax.numpy as jnp
from jax import lax
from jax.experimental import pallas as pl
from jax.experimental.pallas import tpu as pltpu
from jax.sharding import PartitionSpec as P

LATENT_WIDTH = 512
ROTARY_WIDTH = 64
VALUE_WIDTH = 128
IDX_DIM = 128
BLOCK = 64
HEAD_GROUPS = 2
NEG = -1e30
LOG2E = 1.4426950408889634
FIRST = 4
MORE = 2
STRIP = 128
SLOTS = 62
LANES = 128
PACKED = LATENT_WIDTH + LANES
MIB = 1024 * 1024
MESH = pl.DeviceIdType.MESH


class Line:
    def __init__(self, n):
        self.half = n // 2
        self.me = lax.axis_index("seq")
        self.z = lax.div(self.me, 2)
        self.y = lax.rem(self.me, 2)
        self.partner = self.me + 1 - 2 * self.y
        self.order = list(range(1, self.half))
        self.far = sorted(self.order, key=lambda k: (-k.bit_length(), k))

    def step(self, k, sign):
        if self.half & (self.half - 1):
            return lax.rem(self.z + sign * k + self.half, self.half)
        out = self.z
        for j in range(k.bit_length()):
            if k >> j & 1:
                bit = lax.rem(lax.div(self.z, 1 << j), 2)
                out = out + (1 - 2 * bit) * (1 << j)
        return out

    def to(self, k):
        return self.step(k, 1)

    def frm(self, k):
        return self.step(k, -1)

    def device(self, z):
        return 2 * z + self.y

    def opposite(self, z):
        return 2 * z + 1 - self.y

    def greet(self):
        barrier = pltpu.get_barrier_semaphore()
        n = 2 * self.half
        for k in range(1, n):
            peer = lax.rem(self.me + k, n)
            pl.semaphore_signal(
                barrier, inc=1, device_id={"seq": peer}, device_id_type=MESH
            )
        return lambda: pl.semaphore_wait(barrier, n - 1)


def push(peer, src, dst, send_sem, recv_sem):
    return pltpu.make_async_remote_copy(
        src_ref=src,
        dst_ref=dst,
        send_sem=send_sem,
        recv_sem=recv_sem,
        device_id={"seq": peer},
        device_id_type=MESH,
    )


def index_row(n, b, gq, giw, kbuf, length, store):
    me = lax.axis_index("seq")
    heads, held, span = gq.shape[2], giw.shape[2], kbuf.shape[1]
    tile = min(512, span)
    group = 8
    lane = lax.broadcasted_iota(jnp.int32, (1, tile), 1)
    diagonal = (
        lax.broadcasted_iota(jnp.int32, (n * group, held), 0) % group
        == lax.broadcasted_iota(jnp.int32, (n * group, held), 1)
    )
    low = lax.broadcasted_iota(jnp.int32, (n * group, LANES), 1) < LANES // 2
    packed = gq[:, b, :, LATENT_WIDTH:PACKED].astype(jnp.float32)
    if heads == 2 * group:
        left = packed[:, :group].reshape(n * group, LANES)
        right = packed[:, group:].reshape(n * group, LANES)
    else:
        left = packed.reshape(n * group, LANES)
        right = pltpu.roll(left, n * group - held, 0)
    query = jnp.where(low, pltpu.roll(left, LANES // 2, 1), right)
    query = query.astype(jnp.bfloat16)
    weight = giw[:, b : b + 1].astype(jnp.float32)
    weight = jnp.broadcast_to(weight, (n, group, held)).reshape(n * group, held)
    weight = jnp.sum(jnp.where(diagonal, weight, 0.0), axis=1, keepdims=True)
    weight = jnp.broadcast_to(weight * IDX_DIM ** (-0.5), (n * group, LANES))

    def step(c, carry):
        start = pl.multiple_of(c * tile, tile)
        dots = lax.dot_general(
            query,
            kbuf[b, pl.ds(start, tile), :],
            (((1,), (1,)), ((), ())),
            preferred_element_type=jnp.float32,
        )
        pieces = []
        for j in range(tile // LANES):
            part = jnp.maximum(dots[:, j * LANES : (j + 1) * LANES], 0.0) * weight
            pieces.append(jnp.sum(part, axis=0, keepdims=True))
        total = jnp.concatenate(pieces, axis=1)
        live = me * span + c * tile + lane < length
        store(pl.ds(start, tile), jnp.where(live, total, 0.0))
        return carry

    lax.fori_loop(0, span // tile, step, 0)


def gather_kernel(
    n, lq, iq, iw, sel, lens, cache, gq, giw, cbuf, table,
    lqs, iqs, sels, ends, load_sem, zsend, zrecv, ysend, yrecv,
):
    line = Line(n)
    me = line.me
    rows, heads, width = lqs.shape
    held = iw.shape[1]
    loads = [
        pltpu.make_async_copy(lq, lqs, load_sem.at[0]),
        pltpu.make_async_copy(iq, iqs, load_sem.at[1]),
        pltpu.make_async_copy(iw, giw.at[me], load_sem.at[2]),
        pltpu.make_async_copy(sel, sels, load_sem.at[3]),
        pltpu.make_async_copy(lens, ends, load_sem.at[4]),
    ]
    strips = cbuf.shape[1]
    for b in range(rows):
        for j in range(strips):
            loads.append(
                pltpu.make_async_copy(
                    cache.at[b, :, pl.ds(j * STRIP, STRIP)],
                    cbuf.at[b, j],
                    load_sem.at[5 + b * strips + j],
                )
            )
    for copy in loads[:5]:
        copy.start()
    entered = line.greet()
    for copy in loads[:3]:
        copy.wait()

    lane = lax.broadcasted_iota(jnp.int32, (iqs.shape[1], LANES), 1)
    row = lax.broadcasted_iota(jnp.int32, (iqs.shape[1], LANES), 0)
    for b in range(rows):
        mine = iqs[b].astype(jnp.float32)
        turned = pltpu.roll(mine, LANES // 2, 1)
        if heads == 2 * iqs.shape[1]:
            spare = jnp.concatenate([turned, mine], axis=0)
        else:
            spare = jnp.where(row < held, turned, pltpu.roll(mine, held, 0))
        gq[me, b, :, 0:LATENT_WIDTH] = lqs[b, :, 0:LATENT_WIDTH]
        gq[me, b, :, LATENT_WIDTH:width] = lqs[b, :, LATENT_WIDTH:width]
        spare = spare.astype(jnp.bfloat16)
        gq[me, b, :, width:PACKED] = spare[:, width - LATENT_WIDTH :]
    entered()

    def piece(owner, r):
        return gq.at[owner, r] if r < rows else giw.at[owner]

    relayed = (0,) if line.half == 4 else ()
    turns = [0, rows] + list(range(1, rows))
    across, along, onward, relay = {}, {}, {}, {}
    for r in turns:
        ref = piece(me, r)
        across[r] = push(line.partner, ref, ref, ysend.at[0, r], yrecv.at[0, r])
        for k in line.order:
            ref = piece(me, r)
            if r in relayed and k == 3:
                ref = piece(line.device(line.frm(2)), r)
                target = line.device(line.to(1))
            else:
                target = line.device(line.to(k))
            along[k, r] = push(target, ref, ref, zsend.at[k, r], zrecv.at[k, r])
            ref = piece(line.device(line.frm(k)), r)
            onward[k, r] = push(line.partner, ref, ref, ysend.at[k, r], yrecv.at[k, r])
    for r in turns:
        across[r].start()
    for r in turns:
        for k in line.order:
            if not (r in relayed and k == 3):
                along[k, r].start()
    for copy in loads[5:]:
        copy.start()

    for copy in loads[3:5]:
        copy.wait()
    here = strips * STRIP // BLOCK
    first = me * here
    chosen = sels[...]
    spots = lax.broadcasted_iota(jnp.int32, table.shape, 2)
    which = lax.broadcasted_iota(jnp.int32, table.shape, 0)
    kept = jnp.zeros(table.shape, jnp.int32)
    counts = [jnp.zeros(table.shape, jnp.int32)] * 2
    for i in range(sels.shape[2]):
        block = jnp.broadcast_to(chosen[:, :, i : i + 1], table.shape)
        mine = (block >= first) & (block < first + here)
        odd = block & 1
        for part in range(2):
            take = mine & (odd == part)
            kept = jnp.where(take & (spots == part * SLOTS + counts[part]), block, kept)
            counts[part] = counts[part] + jnp.where(take, 1, 0)
    for b in range(rows):
        kept = jnp.where((spots == LANES - 3) & (which == b), ends[b], kept)
    kept = jnp.where(spots == LANES - 2, counts[0], kept)
    table[...] = jnp.where(spots == LANES - 1, counts[1], kept)

    for r in turns:
        for k in line.order:
            if not (r in relayed and k == 3):
                along[k, r].wait_recv()
                onward[k, r].start()
                if r in relayed and k == 2:
                    along[3, r].start()
    for r in relayed:
        along[3, r].wait_recv()
        onward[3, r].start()

    def complete(r):
        across[r].wait_recv()
        for k in line.order:
            onward[k, r].wait_recv()

    for r in turns:
        complete(r)
    for copy in loads[5:]:
        copy.wait()
    for group in (across, along, onward):
        for copy in group.values():
            copy.wait_send()


def tiles_of(table, cache, b, g, base, tiles):
    rows, strips, width, strip = cache.shape
    first = lax.axis_index("seq") * (strips * strip // BLOCK)
    lane = lax.broadcasted_iota(jnp.int32, (1, LANES), 1)
    keys, bias = [], []
    for j in range(tiles):
        halves, ends = [], []
        for part in range(2):
            held = base + j < table[b, g, LANES - 2 + part]
            block = table[b, g, part * SLOTS + base + j]
            tile = jnp.where(held, (block - first) // 2, 0)
            halves.append(cache[b, tile])
            live = jnp.minimum(BLOCK, table[b, g, LANES - 3] - block * BLOCK)
            ends.append(part * BLOCK + jnp.where(held, live, 0))
        usable = (lane < ends[0]) | ((lane >= BLOCK) & (lane < ends[1]))
        low, high = halves
        keys.append(jnp.concatenate([low[:, :BLOCK], high[:, BLOCK:]], axis=1))
        bias.append(jnp.where(usable, 0.0, NEG))
    return jnp.concatenate(keys, axis=1), jnp.concatenate(bias, axis=1)


def query_of(gq, b, g, width):
    n, _, heads, _ = gq.shape
    per_group = n // HEAD_GROUPS
    query = gq[pl.ds(g * per_group, per_group), b]
    if heads % 16:
        query = query.astype(jnp.float32)
    return query.reshape(per_group * heads, PACKED)[:, :width].astype(jnp.bfloat16)


def scores_of(query, keys, bias):
    scale = (VALUE_WIDTH + ROTARY_WIDTH) ** (-0.5) * LOG2E
    return jnp.dot(query, keys, preferred_element_type=jnp.float32) * scale + bias


def absorb(state, s, keys):
    new = jnp.max(s, axis=1, keepdims=True)
    if state is not None:
        new = jnp.maximum(state[0], new)
    p = jnp.exp2(s - new)
    mixed = lax.dot_general(
        p.astype(jnp.bfloat16),
        keys[:LATENT_WIDTH],
        (((1,), (1,)), ((), ())),
        preferred_element_type=jnp.float32,
    )
    whole = jnp.sum(p, axis=1, keepdims=True)
    if state is None:
        return new, whole, mixed
    top, total, acc = state
    keep = jnp.exp2(top - new)
    return new, total * keep + whole, acc * keep + mixed


def surplus_kernel(table, gq, cache, accs, norms):
    rows, _, width, _ = cache.shape
    wide = accs.shape[1]

    @pl.loop(0, rows)
    def _(b):
        for g in range(HEAD_GROUPS):
            tiles = jnp.maximum(table[b, g, LANES - 2], table[b, g, LANES - 1])
            steps = (jnp.maximum(tiles - FIRST, 0) + MORE - 1) // MORE

            def more(c, state, g=g):
                keys, bias = tiles_of(table, cache, b, g, FIRST + c * MORE, MORE)
                return absorb(state, scores_of(query_of(gq, b, g, width), keys, bias), keys)

            start = (
                jnp.full((wide, 1), NEG, jnp.float32),
                jnp.zeros((wide, 1), jnp.float32),
                jnp.zeros((wide, LATENT_WIDTH), jnp.float32),
            )
            top, total, acc = lax.fori_loop(0, steps, more, start)
            accs[b * HEAD_GROUPS + g] = acc
            norms[b * HEAD_GROUPS + g, 0] = jnp.broadcast_to(top, (wide, LANES))
            norms[b * HEAD_GROUPS + g, 1] = jnp.broadcast_to(total, (wide, LANES))


def attend_kernel(
    n, slots, gq, giw, cache, accs, norms, keys, weight, attended, scores, wbuf,
    kbuf, table, own, sent, from_pair, joint, from_line, lse, lses, share,
    slot_sem, ysend, yrecv, zsend, zrecv, lsend, lrecv,
):
    line = Line(n)
    half, me = line.half, line.me
    _, rows, heads, latent = own.shape
    width = cache.shape[2]
    per_group = n // HEAD_GROUPS
    wide = per_group * heads
    fetch = pltpu.make_async_copy(slots, table, slot_sem.at[0])
    key_load = pltpu.make_async_copy(keys, kbuf, slot_sem.at[1])
    weight_load = pltpu.make_async_copy(weight, wbuf, slot_sem.at[2])
    fetch.start()
    entered = line.greet()
    key_load.start()
    weight_load.start()
    fetch.wait()
    even = line.y == 0
    head = lax.broadcasted_iota(jnp.int32, (wide, LANES), 0)
    spot = lax.broadcasted_iota(jnp.int32, (wide, LANES), 1)
    ring = line.far + [0]

    def told(k, b):
        return push(
            lax.rem(me + k, n), lse.at[b], lses.at[me, b], lsend.at[k, b], lrecv.at[k, b]
        )

    def across(k, b):
        z = line.to(k)
        return push(
            line.partner, sent.at[z, b], from_pair.at[z, b], ysend.at[k, b], yrecv.at[k, b]
        )

    def along(k, b):
        z = line.to(k)
        return push(
            line.device(z), joint.at[z, b], from_line.at[line.z, b],
            zsend.at[k, b], zrecv.at[k, b],
        )

    @pl.loop(0, rows)
    def _(b):
        loaded = []
        for g in range(HEAD_GROUPS):
            keys, bias = tiles_of(table, cache, b, g, 0, FIRST)
            loaded.append((scores_of(query_of(gq, b, g, width), keys, bias), keys))
        lses_now = jnp.zeros((1, LANES), jnp.float32)
        for g, (s, keys) in enumerate(loaded):
            rg = b * HEAD_GROUPS + g
            top, total, acc = absorb(None, s, keys)
            top = jnp.broadcast_to(top, (wide, LANES))
            best = jnp.maximum(top, norms[rg, 0])
            grown, added = jnp.exp2(top - best), jnp.exp2(norms[rg, 0] - best)
            total = grown * total + added * norms[rg, 1]
            scaled = 1.0 / total
            grown, added = grown * scaled, added * scaled
            acc = jnp.concatenate(
                [
                    acc[:, j : j + LANES] * grown + accs[rg, :, j : j + LANES] * added
                    for j in range(0, latent, LANES)
                ],
                axis=1,
            ).reshape(per_group // 2, 2, heads, latent)
            part = best + jnp.log2(total)
            part = jnp.where(spot == head + g * wide, part, 0.0)
            lses_now += jnp.sum(part, axis=0, keepdims=True)
            here_z = pl.ds(g * per_group // 2, per_group // 2)
            own[here_z, b] = jnp.where(even, acc[:, 0], acc[:, 1])
            sent[here_z, b] = jnp.where(even, acc[:, 1], acc[:, 0]).astype(jnp.bfloat16)
        lse[b] = lses_now
        lses[me, b] = lses_now

        @pl.when(b == 0)
        def _():
            entered()

        for k in range(1, n):
            told(k, b).start()
        for k in ring:
            across(k, b).start()

    def combine(b):
        for k in range(1, n):
            told(k, b).wait_recv()
        parts = [lses[s, b] for s in range(n)]
        best = functools.reduce(jnp.maximum, parts)
        whole = functools.reduce(jnp.add, [jnp.exp2(part - best) for part in parts])
        best = best + jnp.log2(whole)
        both = [jnp.exp2(lses[me, b] - best), jnp.exp2(lses[line.partner, b] - best)]
        share[...] = jnp.transpose(jnp.concatenate(both * 4, axis=0))
        for k in ring:
            z = line.to(k)
            target = line.device(z)
            part = share[pl.ds(pl.multiple_of(target * heads, heads), heads)]
            across(k, b).wait_recv()
            value = part[:, 0:1] * own[z, b]
            value += part[:, 1:2] * from_pair[z, b].astype(jnp.float32)
            if k:
                joint[z, b] = value.astype(jnp.bfloat16)
            else:
                own[z, b] = value
        for k in line.far:
            along(k, b).start()

    def index(b):
        def store(window, value):
            scores[b : b + 1, window] = value

        index_row(n, b, gq, giw, kbuf, table[b, 0, LANES - 3], store)

    key_load.wait()
    index(0)
    for b in range(rows // 2):
        combine(b)
    for b in range(1, rows // 2):
        index(b)
    for b in range(rows // 2, rows):
        combine(b)
    for b in range(rows // 2, rows):
        index(b)

    @pl.loop(0, rows)
    def _(b):
        value = own[line.z, b]
        for k in line.far:
            along(k, b).wait_recv()
            value += from_line[line.frm(k), b].astype(jnp.float32)
        attended[b] = value.astype(attended.dtype)

    @pl.loop(0, rows)
    def _(b):
        for k in range(1, n):
            told(k, b).wait_send()
        for k in ring:
            across(k, b).wait_send()
        for k in line.far:
            along(k, b).wait_send()
    weight_load.wait()


def project_kernel(attended, weight, scores, out, scores_out, sem):
    copy = pltpu.make_async_copy(scores, scores_out, sem.at[0])
    copy.start()
    rows, heads, latent = attended.shape
    flat = attended[...]
    if heads % 16:
        flat = flat.astype(jnp.float32)
    flat = flat.reshape(rows * heads, latent).astype(jnp.bfloat16)
    which = lax.broadcasted_iota(jnp.int32, (rows * heads, 1), 0) % heads
    y = jnp.zeros((rows * heads, weight.shape[2]), jnp.float32)
    for h in range(heads):
        part = jnp.dot(flat, weight[h], preferred_element_type=jnp.float32)
        y = jnp.where(which == h, part, y)
    out[...] = y.reshape(rows, heads, weight.shape[2]).astype(out.dtype)
    copy.wait()


def on_device(
    n,
    latent_cache,
    index_keys,
    latent_query,
    index_query,
    index_weight,
    value_up_weight,
    selected,
    lengths,
):
    cache, keys, lq = latent_cache[0], index_keys[0], latent_query[0]
    iq, iw, weight, sel = index_query[0], index_weight[0], value_up_weight[0], selected[0]
    rows, span, width = cache.shape
    heads = lq.shape[1]
    half = n // 2
    extra = -iq.shape[1] % 8
    if extra:
        iq = jnp.pad(iq, ((0, 0), (0, extra), (0, 0)))
    vmem = pl.BlockSpec(memory_space=pltpu.VMEM)
    smem = pl.BlockSpec(memory_space=pltpu.SMEM)
    hbm = pl.BlockSpec(memory_space=pl.ANY)
    dma = pltpu.SemaphoreType.DMA

    def far(x):
        return pltpu.with_memory_space_constraint(x, pltpu.HBM)

    def near(x):
        return pltpu.with_memory_space_constraint(x, pltpu.VMEM)

    params = functools.partial(pltpu.CompilerParams, vmem_limit_bytes=16 * MIB)
    gq, giw, cbuf, table = pl.pallas_call(
        functools.partial(gather_kernel, n),
        out_shape=(
            pltpu.VMEM((n, rows, heads, PACKED), lq.dtype),
            pltpu.VMEM((n,) + iw.shape, iw.dtype),
            pltpu.VMEM((rows, span // STRIP, width, STRIP), cache.dtype),
            pltpu.VMEM((rows, HEAD_GROUPS, LANES), jnp.int32),
        ),
        in_specs=[hbm] * 6,
        out_specs=(vmem,) * 4,
        scratch_shapes=[
            pltpu.VMEM(lq.shape, lq.dtype),
            pltpu.VMEM(iq.shape, iq.dtype),
            pltpu.VMEM(sel.shape, sel.dtype),
            pltpu.SMEM(lengths.shape, lengths.dtype),
            dma((5 + rows * (span // STRIP),)),
            dma((half, rows + 1)), dma((half, rows + 1)),
            dma((half, rows + 1)), dma((half, rows + 1)),
        ],
        compiler_params=params(collective_id=0, has_side_effects=True),
        name="gather",
    )(
        far(lq), far(iq), far(iw), far(sel), far(lengths),
        far(jnp.swapaxes(cache, 1, 2)),
    )

    pairs = rows * HEAD_GROUPS
    wide = n // HEAD_GROUPS * heads
    accs, norms = pl.pallas_call(
        surplus_kernel,
        out_shape=(
            pltpu.VMEM((pairs, wide, LATENT_WIDTH), jnp.float32),
            pltpu.VMEM((pairs, 2, wide, LANES), jnp.float32),
        ),
        in_specs=[smem, vmem, vmem],
        out_specs=(vmem,) * 2,
        compiler_params=params(),
        name="surplus",
    )(table, near(gq), near(cbuf))

    parts = (half, rows, heads, LATENT_WIDTH)
    attended, scores, wbuf = pl.pallas_call(
        functools.partial(attend_kernel, n),
        out_shape=(
            pltpu.VMEM((rows, heads, LATENT_WIDTH), jnp.bfloat16),
            pltpu.VMEM((rows, span), jnp.float32),
            pltpu.VMEM(weight.shape, weight.dtype),
        ),
        in_specs=[vmem] * 6 + [hbm] * 2,
        out_specs=(vmem,) * 3,
        scratch_shapes=[
            pltpu.VMEM(keys.shape, keys.dtype),
            pltpu.SMEM(table.shape, table.dtype),
            pltpu.VMEM(parts, jnp.float32),
            pltpu.VMEM(parts, jnp.bfloat16),
            pltpu.VMEM(parts, jnp.bfloat16),
            pltpu.VMEM(parts, jnp.bfloat16),
            pltpu.VMEM(parts, jnp.bfloat16),
            pltpu.VMEM((rows, 1, n * heads), jnp.float32),
            pltpu.VMEM((n, rows, 1, n * heads), jnp.float32),
            pltpu.VMEM((n * heads, 8), jnp.float32),
            dma((3,)),
            dma((half, rows)), dma((half, rows)), dma((half, rows)), dma((half, rows)),
            dma((n, rows)), dma((n, rows)),
        ],
        compiler_params=params(collective_id=1, has_side_effects=True),
        name="attend",
    )(
        near(table), near(gq), near(giw), near(cbuf), near(accs), near(norms),
        far(keys), far(weight),
    )

    head_out, index_scores = pl.pallas_call(
        project_kernel,
        out_shape=(
            jax.ShapeDtypeStruct((rows, heads, weight.shape[2]), jnp.bfloat16),
            jax.ShapeDtypeStruct((rows, span), jnp.float32),
        ),
        in_specs=[vmem, vmem, vmem],
        out_specs=(vmem, hbm),
        scratch_shapes=[dma((1,))],
        compiler_params=pltpu.CompilerParams(vmem_limit_bytes=16 * MIB),
        name="project",
    )(near(attended), near(wbuf), near(scores))
    return (index_scores[None], head_out[None])


def solution(mesh):
    return jax.shard_map(
        functools.partial(on_device, mesh.shape["seq"]),
        mesh=mesh,
        in_specs=(
            P("section", "groups", "seq", None),
            P("section", "groups", "seq", None),
            P("section", "groups", "seq", None),
            P("section", "groups", "seq", None),
            P("section", "groups", "seq"),
            P("section", "seq", None, None),
            P("section", "groups", None, None),
            P("groups"),
        ),
        out_specs=(P("section", "groups", "seq"), P("section", "groups", "seq", None)),
        check_vma=False,
    )
```

```python
import functools

import jax
import jax.numpy as jnp
from jax import lax
from jax.experimental import pallas as pl
from jax.experimental.pallas import tpu as pltpu
from jax.sharding import PartitionSpec as P

LATENT_WIDTH = 512
ROTARY_WIDTH = 64
VALUE_WIDTH = 128
IDX_DIM = 128
BLOCK = 64
HEAD_GROUPS = 2
NEG = -1e30
LOG2E = 1.4426950408889634
FIRST = 5
MORE = 2
STRIP = 128
SLOTS = 62
LANES = 128
PACKED = LATENT_WIDTH + LANES
MIB = 1024 * 1024
MESH = pl.DeviceIdType.MESH


class Line:
    def __init__(self, n):
        self.half = n // 2
        self.me = lax.axis_index("seq")
        self.z = lax.div(self.me, 2)
        self.y = lax.rem(self.me, 2)
        self.partner = self.me + 1 - 2 * self.y
        self.order = list(range(1, self.half))
        self.far = sorted(self.order, key=lambda k: (-k.bit_length(), k))

    def step(self, k, sign):
        if self.half & (self.half - 1):
            return lax.rem(self.z + sign * k + self.half, self.half)
        out = self.z
        for j in range(k.bit_length()):
            if k >> j & 1:
                bit = lax.rem(lax.div(self.z, 1 << j), 2)
                out = out + (1 - 2 * bit) * (1 << j)
        return out

    def to(self, k):
        return self.step(k, 1)

    def frm(self, k):
        return self.step(k, -1)

    def device(self, z):
        return 2 * z + self.y

    def opposite(self, z):
        return 2 * z + 1 - self.y

    def greet(self):
        barrier = pltpu.get_barrier_semaphore()
        n = 2 * self.half
        for k in range(1, n):
            peer = lax.rem(self.me + k, n)
            pl.semaphore_signal(
                barrier, inc=1, device_id={"seq": peer}, device_id_type=MESH
            )
        return lambda: pl.semaphore_wait(barrier, n - 1)


def push(peer, src, dst, send_sem, recv_sem):
    return pltpu.make_async_remote_copy(
        src_ref=src,
        dst_ref=dst,
        send_sem=send_sem,
        recv_sem=recv_sem,
        device_id={"seq": peer},
        device_id_type=MESH,
    )


def index_row(n, b, gq, giw, kbuf, length, store):
    me = lax.axis_index("seq")
    heads, held, span = gq.shape[2], giw.shape[2], kbuf.shape[1]
    tile = min(512, span)
    group = 8
    lane = lax.broadcasted_iota(jnp.int32, (1, tile), 1)
    diagonal = (
        lax.broadcasted_iota(jnp.int32, (n * group, held), 0) % group
        == lax.broadcasted_iota(jnp.int32, (n * group, held), 1)
    )
    low = lax.broadcasted_iota(jnp.int32, (n * group, LANES), 1) < LANES // 2
    packed = gq[:, b, :, LATENT_WIDTH:PACKED].astype(jnp.float32)
    if heads == 2 * group:
        left = packed[:, :group].reshape(n * group, LANES)
        right = packed[:, group:].reshape(n * group, LANES)
    else:
        left = packed.reshape(n * group, LANES)
        right = pltpu.roll(left, n * group - held, 0)
    query = jnp.where(low, pltpu.roll(left, LANES // 2, 1), right)
    query = query.astype(jnp.bfloat16)
    weight = giw[:, b : b + 1].astype(jnp.float32)
    weight = jnp.broadcast_to(weight, (n, group, held)).reshape(n * group, held)
    weight = jnp.sum(jnp.where(diagonal, weight, 0.0), axis=1, keepdims=True)
    weight = jnp.broadcast_to(weight * IDX_DIM ** (-0.5), (n * group, LANES))

    def step(c, carry):
        start = pl.multiple_of(c * tile, tile)
        dots = lax.dot_general(
            query,
            kbuf[b, pl.ds(start, tile), :],
            (((1,), (1,)), ((), ())),
            preferred_element_type=jnp.float32,
        )
        pieces = []
        for j in range(tile // LANES):
            part = jnp.maximum(dots[:, j * LANES : (j + 1) * LANES], 0.0) * weight
            pieces.append(jnp.sum(part, axis=0, keepdims=True))
        total = jnp.concatenate(pieces, axis=1)
        live = me * span + c * tile + lane < length
        store(pl.ds(start, tile), jnp.where(live, total, 0.0))
        return carry

    lax.fori_loop(0, span // tile, step, 0)


def gather_kernel(
    n, lq, iq, iw, sel, lens, cache, gq, giw, cbuf, table,
    lqs, iqs, sels, ends, load_sem, zsend, zrecv, ysend, yrecv,
):
    line = Line(n)
    me = line.me
    rows, heads, width = lqs.shape
    held = iw.shape[1]
    loads = [
        pltpu.make_async_copy(lq, lqs, load_sem.at[0]),
        pltpu.make_async_copy(iq, iqs, load_sem.at[1]),
        pltpu.make_async_copy(iw, giw.at[me], load_sem.at[2]),
        pltpu.make_async_copy(sel, sels, load_sem.at[3]),
        pltpu.make_async_copy(lens, ends, load_sem.at[4]),
    ]
    strips = cbuf.shape[1]
    for b in range(rows):
        for j in range(strips):
            loads.append(
                pltpu.make_async_copy(
                    cache.at[b, :, pl.ds(j * STRIP, STRIP)],
                    cbuf.at[b, j],
                    load_sem.at[5 + b * strips + j],
                )
            )
    for copy in loads[:5]:
        copy.start()
    entered = line.greet()
    for copy in loads[:3]:
        copy.wait()

    lane = lax.broadcasted_iota(jnp.int32, (iqs.shape[1], LANES), 1)
    row = lax.broadcasted_iota(jnp.int32, (iqs.shape[1], LANES), 0)
    for b in range(rows):
        mine = iqs[b].astype(jnp.float32)
        turned = pltpu.roll(mine, LANES // 2, 1)
        if heads == 2 * iqs.shape[1]:
            spare = jnp.concatenate([turned, mine], axis=0)
        else:
            spare = jnp.where(row < held, turned, pltpu.roll(mine, held, 0))
        gq[me, b, :, 0:LATENT_WIDTH] = lqs[b, :, 0:LATENT_WIDTH]
        gq[me, b, :, LATENT_WIDTH:width] = lqs[b, :, LATENT_WIDTH:width]
        spare = spare.astype(jnp.bfloat16)
        gq[me, b, :, width:PACKED] = spare[:, width - LATENT_WIDTH :]
    entered()

    def piece(owner, r):
        return gq.at[owner, r] if r < rows else giw.at[owner]

    relayed = (0, 1) if line.half == 4 else ()
    turns = [0, rows] + list(range(1, rows))
    across, along, onward, relay = {}, {}, {}, {}
    for r in turns:
        ref = piece(me, r)
        across[r] = push(line.partner, ref, ref, ysend.at[0, r], yrecv.at[0, r])
        for k in line.order:
            ref = piece(me, r)
            if r in relayed and k == 3:
                ref = piece(line.device(line.frm(2)), r)
                target = line.device(line.to(1))
            else:
                target = line.device(line.to(k))
            along[k, r] = push(target, ref, ref, zsend.at[k, r], zrecv.at[k, r])
            ref = piece(line.device(line.frm(k)), r)
            onward[k, r] = push(line.partner, ref, ref, ysend.at[k, r], yrecv.at[k, r])
    for r in turns:
        across[r].start()
    for r in turns:
        for k in line.order:
            if not (r in relayed and k == 3):
                along[k, r].start()
    for copy in loads[5:]:
        copy.start()

    for copy in loads[3:5]:
        copy.wait()
    here = strips * STRIP // BLOCK
    first = me * here
    chosen = sels[...]
    spots = lax.broadcasted_iota(jnp.int32, table.shape, 2)
    which = lax.broadcasted_iota(jnp.int32, table.shape, 0)
    kept = jnp.zeros(table.shape, jnp.int32)
    counts = [jnp.zeros(table.shape, jnp.int32)] * 2
    for i in range(sels.shape[2]):
        block = jnp.broadcast_to(chosen[:, :, i : i + 1], table.shape)
        mine = (block >= first) & (block < first + here)
        odd = block & 1
        for part in range(2):
            take = mine & (odd == part)
            kept = jnp.where(take & (spots == part * SLOTS + counts[part]), block, kept)
            counts[part] = counts[part] + jnp.where(take, 1, 0)
    for b in range(rows):
        kept = jnp.where((spots == LANES - 3) & (which == b), ends[b], kept)
    kept = jnp.where(spots == LANES - 2, counts[0], kept)
    table[...] = jnp.where(spots == LANES - 1, counts[1], kept)

    for r in turns:
        for k in line.order:
            if not (r in relayed and k == 3):
                along[k, r].wait_recv()
                onward[k, r].start()
                if r in relayed and k == 2:
                    along[3, r].start()
    for r in relayed:
        along[3, r].wait_recv()
        onward[3, r].start()

    def complete(r):
        across[r].wait_recv()
        for k in line.order:
            onward[k, r].wait_recv()

    for r in turns:
        complete(r)
    for copy in loads[5:]:
        copy.wait()
    for group in (across, along, onward):
        for copy in group.values():
            copy.wait_send()


def tiles_of(table, cache, b, g, base, tiles):
    rows, strips, width, strip = cache.shape
    first = lax.axis_index("seq") * (strips * strip // BLOCK)
    lane = lax.broadcasted_iota(jnp.int32, (1, LANES), 1)
    keys, bias = [], []
    for j in range(tiles):
        halves, ends = [], []
        for part in range(2):
            held = base + j < table[b, g, LANES - 2 + part]
            block = table[b, g, part * SLOTS + base + j]
            tile = jnp.where(held, (block - first) // 2, 0)
            halves.append(cache[b, tile])
            live = jnp.minimum(BLOCK, table[b, g, LANES - 3] - block * BLOCK)
            ends.append(part * BLOCK + jnp.where(held, live, 0))
        usable = (lane < ends[0]) | ((lane >= BLOCK) & (lane < ends[1]))
        low, high = halves
        keys.append(jnp.concatenate([low[:, :BLOCK], high[:, BLOCK:]], axis=1))
        bias.append(jnp.where(usable, 0.0, NEG))
    return jnp.concatenate(keys, axis=1), jnp.concatenate(bias, axis=1)


def query_of(gq, b, g, width):
    n, _, heads, _ = gq.shape
    per_group = n // HEAD_GROUPS
    query = gq[pl.ds(g * per_group, per_group), b]
    if heads % 16:
        query = query.astype(jnp.float32)
    return query.reshape(per_group * heads, PACKED)[:, :width].astype(jnp.bfloat16)


def scores_of(query, keys, bias):
    scale = (VALUE_WIDTH + ROTARY_WIDTH) ** (-0.5) * LOG2E
    return jnp.dot(query, keys, preferred_element_type=jnp.float32) * scale + bias


def absorb(state, s, keys):
    new = jnp.max(s, axis=1, keepdims=True)
    if state is not None:
        new = jnp.maximum(state[0], new)
    p = jnp.exp2(s - new)
    mixed = lax.dot_general(
        p.astype(jnp.bfloat16),
        keys[:LATENT_WIDTH],
        (((1,), (1,)), ((), ())),
        preferred_element_type=jnp.float32,
    )
    whole = jnp.sum(p, axis=1, keepdims=True)
    if state is None:
        return new, whole, mixed
    top, total, acc = state
    keep = jnp.exp2(top - new)
    return new, total * keep + whole, acc * keep + mixed


def surplus_kernel(table, gq, cache, accs, norms):
    rows, _, width, _ = cache.shape
    wide = accs.shape[1]

    @pl.loop(0, rows)
    def _(b):
        for g in range(HEAD_GROUPS):
            tiles = jnp.maximum(table[b, g, LANES - 2], table[b, g, LANES - 1])
            steps = (jnp.maximum(tiles - FIRST, 0) + MORE - 1) // MORE

            def more(c, state, g=g):
                keys, bias = tiles_of(table, cache, b, g, FIRST + c * MORE, MORE)
                return absorb(state, scores_of(query_of(gq, b, g, width), keys, bias), keys)

            start = (
                jnp.full((wide, 1), NEG, jnp.float32),
                jnp.zeros((wide, 1), jnp.float32),
                jnp.zeros((wide, LATENT_WIDTH), jnp.float32),
            )
            top, total, acc = lax.fori_loop(0, steps, more, start)
            accs[b * HEAD_GROUPS + g] = acc
            norms[b * HEAD_GROUPS + g, 0] = jnp.broadcast_to(top, (wide, LANES))
            norms[b * HEAD_GROUPS + g, 1] = jnp.broadcast_to(total, (wide, LANES))


def attend_kernel(
    n, slots, gq, giw, cache, accs, norms, keys, weight, attended, scores, wbuf,
    kbuf, table, own, sent, from_pair, joint, from_line, lse, lses, share,
    slot_sem, ysend, yrecv, zsend, zrecv, lsend, lrecv,
):
    line = Line(n)
    half, me = line.half, line.me
    _, rows, heads, latent = own.shape
    width = cache.shape[2]
    per_group = n // HEAD_GROUPS
    wide = per_group * heads
    fetch = pltpu.make_async_copy(slots, table, slot_sem.at[0])
    key_load = pltpu.make_async_copy(keys, kbuf, slot_sem.at[1])
    weight_load = pltpu.make_async_copy(weight, wbuf, slot_sem.at[2])
    fetch.start()
    entered = line.greet()
    key_load.start()
    weight_load.start()
    fetch.wait()
    even = line.y == 0
    head = lax.broadcasted_iota(jnp.int32, (wide, LANES), 0)
    spot = lax.broadcasted_iota(jnp.int32, (wide, LANES), 1)
    ring = line.far + [0]

    def told(k, b):
        return push(
            lax.rem(me + k, n), lse.at[b], lses.at[me, b], lsend.at[k, b], lrecv.at[k, b]
        )

    def across(k, b):
        z = line.to(k)
        return push(
            line.partner, sent.at[z, b], from_pair.at[z, b], ysend.at[k, b], yrecv.at[k, b]
        )

    def along(k, b):
        z = line.to(k)
        return push(
            line.device(z), joint.at[z, b], from_line.at[line.z, b],
            zsend.at[k, b], zrecv.at[k, b],
        )

    @pl.loop(0, rows)
    def _(b):
        loaded = []
        for g in range(HEAD_GROUPS):
            keys, bias = tiles_of(table, cache, b, g, 0, FIRST)
            loaded.append((scores_of(query_of(gq, b, g, width), keys, bias), keys))
        lses_now = jnp.zeros((1, LANES), jnp.float32)
        for g, (s, keys) in enumerate(loaded):
            rg = b * HEAD_GROUPS + g
            top, total, acc = absorb(None, s, keys)
            top = jnp.broadcast_to(top, (wide, LANES))
            best = jnp.maximum(top, norms[rg, 0])
            grown, added = jnp.exp2(top - best), jnp.exp2(norms[rg, 0] - best)
            total = grown * total + added * norms[rg, 1]
            scaled = 1.0 / total
            grown, added = grown * scaled, added * scaled
            acc = jnp.concatenate(
                [
                    acc[:, j : j + LANES] * grown + accs[rg, :, j : j + LANES] * added
                    for j in range(0, latent, LANES)
                ],
                axis=1,
            ).reshape(per_group // 2, 2, heads, latent)
            part = best + jnp.log2(total)
            part = jnp.where(spot == head + g * wide, part, 0.0)
            lses_now += jnp.sum(part, axis=0, keepdims=True)
            here_z = pl.ds(g * per_group // 2, per_group // 2)
            own[here_z, b] = jnp.where(even, acc[:, 0], acc[:, 1])
            sent[here_z, b] = jnp.where(even, acc[:, 1], acc[:, 0]).astype(jnp.bfloat16)
        lse[b] = lses_now
        lses[me, b] = lses_now

        @pl.when(b == 0)
        def _():
            entered()

        for k in ring:
            across(k, b).start()
        for k in range(1, n):
            told(k, b).start()

    def combine(b):
        for k in range(1, n):
            told(k, b).wait_recv()
        parts = [lses[s, b] for s in range(n)]
        best = functools.reduce(jnp.maximum, parts)
        whole = functools.reduce(jnp.add, [jnp.exp2(part - best) for part in parts])
        best = best + jnp.log2(whole)
        both = [jnp.exp2(lses[me, b] - best), jnp.exp2(lses[line.partner, b] - best)]
        share[...] = jnp.transpose(jnp.concatenate(both * 4, axis=0))
        for k in ring:
            z = line.to(k)
            target = line.device(z)
            part = share[pl.ds(pl.multiple_of(target * heads, heads), heads)]
            across(k, b).wait_recv()
            value = part[:, 0:1] * own[z, b]
            value += part[:, 1:2] * from_pair[z, b].astype(jnp.float32)
            if k:
                joint[z, b] = value.astype(jnp.bfloat16)
            else:
                own[z, b] = value
        for k in line.far:
            along(k, b).start()

    def index(b):
        def store(window, value):
            scores[b : b + 1, window] = value

        index_row(n, b, gq, giw, kbuf, table[b, 0, LANES - 3], store)

    key_load.wait()
    index(0)
    for b in range(rows // 2):
        combine(b)
    for b in range(1, rows // 2):
        index(b)
    for b in range(rows // 2, rows):
        combine(b)
    for b in range(rows // 2, rows):
        index(b)

    @pl.loop(0, rows)
    def _(b):
        value = own[line.z, b]
        for k in line.far:
            along(k, b).wait_recv()
            value += from_line[line.frm(k), b].astype(jnp.float32)
        attended[b] = value.astype(attended.dtype)

    @pl.loop(0, rows)
    def _(b):
        for k in range(1, n):
            told(k, b).wait_send()
        for k in ring:
            across(k, b).wait_send()
        for k in line.far:
            along(k, b).wait_send()
    weight_load.wait()


def project_kernel(attended, weight, scores, out, scores_out, sem):
    copy = pltpu.make_async_copy(scores, scores_out, sem.at[0])
    copy.start()
    rows, heads, latent = attended.shape
    flat = attended[...]
    if heads % 16:
        flat = flat.astype(jnp.float32)
    flat = flat.reshape(rows * heads, latent).astype(jnp.bfloat16)
    which = lax.broadcasted_iota(jnp.int32, (rows * heads, 1), 0) % heads

    def project(h, y):
        part = jnp.dot(flat, weight[h], preferred_element_type=jnp.float32)
        return jnp.where(which == h, part, y)

    y = jnp.zeros((rows * heads, weight.shape[2]), jnp.float32)
    y = lax.fori_loop(0, heads, project, y, unroll=8)
    out[...] = y.reshape(rows, heads, weight.shape[2]).astype(out.dtype)
    copy.wait()


def on_device(
    n,
    latent_cache,
    index_keys,
    latent_query,
    index_query,
    index_weight,
    value_up_weight,
    selected,
    lengths,
):
    cache, keys, lq = latent_cache[0], index_keys[0], latent_query[0]
    iq, iw, weight, sel = index_query[0], index_weight[0], value_up_weight[0], selected[0]
    rows, span, width = cache.shape
    heads = lq.shape[1]
    half = n // 2
    extra = -iq.shape[1] % 8
    if extra:
        iq = jnp.pad(iq, ((0, 0), (0, extra), (0, 0)))
    vmem = pl.BlockSpec(memory_space=pltpu.VMEM)
    smem = pl.BlockSpec(memory_space=pltpu.SMEM)
    hbm = pl.BlockSpec(memory_space=pl.ANY)
    dma = pltpu.SemaphoreType.DMA

    def far(x):
        return pltpu.with_memory_space_constraint(x, pltpu.HBM)

    def near(x):
        return pltpu.with_memory_space_constraint(x, pltpu.VMEM)

    params = functools.partial(pltpu.CompilerParams, vmem_limit_bytes=16 * MIB)
    gq, giw, cbuf, table = pl.pallas_call(
        functools.partial(gather_kernel, n),
        out_shape=(
            pltpu.VMEM((n, rows, heads, PACKED), lq.dtype),
            pltpu.VMEM((n,) + iw.shape, iw.dtype),
            pltpu.VMEM((rows, span // STRIP, width, STRIP), cache.dtype),
            pltpu.VMEM((rows, HEAD_GROUPS, LANES), jnp.int32),
        ),
        in_specs=[hbm] * 6,
        out_specs=(vmem,) * 4,
        scratch_shapes=[
            pltpu.VMEM(lq.shape, lq.dtype),
            pltpu.VMEM(iq.shape, iq.dtype),
            pltpu.VMEM(sel.shape, sel.dtype),
            pltpu.SMEM(lengths.shape, lengths.dtype),
            dma((5 + rows * (span // STRIP),)),
            dma((half, rows + 1)), dma((half, rows + 1)),
            dma((half, rows + 1)), dma((half, rows + 1)),
        ],
        compiler_params=params(collective_id=0, has_side_effects=True),
        name="gather",
    )(
        far(lq), far(iq), far(iw), far(sel), far(lengths),
        far(jnp.swapaxes(cache, 1, 2)),
    )

    pairs = rows * HEAD_GROUPS
    wide = n // HEAD_GROUPS * heads
    accs, norms = pl.pallas_call(
        surplus_kernel,
        out_shape=(
            pltpu.VMEM((pairs, wide, LATENT_WIDTH), jnp.float32),
            pltpu.VMEM((pairs, 2, wide, LANES), jnp.float32),
        ),
        in_specs=[smem, vmem, vmem],
        out_specs=(vmem,) * 2,
        compiler_params=params(),
        name="surplus",
    )(table, near(gq), near(cbuf))

    parts = (half, rows, heads, LATENT_WIDTH)
    attended, scores, wbuf = pl.pallas_call(
        functools.partial(attend_kernel, n),
        out_shape=(
            pltpu.VMEM((rows, heads, LATENT_WIDTH), jnp.bfloat16),
            pltpu.VMEM((rows, span), jnp.float32),
            pltpu.VMEM(weight.shape, weight.dtype),
        ),
        in_specs=[vmem] * 6 + [hbm] * 2,
        out_specs=(vmem,) * 3,
        scratch_shapes=[
            pltpu.VMEM(keys.shape, keys.dtype),
            pltpu.SMEM(table.shape, table.dtype),
            pltpu.VMEM(parts, jnp.float32),
            pltpu.VMEM(parts, jnp.bfloat16),
            pltpu.VMEM(parts, jnp.bfloat16),
            pltpu.VMEM(parts, jnp.bfloat16),
            pltpu.VMEM(parts, jnp.bfloat16),
            pltpu.VMEM((rows, 1, n * heads), jnp.float32),
            pltpu.VMEM((n, rows, 1, n * heads), jnp.float32),
            pltpu.VMEM((n * heads, 8), jnp.float32),
            dma((3,)),
            dma((half, rows)), dma((half, rows)), dma((half, rows)), dma((half, rows)),
            dma((n, rows)), dma((n, rows)),
        ],
        compiler_params=params(collective_id=1, has_side_effects=True),
        name="attend",
    )(
        near(table), near(gq), near(giw), near(cbuf), near(accs), near(norms),
        far(keys), far(weight),
    )

    head_out, index_scores = pl.pallas_call(
        project_kernel,
        out_shape=(
            jax.ShapeDtypeStruct((rows, heads, weight.shape[2]), jnp.bfloat16),
            jax.ShapeDtypeStruct((rows, span), jnp.float32),
        ),
        in_specs=[vmem, vmem, vmem],
        out_specs=(vmem, hbm),
        scratch_shapes=[dma((1,))],
        compiler_params=pltpu.CompilerParams(vmem_limit_bytes=16 * MIB),
        name="project",
    )(near(attended), near(wbuf), near(scores))
    return (index_scores[None], head_out[None])


def solution(mesh):
    return jax.shard_map(
        functools.partial(on_device, mesh.shape["seq"]),
        mesh=mesh,
        in_specs=(
            P("section", "groups", "seq", None),
            P("section", "groups", "seq", None),
            P("section", "groups", "seq", None),
            P("section", "groups", "seq", None),
            P("section", "groups", "seq"),
            P("section", "seq", None, None),
            P("section", "groups", None, None),
            P("groups"),
        ),
        out_specs=(P("section", "groups", "seq"), P("section", "groups", "seq", None)),
        check_vma=False,
    )
```

```python
import functools

import jax
import jax.numpy as jnp
from jax import lax
from jax.experimental import pallas as pl
from jax.experimental.pallas import tpu as pltpu
from jax.sharding import PartitionSpec as P

LATENT_WIDTH = 512
ROTARY_WIDTH = 64
VALUE_WIDTH = 128
IDX_DIM = 128
BLOCK = 64
HEAD_GROUPS = 2
NEG = -1e30
LOG2E = 1.4426950408889634
FIRST = 6
MORE = 2
STRIP = 128
SLOTS = 62
LANES = 128
PACKED = LATENT_WIDTH + LANES
MIB = 1024 * 1024
MESH = pl.DeviceIdType.MESH


class Line:
    def __init__(self, n):
        self.half = n // 2
        self.me = lax.axis_index("seq")
        self.z = lax.div(self.me, 2)
        self.y = lax.rem(self.me, 2)
        self.partner = self.me + 1 - 2 * self.y
        self.order = list(range(1, self.half))
        self.far = sorted(self.order, key=lambda k: (-k.bit_length(), k))

    def step(self, k, sign):
        if self.half & (self.half - 1):
            return lax.rem(self.z + sign * k + self.half, self.half)
        out = self.z
        for j in range(k.bit_length()):
            if k >> j & 1:
                bit = lax.rem(lax.div(self.z, 1 << j), 2)
                out = out + (1 - 2 * bit) * (1 << j)
        return out

    def to(self, k):
        return self.step(k, 1)

    def frm(self, k):
        return self.step(k, -1)

    def device(self, z):
        return 2 * z + self.y

    def opposite(self, z):
        return 2 * z + 1 - self.y

    def greet(self):
        barrier = pltpu.get_barrier_semaphore()
        n = 2 * self.half
        for k in range(1, n):
            peer = lax.rem(self.me + k, n)
            pl.semaphore_signal(
                barrier, inc=1, device_id={"seq": peer}, device_id_type=MESH
            )
        return lambda: pl.semaphore_wait(barrier, n - 1)


def push(peer, src, dst, send_sem, recv_sem):
    return pltpu.make_async_remote_copy(
        src_ref=src,
        dst_ref=dst,
        send_sem=send_sem,
        recv_sem=recv_sem,
        device_id={"seq": peer},
        device_id_type=MESH,
    )


def index_row(n, b, gq, giw, kbuf, length, store):
    me = lax.axis_index("seq")
    heads, held, span = gq.shape[2], giw.shape[2], kbuf.shape[1]
    tile = min(512, span)
    group = 8
    lane = lax.broadcasted_iota(jnp.int32, (1, tile), 1)
    diagonal = (
        lax.broadcasted_iota(jnp.int32, (n * group, held), 0) % group
        == lax.broadcasted_iota(jnp.int32, (n * group, held), 1)
    )
    low = lax.broadcasted_iota(jnp.int32, (n * group, LANES), 1) < LANES // 2
    packed = gq[:, b, :, LATENT_WIDTH:PACKED].astype(jnp.float32)
    if heads == 2 * group:
        left = packed[:, :group].reshape(n * group, LANES)
        right = packed[:, group:].reshape(n * group, LANES)
    else:
        left = packed.reshape(n * group, LANES)
        right = pltpu.roll(left, n * group - held, 0)
    query = jnp.where(low, pltpu.roll(left, LANES // 2, 1), right)
    query = query.astype(jnp.bfloat16)
    weight = giw[:, b : b + 1].astype(jnp.float32)
    weight = jnp.broadcast_to(weight, (n, group, held)).reshape(n * group, held)
    weight = jnp.sum(jnp.where(diagonal, weight, 0.0), axis=1, keepdims=True)
    weight = jnp.broadcast_to(weight * IDX_DIM ** (-0.5), (n * group, LANES))

    def step(c, carry):
        start = pl.multiple_of(c * tile, tile)
        dots = lax.dot_general(
            query,
            kbuf[b, pl.ds(start, tile), :],
            (((1,), (1,)), ((), ())),
            preferred_element_type=jnp.float32,
        )
        pieces = []
        for j in range(tile // LANES):
            part = jnp.maximum(dots[:, j * LANES : (j + 1) * LANES], 0.0) * weight
            pieces.append(jnp.sum(part, axis=0, keepdims=True))
        total = jnp.concatenate(pieces, axis=1)
        live = me * span + c * tile + lane < length
        store(pl.ds(start, tile), jnp.where(live, total, 0.0))
        return carry

    lax.fori_loop(0, span // tile, step, 0)


def gather_kernel(
    n, lq, iq, iw, sel, lens, cache, gq, giw, cbuf, table,
    lqs, iqs, sels, ends, load_sem, zsend, zrecv, ysend, yrecv,
):
    line = Line(n)
    me = line.me
    rows, heads, width = lqs.shape
    held = iw.shape[1]
    loads = [
        pltpu.make_async_copy(lq, lqs, load_sem.at[0]),
        pltpu.make_async_copy(iq, iqs, load_sem.at[1]),
        pltpu.make_async_copy(iw, giw.at[me], load_sem.at[2]),
        pltpu.make_async_copy(sel, sels, load_sem.at[3]),
        pltpu.make_async_copy(lens, ends, load_sem.at[4]),
    ]
    strips = cbuf.shape[1]
    for b in range(rows):
        for j in range(strips):
            loads.append(
                pltpu.make_async_copy(
                    cache.at[b, :, pl.ds(j * STRIP, STRIP)],
                    cbuf.at[b, j],
                    load_sem.at[5 + b * strips + j],
                )
            )
    for copy in loads[:5]:
        copy.start()
    entered = line.greet()
    for copy in loads[:3]:
        copy.wait()

    lane = lax.broadcasted_iota(jnp.int32, (iqs.shape[1], LANES), 1)
    row = lax.broadcasted_iota(jnp.int32, (iqs.shape[1], LANES), 0)
    for b in range(rows):
        mine = iqs[b].astype(jnp.float32)
        turned = pltpu.roll(mine, LANES // 2, 1)
        if heads == 2 * iqs.shape[1]:
            spare = jnp.concatenate([turned, mine], axis=0)
        else:
            spare = jnp.where(row < held, turned, pltpu.roll(mine, held, 0))
        gq[me, b, :, 0:LATENT_WIDTH] = lqs[b, :, 0:LATENT_WIDTH]
        gq[me, b, :, LATENT_WIDTH:width] = lqs[b, :, LATENT_WIDTH:width]
        spare = spare.astype(jnp.bfloat16)
        gq[me, b, :, width:PACKED] = spare[:, width - LATENT_WIDTH :]
    entered()

    def piece(owner, r):
        return gq.at[owner, r] if r < rows else giw.at[owner]

    relayed = (0, 1) if line.half == 4 else ()
    turns = [0, rows] + list(range(1, rows))
    across, along, onward, relay = {}, {}, {}, {}
    for r in turns:
        ref = piece(me, r)
        across[r] = push(line.partner, ref, ref, ysend.at[0, r], yrecv.at[0, r])
        for k in line.order:
            ref = piece(me, r)
            if r in relayed and k == 3:
                ref = piece(line.device(line.frm(2)), r)
                target = line.device(line.to(1))
            else:
                target = line.device(line.to(k))
            along[k, r] = push(target, ref, ref, zsend.at[k, r], zrecv.at[k, r])
            ref = piece(line.device(line.frm(k)), r)
            onward[k, r] = push(line.partner, ref, ref, ysend.at[k, r], yrecv.at[k, r])
    for r in turns:
        across[r].start()
    for r in turns:
        for k in line.order:
            if not (r in relayed and k == 3):
                along[k, r].start()
    for copy in loads[5:]:
        copy.start()

    for copy in loads[3:5]:
        copy.wait()
    here = strips * STRIP // BLOCK
    first = me * here
    chosen = sels[...]
    shape = table.shape[1:]
    spots = lax.broadcasted_iota(jnp.int32, shape, 2)
    which = lax.broadcasted_iota(jnp.int32, shape, 0)
    kept = jnp.zeros(shape, jnp.int32)
    counts = [jnp.zeros(shape, jnp.int32)] * 2
    for i in range(sels.shape[2]):
        block = jnp.broadcast_to(chosen[:, :, i : i + 1], shape)
        mine = (block >= first) & (block < first + here)
        odd = block & 1
        for part in range(2):
            take = mine & (odd == part)
            kept = jnp.where(take & (spots == part * SLOTS + counts[part]), block, kept)
            counts[part] = counts[part] + jnp.where(take, 1, 0)
    ends_now = jnp.zeros(spots.shape, jnp.int32)
    for b in range(rows):
        ends_now = jnp.where(which == b, ends[b], ends_now)
    late = spots >= SLOTS
    held = spots - jnp.where(late, SLOTS, 0) < jnp.where(late, counts[1], counts[0])
    live = jnp.minimum(BLOCK, ends_now - kept * BLOCK) + jnp.where(late, BLOCK, 0)
    table[1] = jnp.where(held, live, 0)
    tiles = jnp.where(held, (kept - first) >> 1, 0)
    tiles = jnp.where(spots == LANES - 3, ends_now, tiles)
    tiles = jnp.where(spots == LANES - 2, counts[0], tiles)
    table[0] = jnp.where(spots == LANES - 1, counts[1], tiles)

    for r in turns:
        for k in line.order:
            if not (r in relayed and k == 3):
                along[k, r].wait_recv()
                onward[k, r].start()
                if r in relayed and k == 2:
                    along[3, r].start()
    for r in relayed:
        along[3, r].wait_recv()
        onward[3, r].start()

    def complete(r):
        across[r].wait_recv()
        for k in line.order:
            onward[k, r].wait_recv()

    for r in turns:
        complete(r)
    for copy in loads[5:]:
        copy.wait()
    for group in (across, along, onward):
        for copy in group.values():
            copy.wait_send()


def tiles_of(table, cache, b, g, base, tiles):
    lane = lax.broadcasted_iota(jnp.int32, (1, LANES), 1)
    keys, bias = [], []
    for j in range(tiles):
        even, odd = base + j, SLOTS + base + j
        low, high = cache[b, table[0, b, g, even]], cache[b, table[0, b, g, odd]]
        usable = (lane < table[1, b, g, even]) | (
            (lane >= BLOCK) & (lane < table[1, b, g, odd])
        )
        keys.append(jnp.concatenate([low[:, :BLOCK], high[:, BLOCK:]], axis=1))
        bias.append(jnp.where(usable, 0.0, NEG))
    return jnp.concatenate(keys, axis=1), jnp.concatenate(bias, axis=1)


def query_of(gq, b, g, width):
    n, _, heads, _ = gq.shape
    per_group = n // HEAD_GROUPS
    query = gq[pl.ds(g * per_group, per_group), b]
    if heads % 16:
        query = query.astype(jnp.float32)
    return query.reshape(per_group * heads, PACKED)[:, :width].astype(jnp.bfloat16)


def scores_of(query, keys, bias):
    scale = (VALUE_WIDTH + ROTARY_WIDTH) ** (-0.5) * LOG2E
    return jnp.dot(query, keys, preferred_element_type=jnp.float32) * scale + bias


def absorb(state, s, keys):
    new = jnp.max(s, axis=1, keepdims=True)
    if state is not None:
        new = jnp.maximum(state[0], new)
    p = jnp.exp2(s - new)
    mixed = lax.dot_general(
        p.astype(jnp.bfloat16),
        keys[:LATENT_WIDTH],
        (((1,), (1,)), ((), ())),
        preferred_element_type=jnp.float32,
    )
    whole = jnp.sum(p, axis=1, keepdims=True)
    if state is None:
        return new, whole, mixed
    top, total, acc = state
    keep = jnp.exp2(top - new)
    return new, total * keep + whole, acc * keep + mixed


def surplus_kernel(table, gq, cache, accs, norms):
    rows, _, width, _ = cache.shape
    wide = accs.shape[1]

    @pl.loop(0, rows)
    def _(b):
        for g in range(HEAD_GROUPS):
            tiles = jnp.maximum(table[0, b, g, LANES - 2], table[0, b, g, LANES - 1])
            steps = (jnp.maximum(tiles - FIRST, 0) + MORE - 1) // MORE

            def more(c, state, g=g):
                keys, bias = tiles_of(table, cache, b, g, FIRST + c * MORE, MORE)
                return absorb(state, scores_of(query_of(gq, b, g, width), keys, bias), keys)

            start = (
                jnp.full((wide, 1), NEG, jnp.float32),
                jnp.zeros((wide, 1), jnp.float32),
                jnp.zeros((wide, LATENT_WIDTH), jnp.float32),
            )
            top, total, acc = lax.fori_loop(0, steps, more, start)
            accs[b * HEAD_GROUPS + g] = acc
            norms[b * HEAD_GROUPS + g, 0] = jnp.broadcast_to(top, (wide, LANES))
            norms[b * HEAD_GROUPS + g, 1] = jnp.broadcast_to(total, (wide, LANES))


def attend_kernel(
    n, slots, gq, giw, cache, accs, norms, keys, weight, attended, scores, wbuf,
    kbuf, table, own, sent, from_pair, joint, from_line, lse, lses, share,
    slot_sem, ysend, yrecv, zsend, zrecv, lsend, lrecv,
):
    line = Line(n)
    half, me = line.half, line.me
    _, rows, heads, latent = own.shape
    width = cache.shape[2]
    per_group = n // HEAD_GROUPS
    wide = per_group * heads
    fetch = pltpu.make_async_copy(slots, table, slot_sem.at[0])
    key_load = pltpu.make_async_copy(keys, kbuf, slot_sem.at[1])
    weight_load = pltpu.make_async_copy(weight, wbuf, slot_sem.at[2])
    fetch.start()
    entered = line.greet()
    key_load.start()
    weight_load.start()
    fetch.wait()
    even = line.y == 0
    head = lax.broadcasted_iota(jnp.int32, (wide, LANES), 0)
    spot = lax.broadcasted_iota(jnp.int32, (wide, LANES), 1)
    ring = line.far + [0]

    def told(k, b):
        return push(
            lax.rem(me + k, n), lse.at[b], lses.at[me, b], lsend.at[k, b], lrecv.at[k, b]
        )

    def across(k, b):
        z = line.to(k)
        return push(
            line.partner, sent.at[z, b], from_pair.at[z, b], ysend.at[k, b], yrecv.at[k, b]
        )

    def along(k, b):
        z = line.to(k)
        return push(
            line.device(z), joint.at[z, b], from_line.at[line.z, b],
            zsend.at[k, b], zrecv.at[k, b],
        )

    @pl.loop(0, rows)
    def _(b):
        loaded = []
        for g in range(HEAD_GROUPS):
            keys, bias = tiles_of(table, cache, b, g, 0, FIRST)
            loaded.append((scores_of(query_of(gq, b, g, width), keys, bias), keys))
        lses_now = jnp.zeros((1, LANES), jnp.float32)
        for g, (s, keys) in enumerate(loaded):
            rg = b * HEAD_GROUPS + g
            top, total, acc = absorb(None, s, keys)
            top = jnp.broadcast_to(top, (wide, LANES))
            best = jnp.maximum(top, norms[rg, 0])
            grown, added = jnp.exp2(top - best), jnp.exp2(norms[rg, 0] - best)
            total = grown * total + added * norms[rg, 1]
            scaled = 1.0 / total
            grown, added = grown * scaled, added * scaled
            acc = jnp.concatenate(
                [
                    acc[:, j : j + LANES] * grown + accs[rg, :, j : j + LANES] * added
                    for j in range(0, latent, LANES)
                ],
                axis=1,
            ).reshape(per_group // 2, 2, heads, latent)
            part = best + jnp.log2(total)
            part = jnp.where(spot == head + g * wide, part, 0.0)
            lses_now += jnp.sum(part, axis=0, keepdims=True)
            here_z = pl.ds(g * per_group // 2, per_group // 2)
            own[here_z, b] = jnp.where(even, acc[:, 0], acc[:, 1])
            sent[here_z, b] = jnp.where(even, acc[:, 1], acc[:, 0]).astype(jnp.bfloat16)
        lse[b] = lses_now
        lses[me, b] = lses_now

        @pl.when(b == 0)
        def _():
            entered()

        for k in ring:
            across(k, b).start()
        for k in range(1, n):
            told(k, b).start()

    def combine(b):
        for k in range(1, n):
            told(k, b).wait_recv()
        parts = [lses[s, b] for s in range(n)]
        best = functools.reduce(jnp.maximum, parts)
        whole = functools.reduce(jnp.add, [jnp.exp2(part - best) for part in parts])
        best = best + jnp.log2(whole)
        both = [jnp.exp2(lses[me, b] - best), jnp.exp2(lses[line.partner, b] - best)]
        share[...] = jnp.transpose(jnp.concatenate(both * 4, axis=0))
        ready = []
        for k in ring:
            z = line.to(k)
            target = line.device(z)
            part = share[pl.ds(pl.multiple_of(target * heads, heads), heads)]
            across(k, b).wait_recv()
            for copy in ready:
                copy.start()
            value = part[:, 0:1] * own[z, b]
            value += part[:, 1:2] * from_pair[z, b].astype(jnp.float32)
            ready = []
            if k:
                joint[z, b] = value.astype(jnp.bfloat16)
                ready = [along(k, b)]
            else:
                own[z, b] = value
        for copy in ready:
            copy.start()

    def index(b):
        def store(window, value):
            scores[b : b + 1, window] = value

        index_row(n, b, gq, giw, kbuf, table[0, b, 0, LANES - 3], store)

    key_load.wait()
    index(0)
    for b in range(rows // 2):
        combine(b)
    for b in range(1, rows // 2):
        index(b)
    for b in range(rows // 2, rows):
        combine(b)
    for b in range(rows // 2, rows):
        index(b)

    @pl.loop(0, rows)
    def _(b):
        value = own[line.z, b]
        for k in line.far:
            along(k, b).wait_recv()
            value += from_line[line.frm(k), b].astype(jnp.float32)
        attended[b] = value.astype(attended.dtype)

    @pl.loop(0, rows)
    def _(b):
        for k in range(1, n):
            told(k, b).wait_send()
        for k in ring:
            across(k, b).wait_send()
        for k in line.far:
            along(k, b).wait_send()
    weight_load.wait()


def project_kernel(attended, weight, scores, out, scores_out, sem):
    copy = pltpu.make_async_copy(scores, scores_out, sem.at[0])
    copy.start()
    rows, heads, latent = attended.shape
    flat = attended[...]
    if heads % 16:
        flat = flat.astype(jnp.float32)
    flat = flat.reshape(rows * heads, latent).astype(jnp.bfloat16)
    which = lax.broadcasted_iota(jnp.int32, (rows * heads, 1), 0) % heads

    def project(h, y):
        part = jnp.dot(flat, weight[h], preferred_element_type=jnp.float32)
        return jnp.where(which == h, part, y)

    y = jnp.zeros((rows * heads, weight.shape[2]), jnp.float32)
    y = lax.fori_loop(0, heads, project, y, unroll=8)
    out[...] = y.reshape(rows, heads, weight.shape[2]).astype(out.dtype)
    copy.wait()


def on_device(
    n,
    latent_cache,
    index_keys,
    latent_query,
    index_query,
    index_weight,
    value_up_weight,
    selected,
    lengths,
):
    cache, keys, lq = latent_cache[0], index_keys[0], latent_query[0]
    iq, iw, weight, sel = index_query[0], index_weight[0], value_up_weight[0], selected[0]
    rows, span, width = cache.shape
    heads = lq.shape[1]
    half = n // 2
    extra = -iq.shape[1] % 8
    if extra:
        iq = jnp.pad(iq, ((0, 0), (0, extra), (0, 0)))
    vmem = pl.BlockSpec(memory_space=pltpu.VMEM)
    smem = pl.BlockSpec(memory_space=pltpu.SMEM)
    hbm = pl.BlockSpec(memory_space=pl.ANY)
    dma = pltpu.SemaphoreType.DMA

    def far(x):
        return pltpu.with_memory_space_constraint(x, pltpu.HBM)

    def near(x):
        return pltpu.with_memory_space_constraint(x, pltpu.VMEM)

    params = functools.partial(pltpu.CompilerParams, vmem_limit_bytes=16 * MIB)
    gq, giw, cbuf, table = pl.pallas_call(
        functools.partial(gather_kernel, n),
        out_shape=(
            pltpu.VMEM((n, rows, heads, PACKED), lq.dtype),
            pltpu.VMEM((n,) + iw.shape, iw.dtype),
            pltpu.VMEM((rows, span // STRIP, width, STRIP), cache.dtype),
            pltpu.VMEM((2, rows, HEAD_GROUPS, LANES), jnp.int32),
        ),
        in_specs=[hbm] * 6,
        out_specs=(vmem,) * 4,
        scratch_shapes=[
            pltpu.VMEM(lq.shape, lq.dtype),
            pltpu.VMEM(iq.shape, iq.dtype),
            pltpu.VMEM(sel.shape, sel.dtype),
            pltpu.SMEM(lengths.shape, lengths.dtype),
            dma((5 + rows * (span // STRIP),)),
            dma((half, rows + 1)), dma((half, rows + 1)),
            dma((half, rows + 1)), dma((half, rows + 1)),
        ],
        compiler_params=params(collective_id=0, has_side_effects=True),
        name="gather",
    )(
        far(lq), far(iq), far(iw), far(sel), far(lengths),
        far(jnp.swapaxes(cache, 1, 2)),
    )

    pairs = rows * HEAD_GROUPS
    wide = n // HEAD_GROUPS * heads
    accs, norms = pl.pallas_call(
        surplus_kernel,
        out_shape=(
            pltpu.VMEM((pairs, wide, LATENT_WIDTH), jnp.float32),
            pltpu.VMEM((pairs, 2, wide, LANES), jnp.float32),
        ),
        in_specs=[smem, vmem, vmem],
        out_specs=(vmem,) * 2,
        compiler_params=params(),
        name="surplus",
    )(table, near(gq), near(cbuf))

    parts = (half, rows, heads, LATENT_WIDTH)
    attended, scores, wbuf = pl.pallas_call(
        functools.partial(attend_kernel, n),
        out_shape=(
            pltpu.VMEM((rows, heads, LATENT_WIDTH), jnp.bfloat16),
            pltpu.VMEM((rows, span), jnp.float32),
            pltpu.VMEM(weight.shape, weight.dtype),
        ),
        in_specs=[vmem] * 6 + [hbm] * 2,
        out_specs=(vmem,) * 3,
        scratch_shapes=[
            pltpu.VMEM(keys.shape, keys.dtype),
            pltpu.SMEM(table.shape, table.dtype),
            pltpu.VMEM(parts, jnp.float32),
            pltpu.VMEM(parts, jnp.bfloat16),
            pltpu.VMEM(parts, jnp.bfloat16),
            pltpu.VMEM(parts, jnp.bfloat16),
            pltpu.VMEM(parts, jnp.bfloat16),
            pltpu.VMEM((rows, 1, n * heads), jnp.float32),
            pltpu.VMEM((n, rows, 1, n * heads), jnp.float32),
            pltpu.VMEM((n * heads, 8), jnp.float32),
            dma((3,)),
            dma((half, rows)), dma((half, rows)), dma((half, rows)), dma((half, rows)),
            dma((n, rows)), dma((n, rows)),
        ],
        compiler_params=params(collective_id=1, has_side_effects=True),
        name="attend",
    )(
        near(table), near(gq), near(giw), near(cbuf), near(accs), near(norms),
        far(keys), far(weight),
    )

    head_out, index_scores = pl.pallas_call(
        project_kernel,
        out_shape=(
            jax.ShapeDtypeStruct((rows, heads, weight.shape[2]), jnp.bfloat16),
            jax.ShapeDtypeStruct((rows, span), jnp.float32),
        ),
        in_specs=[vmem, vmem, vmem],
        out_specs=(vmem, hbm),
        scratch_shapes=[dma((1,))],
        compiler_params=pltpu.CompilerParams(vmem_limit_bytes=16 * MIB),
        name="project",
    )(near(attended), near(wbuf), near(scores))
    return (index_scores[None], head_out[None])


def solution(mesh):
    return jax.shard_map(
        functools.partial(on_device, mesh.shape["seq"]),
        mesh=mesh,
        in_specs=(
            P("section", "groups", "seq", None),
            P("section", "groups", "seq", None),
            P("section", "groups", "seq", None),
            P("section", "groups", "seq", None),
            P("section", "groups", "seq"),
            P("section", "seq", None, None),
            P("section", "groups", None, None),
            P("groups"),
        ),
        out_specs=(P("section", "groups", "seq"), P("section", "groups", "seq", None)),
        check_vma=False,
    )
```

```python
import functools

import jax
import jax.numpy as jnp
from jax import lax
from jax.experimental import pallas as pl
from jax.experimental.pallas import tpu as pltpu
from jax.sharding import PartitionSpec as P

LATENT_WIDTH = 512
ROTARY_WIDTH = 64
VALUE_WIDTH = 128
IDX_DIM = 128
BLOCK = 64
HEAD_GROUPS = 2
NEG = -1e30
LOG2E = 1.4426950408889634
FIRST = 5
MORE = 2
STRIP = 128
SLOTS = 62
LANES = 128
PACKED = LATENT_WIDTH + LANES
MIB = 1024 * 1024
MESH = pl.DeviceIdType.MESH


class Line:
    def __init__(self, n):
        self.half = n // 2
        self.me = lax.axis_index("seq")
        self.z = lax.div(self.me, 2)
        self.y = lax.rem(self.me, 2)
        self.partner = self.me + 1 - 2 * self.y
        self.order = list(range(1, self.half))
        self.far = sorted(self.order, key=lambda k: (-k.bit_length(), k))

    def step(self, k, sign):
        if self.half & (self.half - 1):
            return lax.rem(self.z + sign * k + self.half, self.half)
        out = self.z
        for j in range(k.bit_length()):
            if k >> j & 1:
                bit = lax.rem(lax.div(self.z, 1 << j), 2)
                out = out + (1 - 2 * bit) * (1 << j)
        return out

    def to(self, k):
        return self.step(k, 1)

    def frm(self, k):
        return self.step(k, -1)

    def device(self, z):
        return 2 * z + self.y

    def opposite(self, z):
        return 2 * z + 1 - self.y

    def greet(self):
        barrier = pltpu.get_barrier_semaphore()
        n = 2 * self.half
        for k in range(1, n):
            peer = lax.rem(self.me + k, n)
            pl.semaphore_signal(
                barrier, inc=1, device_id={"seq": peer}, device_id_type=MESH
            )
        return lambda: pl.semaphore_wait(barrier, n - 1)


def push(peer, src, dst, send_sem, recv_sem):
    return pltpu.make_async_remote_copy(
        src_ref=src,
        dst_ref=dst,
        send_sem=send_sem,
        recv_sem=recv_sem,
        device_id={"seq": peer},
        device_id_type=MESH,
    )


def index_row(n, b, gq, giw, kbuf, length, store):
    me = lax.axis_index("seq")
    heads, held, span = gq.shape[2], giw.shape[2], kbuf.shape[1]
    tile = min(512, span)
    group = 8
    lane = lax.broadcasted_iota(jnp.int32, (1, tile), 1)
    diagonal = (
        lax.broadcasted_iota(jnp.int32, (n * group, held), 0) % group
        == lax.broadcasted_iota(jnp.int32, (n * group, held), 1)
    )
    low = lax.broadcasted_iota(jnp.int32, (n * group, LANES), 1) < LANES // 2
    packed = gq[:, b, :, LATENT_WIDTH:PACKED].astype(jnp.float32)
    if heads == 2 * group:
        left = packed[:, :group].reshape(n * group, LANES)
        right = packed[:, group:].reshape(n * group, LANES)
    else:
        left = packed.reshape(n * group, LANES)
        right = pltpu.roll(left, n * group - held, 0)
    query = jnp.where(low, pltpu.roll(left, LANES // 2, 1), right)
    query = query.astype(jnp.bfloat16)
    weight = giw[:, b : b + 1].astype(jnp.float32)
    weight = jnp.broadcast_to(weight, (n, group, held)).reshape(n * group, held)
    weight = jnp.sum(jnp.where(diagonal, weight, 0.0), axis=1, keepdims=True)
    weight = jnp.broadcast_to(weight * IDX_DIM ** (-0.5), (n * group, LANES))

    def step(c, carry):
        start = pl.multiple_of(c * tile, tile)
        dots = lax.dot_general(
            query,
            kbuf[b, pl.ds(start, tile), :],
            (((1,), (1,)), ((), ())),
            preferred_element_type=jnp.float32,
        )
        pieces = []
        for j in range(tile // LANES):
            part = jnp.maximum(dots[:, j * LANES : (j + 1) * LANES], 0.0) * weight
            pieces.append(jnp.sum(part, axis=0, keepdims=True))
        total = jnp.concatenate(pieces, axis=1)
        live = me * span + c * tile + lane < length
        store(pl.ds(start, tile), jnp.where(live, total, 0.0))
        return carry

    lax.fori_loop(0, span // tile, step, 0)


def gather_kernel(
    n, lq, iq, iw, sel, lens, cache, gq, giw, cbuf, table,
    lqs, iqs, sels, ends, load_sem, zsend, zrecv, ysend, yrecv,
):
    line = Line(n)
    me = line.me
    rows, heads, width = lqs.shape
    held = iw.shape[1]
    loads = [
        pltpu.make_async_copy(lq, lqs, load_sem.at[0]),
        pltpu.make_async_copy(iq, iqs, load_sem.at[1]),
        pltpu.make_async_copy(iw, giw.at[me], load_sem.at[2]),
        pltpu.make_async_copy(sel, sels, load_sem.at[3]),
        pltpu.make_async_copy(lens, ends, load_sem.at[4]),
    ]
    strips = cbuf.shape[1]
    for b in range(rows):
        for j in range(strips):
            loads.append(
                pltpu.make_async_copy(
                    cache.at[b, :, pl.ds(j * STRIP, STRIP)],
                    cbuf.at[b, j],
                    load_sem.at[5 + b * strips + j],
                )
            )
    for copy in loads[:5]:
        copy.start()
    entered = line.greet()
    for copy in loads[:3]:
        copy.wait()

    lane = lax.broadcasted_iota(jnp.int32, (iqs.shape[1], LANES), 1)
    row = lax.broadcasted_iota(jnp.int32, (iqs.shape[1], LANES), 0)
    for b in range(rows):
        mine = iqs[b].astype(jnp.float32)
        turned = pltpu.roll(mine, LANES // 2, 1)
        if heads == 2 * iqs.shape[1]:
            spare = jnp.concatenate([turned, mine], axis=0)
        else:
            spare = jnp.where(row < held, turned, pltpu.roll(mine, held, 0))
        gq[me, b, :, 0:LATENT_WIDTH] = lqs[b, :, 0:LATENT_WIDTH]
        gq[me, b, :, LATENT_WIDTH:width] = lqs[b, :, LATENT_WIDTH:width]
        spare = spare.astype(jnp.bfloat16)
        gq[me, b, :, width:PACKED] = spare[:, width - LATENT_WIDTH :]
    entered()

    def piece(owner, r):
        return gq.at[owner, r] if r < rows else giw.at[owner]

    relayed = (0, 1) if line.half == 4 else ()
    turns = [0, rows] + list(range(1, rows))
    across, along, onward, relay = {}, {}, {}, {}
    for r in turns:
        ref = piece(me, r)
        across[r] = push(line.partner, ref, ref, ysend.at[0, r], yrecv.at[0, r])
        for k in line.order:
            ref = piece(me, r)
            if r in relayed and k == 3:
                ref = piece(line.device(line.frm(2)), r)
                target = line.device(line.to(1))
            else:
                target = line.device(line.to(k))
            along[k, r] = push(target, ref, ref, zsend.at[k, r], zrecv.at[k, r])
            ref = piece(line.device(line.frm(k)), r)
            onward[k, r] = push(line.partner, ref, ref, ysend.at[k, r], yrecv.at[k, r])
    for r in turns:
        across[r].start()
    for r in turns:
        for k in line.order:
            if not (r in relayed and k == 3):
                along[k, r].start()
    for copy in loads[5:]:
        copy.start()

    for copy in loads[3:5]:
        copy.wait()
    here = strips * STRIP // BLOCK
    first = me * here
    chosen = sels[...]
    shape = table.shape[1:]
    spots = lax.broadcasted_iota(jnp.int32, shape, 2)
    which = lax.broadcasted_iota(jnp.int32, shape, 0)
    kept = jnp.zeros(shape, jnp.int32)
    counts = [jnp.zeros(shape, jnp.int32)] * 2
    for i in range(sels.shape[2]):
        block = jnp.broadcast_to(chosen[:, :, i : i + 1], shape)
        mine = (block >= first) & (block < first + here)
        odd = block & 1
        for part in range(2):
            take = mine & (odd == part)
            kept = jnp.where(take & (spots == part * SLOTS + counts[part]), block, kept)
            counts[part] = counts[part] + jnp.where(take, 1, 0)
    ends_now = jnp.zeros(spots.shape, jnp.int32)
    for b in range(rows):
        ends_now = jnp.where(which == b, ends[b], ends_now)
    late = spots >= SLOTS
    held = spots - jnp.where(late, SLOTS, 0) < jnp.where(late, counts[1], counts[0])
    live = jnp.minimum(BLOCK, ends_now - kept * BLOCK) + jnp.where(late, BLOCK, 0)
    table[1] = jnp.where(held, live, 0)
    tiles = jnp.where(held, (kept - first) >> 1, 0)
    tiles = jnp.where(spots == LANES - 3, ends_now, tiles)
    tiles = jnp.where(spots == LANES - 2, counts[0], tiles)
    table[0] = jnp.where(spots == LANES - 1, counts[1], tiles)

    for r in turns:
        for k in line.order:
            if not (r in relayed and k == 3):
                along[k, r].wait_recv()
                onward[k, r].start()
                if r in relayed and k == 2:
                    along[3, r].start()
    for r in relayed:
        along[3, r].wait_recv()
        onward[3, r].start()

    def complete(r):
        across[r].wait_recv()
        for k in line.order:
            onward[k, r].wait_recv()

    for copy in loads[5:]:
        copy.wait()
    for group in (across, along):
        for copy in group.values():
            copy.wait_send()
    for r in turns:
        complete(r)
    for copy in onward.values():
        copy.wait_send()


def tiles_of(table, cache, b, g, base, tiles):
    lane = lax.broadcasted_iota(jnp.int32, (1, LANES), 1)
    keys, bias = [], []
    for j in range(tiles):
        even, odd = base + j, SLOTS + base + j
        low, high = cache[b, table[0, b, g, even]], cache[b, table[0, b, g, odd]]
        usable = (lane < table[1, b, g, even]) | (
            (lane >= BLOCK) & (lane < table[1, b, g, odd])
        )
        keys.append(jnp.concatenate([low[:, :BLOCK], high[:, BLOCK:]], axis=1))
        bias.append(jnp.where(usable, 0.0, NEG))
    return jnp.concatenate(keys, axis=1), jnp.concatenate(bias, axis=1)


def query_of(gq, b, g, width):
    n, _, heads, _ = gq.shape
    per_group = n // HEAD_GROUPS
    query = gq[pl.ds(g * per_group, per_group), b]
    if heads % 16:
        query = query.astype(jnp.float32)
    return query.reshape(per_group * heads, PACKED)[:, :width].astype(jnp.bfloat16)


def scores_of(query, keys, bias):
    scale = (VALUE_WIDTH + ROTARY_WIDTH) ** (-0.5) * LOG2E
    return jnp.dot(query, keys, preferred_element_type=jnp.float32) * scale + bias


def absorb(state, s, keys):
    new = jnp.max(s, axis=1, keepdims=True)
    if state is not None:
        new = jnp.maximum(state[0], new)
    p = jnp.exp2(s - new)
    mixed = lax.dot_general(
        p.astype(jnp.bfloat16),
        keys[:LATENT_WIDTH],
        (((1,), (1,)), ((), ())),
        preferred_element_type=jnp.float32,
    )
    whole = jnp.sum(p, axis=1, keepdims=True)
    if state is None:
        return new, whole, mixed
    top, total, acc = state
    keep = jnp.exp2(top - new)
    return new, total * keep + whole, acc * keep + mixed


def surplus_kernel(table, gq, cache, accs, norms):
    rows, _, width, _ = cache.shape
    wide = accs.shape[1]

    @pl.loop(0, rows)
    def _(b):
        for g in range(HEAD_GROUPS):
            tiles = jnp.maximum(table[0, b, g, LANES - 2], table[0, b, g, LANES - 1])
            steps = (jnp.maximum(tiles - FIRST, 0) + MORE - 1) // MORE

            def more(c, state, g=g):
                keys, bias = tiles_of(table, cache, b, g, FIRST + c * MORE, MORE)
                return absorb(state, scores_of(query_of(gq, b, g, width), keys, bias), keys)

            start = (
                jnp.full((wide, 1), NEG, jnp.float32),
                jnp.zeros((wide, 1), jnp.float32),
                jnp.zeros((wide, LATENT_WIDTH), jnp.float32),
            )
            top, total, acc = lax.fori_loop(0, steps, more, start)
            accs[b * HEAD_GROUPS + g] = acc
            norms[b * HEAD_GROUPS + g, 0] = jnp.broadcast_to(top, (wide, LANES))
            norms[b * HEAD_GROUPS + g, 1] = jnp.broadcast_to(total, (wide, LANES))


def attend_kernel(
    n, slots, gq, giw, cache, accs, norms, keys, weight, attended, scores, wbuf,
    kbuf, table, own, sent, from_pair, joint, from_line, lse, lses, share,
    slot_sem, ysend, yrecv, zsend, zrecv, lsend, lrecv,
):
    line = Line(n)
    half, me = line.half, line.me
    _, rows, heads, latent = own.shape
    width = cache.shape[2]
    per_group = n // HEAD_GROUPS
    wide = per_group * heads
    fetch = pltpu.make_async_copy(slots, table, slot_sem.at[0])
    key_load = pltpu.make_async_copy(keys, kbuf, slot_sem.at[1])
    weight_load = pltpu.make_async_copy(weight, wbuf, slot_sem.at[2])
    fetch.start()
    entered = line.greet()
    key_load.start()
    weight_load.start()
    fetch.wait()
    even = line.y == 0
    head = lax.broadcasted_iota(jnp.int32, (wide, LANES), 0)
    spot = lax.broadcasted_iota(jnp.int32, (wide, LANES), 1)
    ring = line.far + [0]

    def told(k, b):
        return push(
            lax.rem(me + k, n), lse.at[b], lses.at[me, b], lsend.at[k, b], lrecv.at[k, b]
        )

    def across(k, b):
        z = line.to(k)
        return push(
            line.partner, sent.at[z, b], from_pair.at[z, b], ysend.at[k, b], yrecv.at[k, b]
        )

    def along(k, b):
        z = line.to(k)
        return push(
            line.device(z), joint.at[z, b], from_line.at[line.z, b],
            zsend.at[k, b], zrecv.at[k, b],
        )

    @pl.loop(0, rows)
    def _(b):
        loaded = []
        for g in range(HEAD_GROUPS):
            keys, bias = tiles_of(table, cache, b, g, 0, FIRST)
            loaded.append((scores_of(query_of(gq, b, g, width), keys, bias), keys))
        lses_now = jnp.zeros((1, LANES), jnp.float32)
        for g, (s, keys) in enumerate(loaded):
            rg = b * HEAD_GROUPS + g
            top, total, acc = absorb(None, s, keys)
            top = jnp.broadcast_to(top, (wide, LANES))
            best = jnp.maximum(top, norms[rg, 0])
            grown, added = jnp.exp2(top - best), jnp.exp2(norms[rg, 0] - best)
            total = grown * total + added * norms[rg, 1]
            scaled = 1.0 / total
            grown, added = grown * scaled, added * scaled
            acc = jnp.concatenate(
                [
                    acc[:, j : j + LANES] * grown + accs[rg, :, j : j + LANES] * added
                    for j in range(0, latent, LANES)
                ],
                axis=1,
            ).reshape(per_group // 2, 2, heads, latent)
            part = best + jnp.log2(total)
            part = jnp.where(spot == head + g * wide, part, 0.0)
            lses_now += jnp.sum(part, axis=0, keepdims=True)
            here_z = pl.ds(g * per_group // 2, per_group // 2)
            own[here_z, b] = jnp.where(even, acc[:, 0], acc[:, 1])
            sent[here_z, b] = jnp.where(even, acc[:, 1], acc[:, 0]).astype(jnp.bfloat16)
        lse[b] = lses_now
        lses[me, b] = lses_now

        @pl.when(b == 0)
        def _():
            entered()

        for k in ring:
            across(k, b).start()
        for k in range(1, n):
            told(k, b).start()

    def combine(b):
        for k in range(1, n):
            told(k, b).wait_recv()
        parts = [lses[s, b] for s in range(n)]
        best = functools.reduce(jnp.maximum, parts)
        whole = functools.reduce(jnp.add, [jnp.exp2(part - best) for part in parts])
        best = best + jnp.log2(whole)
        both = [jnp.exp2(lses[me, b] - best), jnp.exp2(lses[line.partner, b] - best)]
        share[...] = jnp.transpose(jnp.concatenate(both * 4, axis=0))
        ready = []
        for k in ring:
            z = line.to(k)
            target = line.device(z)
            part = share[pl.ds(pl.multiple_of(target * heads, heads), heads)]
            across(k, b).wait_recv()
            for copy in ready:
                copy.start()
            value = part[:, 0:1] * own[z, b]
            value += part[:, 1:2] * from_pair[z, b].astype(jnp.float32)
            ready = []
            if k:
                joint[z, b] = value.astype(jnp.bfloat16)
                ready = [along(k, b)]
            else:
                own[z, b] = value
        for copy in ready:
            copy.start()

    def index(b):
        def store(window, value):
            scores[b : b + 1, window] = value

        index_row(n, b, gq, giw, kbuf, table[0, b, 0, LANES - 3], store)

    key_load.wait()
    index(0)
    for b in range(rows // 2):
        combine(b)
    for b in range(1, rows // 2):
        index(b)
    for b in range(rows // 2, rows):
        combine(b)
    for b in range(rows // 2, rows):
        index(b)

    @pl.loop(0, rows)
    def _(b):
        for k in range(1, n):
            told(k, b).wait_send()
        for k in ring:
            across(k, b).wait_send()

    weight_load.wait()

    @pl.loop(0, rows)
    def _(b):
        value = own[line.z, b]
        for k in line.far:
            along(k, b).wait_recv()
            value += from_line[line.frm(k), b].astype(jnp.float32)
        attended[b] = value.astype(attended.dtype)

    @pl.loop(0, rows)
    def _(b):
        for k in line.far:
            along(k, b).wait_send()


def project_kernel(attended, weight, scores, out, scores_out, sem):
    copy = pltpu.make_async_copy(scores, scores_out, sem.at[0])
    copy.start()
    rows, heads, latent = attended.shape
    flat = attended[...]
    if heads % 16:
        flat = flat.astype(jnp.float32)
    flat = flat.reshape(rows * heads, latent).astype(jnp.bfloat16)
    which = lax.broadcasted_iota(jnp.int32, (rows * heads, 1), 0) % heads

    def project(h, y):
        part = jnp.dot(flat, weight[h], preferred_element_type=jnp.float32)
        return jnp.where(which == h, part, y)

    y = jnp.zeros((rows * heads, weight.shape[2]), jnp.float32)
    y = lax.fori_loop(0, heads, project, y, unroll=8)
    out[...] = y.reshape(rows, heads, weight.shape[2]).astype(out.dtype)
    copy.wait()


def on_device(
    n,
    latent_cache,
    index_keys,
    latent_query,
    index_query,
    index_weight,
    value_up_weight,
    selected,
    lengths,
):
    cache, keys, lq = latent_cache[0], index_keys[0], latent_query[0]
    iq, iw, weight, sel = index_query[0], index_weight[0], value_up_weight[0], selected[0]
    rows, span, width = cache.shape
    heads = lq.shape[1]
    half = n // 2
    extra = -iq.shape[1] % 8
    if extra:
        iq = jnp.pad(iq, ((0, 0), (0, extra), (0, 0)))
    vmem = pl.BlockSpec(memory_space=pltpu.VMEM)
    smem = pl.BlockSpec(memory_space=pltpu.SMEM)
    hbm = pl.BlockSpec(memory_space=pl.ANY)
    dma = pltpu.SemaphoreType.DMA

    def far(x):
        return pltpu.with_memory_space_constraint(x, pltpu.HBM)

    def near(x):
        return pltpu.with_memory_space_constraint(x, pltpu.VMEM)

    params = functools.partial(pltpu.CompilerParams, vmem_limit_bytes=16 * MIB)
    gq, giw, cbuf, table = pl.pallas_call(
        functools.partial(gather_kernel, n),
        out_shape=(
            pltpu.VMEM((n, rows, heads, PACKED), lq.dtype),
            pltpu.VMEM((n,) + iw.shape, iw.dtype),
            pltpu.VMEM((rows, span // STRIP, width, STRIP), cache.dtype),
            pltpu.VMEM((2, rows, HEAD_GROUPS, LANES), jnp.int32),
        ),
        in_specs=[hbm] * 6,
        out_specs=(vmem,) * 4,
        scratch_shapes=[
            pltpu.VMEM(lq.shape, lq.dtype),
            pltpu.VMEM(iq.shape, iq.dtype),
            pltpu.VMEM(sel.shape, sel.dtype),
            pltpu.SMEM(lengths.shape, lengths.dtype),
            dma((5 + rows * (span // STRIP),)),
            dma((half, rows + 1)), dma((half, rows + 1)),
            dma((half, rows + 1)), dma((half, rows + 1)),
        ],
        compiler_params=params(collective_id=0, has_side_effects=True),
        name="gather",
    )(
        far(lq), far(iq), far(iw), far(sel), far(lengths),
        far(jnp.swapaxes(cache, 1, 2)),
    )

    pairs = rows * HEAD_GROUPS
    wide = n // HEAD_GROUPS * heads
    accs, norms = pl.pallas_call(
        surplus_kernel,
        out_shape=(
            pltpu.VMEM((pairs, wide, LATENT_WIDTH), jnp.float32),
            pltpu.VMEM((pairs, 2, wide, LANES), jnp.float32),
        ),
        in_specs=[smem, vmem, vmem],
        out_specs=(vmem,) * 2,
        compiler_params=params(),
        name="surplus",
    )(table, near(gq), near(cbuf))

    parts = (half, rows, heads, LATENT_WIDTH)
    attended, scores, wbuf = pl.pallas_call(
        functools.partial(attend_kernel, n),
        out_shape=(
            pltpu.VMEM((rows, heads, LATENT_WIDTH), jnp.bfloat16),
            pltpu.VMEM((rows, span), jnp.float32),
            pltpu.VMEM(weight.shape, weight.dtype),
        ),
        in_specs=[vmem] * 6 + [hbm] * 2,
        out_specs=(vmem,) * 3,
        scratch_shapes=[
            pltpu.VMEM(keys.shape, keys.dtype),
            pltpu.SMEM(table.shape, table.dtype),
            pltpu.VMEM(parts, jnp.float32),
            pltpu.VMEM(parts, jnp.bfloat16),
            pltpu.VMEM(parts, jnp.bfloat16),
            pltpu.VMEM(parts, jnp.bfloat16),
            pltpu.VMEM(parts, jnp.bfloat16),
            pltpu.VMEM((rows, 1, n * heads), jnp.float32),
            pltpu.VMEM((n, rows, 1, n * heads), jnp.float32),
            pltpu.VMEM((n * heads, 8), jnp.float32),
            dma((3,)),
            dma((half, rows)), dma((half, rows)), dma((half, rows)), dma((half, rows)),
            dma((n, rows)), dma((n, rows)),
        ],
        compiler_params=params(collective_id=1, has_side_effects=True),
        name="attend",
    )(
        near(table), near(gq), near(giw), near(cbuf), near(accs), near(norms),
        far(keys), far(weight),
    )

    head_out, index_scores = pl.pallas_call(
        project_kernel,
        out_shape=(
            jax.ShapeDtypeStruct((rows, heads, weight.shape[2]), jnp.bfloat16),
            jax.ShapeDtypeStruct((rows, span), jnp.float32),
        ),
        in_specs=[vmem, vmem, vmem],
        out_specs=(vmem, hbm),
        scratch_shapes=[dma((1,))],
        compiler_params=pltpu.CompilerParams(vmem_limit_bytes=16 * MIB),
        name="project",
    )(near(attended), near(wbuf), near(scores))
    return (index_scores[None], head_out[None])


def solution(mesh):
    return jax.shard_map(
        functools.partial(on_device, mesh.shape["seq"]),
        mesh=mesh,
        in_specs=(
            P("section", "groups", "seq", None),
            P("section", "groups", "seq", None),
            P("section", "groups", "seq", None),
            P("section", "groups", "seq", None),
            P("section", "groups", "seq"),
            P("section", "seq", None, None),
            P("section", "groups", None, None),
            P("groups"),
        ),
        out_specs=(P("section", "groups", "seq"), P("section", "groups", "seq", None)),
        check_vma=False,
    )
```

```python
import functools

import jax
import jax.numpy as jnp
from jax import lax
from jax.experimental import pallas as pl
from jax.experimental.pallas import tpu as pltpu
from jax.sharding import PartitionSpec as P

LATENT_WIDTH = 512
ROTARY_WIDTH = 64
VALUE_WIDTH = 128
IDX_DIM = 128
BLOCK = 64
HEAD_GROUPS = 2
NEG = -1e30
LOG2E = 1.4426950408889634
FIRST = 5
MORE = 3
STRIP = 128
SLOTS = 62
LANES = 128
PACKED = LATENT_WIDTH + LANES
MIB = 1024 * 1024
MESH = pl.DeviceIdType.MESH


class Line:
    def __init__(self, n):
        self.half = n // 2
        self.me = lax.axis_index("seq")
        self.z = lax.div(self.me, 2)
        self.y = lax.rem(self.me, 2)
        self.partner = self.me + 1 - 2 * self.y
        self.order = list(range(1, self.half))
        self.far = sorted(self.order, key=lambda k: (-k.bit_length(), k))

    def step(self, k, sign):
        if self.half & (self.half - 1):
            return lax.rem(self.z + sign * k + self.half, self.half)
        out = self.z
        for j in range(k.bit_length()):
            if k >> j & 1:
                bit = lax.rem(lax.div(self.z, 1 << j), 2)
                out = out + (1 - 2 * bit) * (1 << j)
        return out

    def to(self, k):
        return self.step(k, 1)

    def frm(self, k):
        return self.step(k, -1)

    def device(self, z):
        return 2 * z + self.y

    def opposite(self, z):
        return 2 * z + 1 - self.y

    def greet(self):
        barrier = pltpu.get_barrier_semaphore()
        n = 2 * self.half
        for k in range(1, n):
            peer = lax.rem(self.me + k, n)
            pl.semaphore_signal(
                barrier, inc=1, device_id={"seq": peer}, device_id_type=MESH
            )
        return lambda: pl.semaphore_wait(barrier, n - 1)


def push(peer, src, dst, send_sem, recv_sem):
    return pltpu.make_async_remote_copy(
        src_ref=src,
        dst_ref=dst,
        send_sem=send_sem,
        recv_sem=recv_sem,
        device_id={"seq": peer},
        device_id_type=MESH,
    )


def index_row(n, b, gq, giw, kbuf, length, store):
    me = lax.axis_index("seq")
    heads, held, span = gq.shape[2], giw.shape[2], kbuf.shape[1]
    tile = min(512, span)
    group = 8
    lane = lax.broadcasted_iota(jnp.int32, (1, tile), 1)
    diagonal = (
        lax.broadcasted_iota(jnp.int32, (n * group, held), 0) % group
        == lax.broadcasted_iota(jnp.int32, (n * group, held), 1)
    )
    low = lax.broadcasted_iota(jnp.int32, (n * group, LANES), 1) < LANES // 2
    packed = gq[:, b, :, LATENT_WIDTH:PACKED].astype(jnp.float32)
    if heads == 2 * group:
        left = packed[:, :group].reshape(n * group, LANES)
        right = packed[:, group:].reshape(n * group, LANES)
    else:
        left = packed.reshape(n * group, LANES)
        right = pltpu.roll(left, n * group - held, 0)
    query = jnp.where(low, pltpu.roll(left, LANES // 2, 1), right)
    query = query.astype(jnp.bfloat16)
    weight = giw[:, b : b + 1].astype(jnp.float32)
    weight = jnp.broadcast_to(weight, (n, group, held)).reshape(n * group, held)
    weight = jnp.sum(jnp.where(diagonal, weight, 0.0), axis=1, keepdims=True)
    weight = jnp.broadcast_to(weight * IDX_DIM ** (-0.5), (n * group, LANES))

    def step(c, carry):
        start = pl.multiple_of(c * tile, tile)
        dots = lax.dot_general(
            query,
            kbuf[b, pl.ds(start, tile), :],
            (((1,), (1,)), ((), ())),
            preferred_element_type=jnp.float32,
        )
        pieces = []
        for j in range(tile // LANES):
            part = jnp.maximum(dots[:, j * LANES : (j + 1) * LANES], 0.0) * weight
            pieces.append(jnp.sum(part, axis=0, keepdims=True))
        total = jnp.concatenate(pieces, axis=1)
        live = me * span + c * tile + lane < length
        store(pl.ds(start, tile), jnp.where(live, total, 0.0))
        return carry

    lax.fori_loop(0, span // tile, step, 0)


def gather_kernel(
    n, lq, iq, iw, sel, lens, cache, gq, giw, cbuf, table,
    lqs, iqs, sels, ends, load_sem, zsend, zrecv, ysend, yrecv,
):
    line = Line(n)
    me = line.me
    rows, heads, width = lqs.shape
    held = iw.shape[1]
    loads = [
        pltpu.make_async_copy(lq, lqs, load_sem.at[0]),
        pltpu.make_async_copy(iq, iqs, load_sem.at[1]),
        pltpu.make_async_copy(iw, giw.at[me], load_sem.at[2]),
        pltpu.make_async_copy(sel, sels, load_sem.at[3]),
        pltpu.make_async_copy(lens, ends, load_sem.at[4]),
    ]
    strips = cbuf.shape[1]
    for b in range(rows):
        for j in range(strips):
            loads.append(
                pltpu.make_async_copy(
                    cache.at[b, :, pl.ds(j * STRIP, STRIP)],
                    cbuf.at[b, j],
                    load_sem.at[5 + b * strips + j],
                )
            )
    for copy in loads[:5]:
        copy.start()
    entered = line.greet()
    for copy in loads[:3]:
        copy.wait()

    lane = lax.broadcasted_iota(jnp.int32, (iqs.shape[1], LANES), 1)
    row = lax.broadcasted_iota(jnp.int32, (iqs.shape[1], LANES), 0)
    for b in range(rows):
        mine = iqs[b].astype(jnp.float32)
        turned = pltpu.roll(mine, LANES // 2, 1)
        if heads == 2 * iqs.shape[1]:
            spare = jnp.concatenate([turned, mine], axis=0)
        else:
            spare = jnp.where(row < held, turned, pltpu.roll(mine, held, 0))
        gq[me, b, :, 0:LATENT_WIDTH] = lqs[b, :, 0:LATENT_WIDTH]
        gq[me, b, :, LATENT_WIDTH:width] = lqs[b, :, LATENT_WIDTH:width]
        spare = spare.astype(jnp.bfloat16)
        gq[me, b, :, width:PACKED] = spare[:, width - LATENT_WIDTH :]
    entered()

    def piece(owner, r):
        return gq.at[owner, r] if r < rows else giw.at[owner]

    relayed = (0, 1) if line.half == 4 else ()
    turns = [0, rows] + list(range(1, rows))
    across, along, onward, relay = {}, {}, {}, {}
    for r in turns:
        ref = piece(me, r)
        across[r] = push(line.partner, ref, ref, ysend.at[0, r], yrecv.at[0, r])
        for k in line.order:
            ref = piece(me, r)
            if r in relayed and k == 3:
                ref = piece(line.device(line.frm(2)), r)
                target = line.device(line.to(1))
            else:
                target = line.device(line.to(k))
            along[k, r] = push(target, ref, ref, zsend.at[k, r], zrecv.at[k, r])
            ref = piece(line.device(line.frm(k)), r)
            onward[k, r] = push(line.partner, ref, ref, ysend.at[k, r], yrecv.at[k, r])
    for r in turns:
        across[r].start()
    for r in turns:
        for k in line.order:
            if not (r in relayed and k == 3):
                along[k, r].start()
    for copy in loads[5:]:
        copy.start()

    for copy in loads[3:5]:
        copy.wait()
    here = strips * STRIP // BLOCK
    first = me * here
    chosen = sels[...]
    shape = table.shape[1:]
    spots = lax.broadcasted_iota(jnp.int32, shape, 2)
    which = lax.broadcasted_iota(jnp.int32, shape, 0)
    kept = jnp.zeros(shape, jnp.int32)
    counts = [jnp.zeros(shape, jnp.int32)] * 2
    for i in range(sels.shape[2]):
        block = jnp.broadcast_to(chosen[:, :, i : i + 1], shape)
        mine = (block >= first) & (block < first + here)
        odd = block & 1
        for part in range(2):
            take = mine & (odd == part)
            kept = jnp.where(take & (spots == part * SLOTS + counts[part]), block, kept)
            counts[part] = counts[part] + jnp.where(take, 1, 0)
    ends_now = jnp.zeros(spots.shape, jnp.int32)
    for b in range(rows):
        ends_now = jnp.where(which == b, ends[b], ends_now)
    late = spots >= SLOTS
    held = spots - jnp.where(late, SLOTS, 0) < jnp.where(late, counts[1], counts[0])
    live = jnp.minimum(BLOCK, ends_now - kept * BLOCK) + jnp.where(late, BLOCK, 0)
    table[1] = jnp.where(held, live, 0)
    tiles = jnp.where(held, (kept - first) >> 1, 0)
    tiles = jnp.where(spots == LANES - 3, ends_now, tiles)
    tiles = jnp.where(spots == LANES - 2, counts[0], tiles)
    table[0] = jnp.where(spots == LANES - 1, counts[1], tiles)

    for r in turns:
        for k in line.order:
            if not (r in relayed and k == 3):
                along[k, r].wait_recv()
                onward[k, r].start()
                if r in relayed and k == 2:
                    along[3, r].start()
    for r in relayed:
        along[3, r].wait_recv()
        onward[3, r].start()

    def complete(r):
        across[r].wait_recv()
        for k in line.order:
            onward[k, r].wait_recv()

    for copy in loads[5:]:
        copy.wait()
    for group in (across, along):
        for copy in group.values():
            copy.wait_send()
    for r in turns:
        complete(r)
    for copy in onward.values():
        copy.wait_send()


def tiles_of(table, cache, b, g, base, tiles):
    lane = lax.broadcasted_iota(jnp.int32, (1, LANES), 1)
    keys, bias = [], []
    for j in range(tiles):
        even, odd = base + j, SLOTS + base + j
        low, high = cache[b, table[0, b, g, even]], cache[b, table[0, b, g, odd]]
        usable = (lane < table[1, b, g, even]) | (
            (lane >= BLOCK) & (lane < table[1, b, g, odd])
        )
        keys.append(jnp.concatenate([low[:, :BLOCK], high[:, BLOCK:]], axis=1))
        bias.append(jnp.where(usable, 0.0, NEG))
    return jnp.concatenate(keys, axis=1), jnp.concatenate(bias, axis=1)


def query_of(gq, b, g, width):
    n, _, heads, _ = gq.shape
    per_group = n // HEAD_GROUPS
    query = gq[pl.ds(g * per_group, per_group), b]
    if heads % 16:
        query = query.astype(jnp.float32)
    return query.reshape(per_group * heads, PACKED)[:, :width].astype(jnp.bfloat16)


def scores_of(query, keys, bias):
    scale = (VALUE_WIDTH + ROTARY_WIDTH) ** (-0.5) * LOG2E
    return jnp.dot(query, keys, preferred_element_type=jnp.float32) * scale + bias


def absorb(state, s, keys):
    new = jnp.max(s, axis=1, keepdims=True)
    if state is not None:
        new = jnp.maximum(state[0], new)
    p = jnp.exp2(s - new)
    mixed = lax.dot_general(
        p.astype(jnp.bfloat16),
        keys[:LATENT_WIDTH],
        (((1,), (1,)), ((), ())),
        preferred_element_type=jnp.float32,
    )
    whole = jnp.sum(p, axis=1, keepdims=True)
    if state is None:
        return new, whole, mixed
    top, total, acc = state
    keep = jnp.exp2(top - new)
    return new, total * keep + whole, acc * keep + mixed


def surplus_kernel(table, gq, cache, accs, norms):
    rows, _, width, _ = cache.shape
    wide = accs.shape[1]

    @pl.loop(0, rows)
    def _(b):
        for g in range(HEAD_GROUPS):
            tiles = jnp.maximum(table[0, b, g, LANES - 2], table[0, b, g, LANES - 1])
            steps = (jnp.maximum(tiles - FIRST, 0) + MORE - 1) // MORE

            def more(c, state, g=g):
                keys, bias = tiles_of(table, cache, b, g, FIRST + c * MORE, MORE)
                return absorb(state, scores_of(query_of(gq, b, g, width), keys, bias), keys)

            start = (
                jnp.full((wide, 1), NEG, jnp.float32),
                jnp.zeros((wide, 1), jnp.float32),
                jnp.zeros((wide, LATENT_WIDTH), jnp.float32),
            )
            top, total, acc = lax.fori_loop(0, steps, more, start)
            accs[b * HEAD_GROUPS + g] = acc
            norms[b * HEAD_GROUPS + g, 0] = jnp.broadcast_to(top, (wide, LANES))
            norms[b * HEAD_GROUPS + g, 1] = jnp.broadcast_to(total, (wide, LANES))


def attend_kernel(
    n, slots, gq, giw, cache, accs, norms, keys, weight, attended, scores, wbuf,
    kbuf, table, own, sent, from_pair, joint, from_line, lse, lses, share,
    slot_sem, ysend, yrecv, zsend, zrecv, lsend, lrecv,
):
    line = Line(n)
    half, me = line.half, line.me
    _, rows, heads, latent = own.shape
    width = cache.shape[2]
    per_group = n // HEAD_GROUPS
    wide = per_group * heads
    fetch = pltpu.make_async_copy(slots, table, slot_sem.at[0])
    key_load = pltpu.make_async_copy(keys, kbuf, slot_sem.at[1])
    weight_load = pltpu.make_async_copy(weight, wbuf, slot_sem.at[2])
    fetch.start()
    entered = line.greet()
    key_load.start()
    weight_load.start()
    fetch.wait()
    even = line.y == 0
    head = lax.broadcasted_iota(jnp.int32, (wide, LANES), 0)
    spot = lax.broadcasted_iota(jnp.int32, (wide, LANES), 1)
    ring = line.far + [0]

    def told(k, b):
        return push(
            lax.rem(me + k, n), lse.at[b], lses.at[me, b], lsend.at[k, b], lrecv.at[k, b]
        )

    def across(k, b):
        z = line.to(k)
        return push(
            line.partner, sent.at[z, b], from_pair.at[z, b], ysend.at[k, b], yrecv.at[k, b]
        )

    def along(k, b):
        z = line.to(k)
        return push(
            line.device(z), joint.at[z, b], from_line.at[line.z, b],
            zsend.at[k, b], zrecv.at[k, b],
        )

    @pl.loop(0, rows)
    def _(b):
        loaded = []
        for g in range(HEAD_GROUPS):
            keys, bias = tiles_of(table, cache, b, g, 0, FIRST)
            loaded.append((scores_of(query_of(gq, b, g, width), keys, bias), keys))
        lses_now = jnp.zeros((1, LANES), jnp.float32)
        for g, (s, keys) in enumerate(loaded):
            rg = b * HEAD_GROUPS + g
            top, total, acc = absorb(None, s, keys)
            top = jnp.broadcast_to(top, (wide, LANES))
            best = jnp.maximum(top, norms[rg, 0])
            grown, added = jnp.exp2(top - best), jnp.exp2(norms[rg, 0] - best)
            total = grown * total + added * norms[rg, 1]
            scaled = 1.0 / total
            grown, added = grown * scaled, added * scaled
            acc = jnp.concatenate(
                [
                    acc[:, j : j + LANES] * grown + accs[rg, :, j : j + LANES] * added
                    for j in range(0, latent, LANES)
                ],
                axis=1,
            ).reshape(per_group // 2, 2, heads, latent)
            part = best + jnp.log2(total)
            part = jnp.where(spot == head + g * wide, part, 0.0)
            lses_now += jnp.sum(part, axis=0, keepdims=True)
            here_z = pl.ds(g * per_group // 2, per_group // 2)
            own[here_z, b] = jnp.where(even, acc[:, 0], acc[:, 1])
            sent[here_z, b] = jnp.where(even, acc[:, 1], acc[:, 0]).astype(jnp.bfloat16)
        lse[b] = lses_now
        lses[me, b] = lses_now

        @pl.when(b == 0)
        def _():
            entered()

        for k in ring:
            across(k, b).start()
        for k in range(1, n):
            told(k, b).start()

    def combine(b):
        for k in range(1, n):
            told(k, b).wait_recv()
        parts = [lses[s, b] for s in range(n)]
        best = functools.reduce(jnp.maximum, parts)
        whole = functools.reduce(jnp.add, [jnp.exp2(part - best) for part in parts])
        best = best + jnp.log2(whole)
        both = [jnp.exp2(lses[me, b] - best), jnp.exp2(lses[line.partner, b] - best)]
        share[...] = jnp.transpose(jnp.concatenate(both * 4, axis=0))
        ready = []
        for k in ring:
            z = line.to(k)
            target = line.device(z)
            part = share[pl.ds(pl.multiple_of(target * heads, heads), heads)]
            across(k, b).wait_recv()
            for copy in ready:
                copy.start()
            value = part[:, 0:1] * own[z, b]
            value += part[:, 1:2] * from_pair[z, b].astype(jnp.float32)
            ready = []
            if k:
                joint[z, b] = value.astype(jnp.bfloat16)
                ready = [along(k, b)]
            else:
                own[z, b] = value
        for copy in ready:
            copy.start()

    def index(b):
        def store(window, value):
            scores[b : b + 1, window] = value

        index_row(n, b, gq, giw, kbuf, table[0, b, 0, LANES - 3], store)

    key_load.wait()
    index(0)
    for b in range(rows // 2):
        combine(b)
    for b in range(1, rows // 2):
        index(b)
    for b in range(rows // 2, rows):
        combine(b)
    for b in range(rows // 2, rows):
        index(b)

    @pl.loop(0, rows)
    def _(b):
        for k in range(1, n):
            told(k, b).wait_send()
        for k in ring:
            across(k, b).wait_send()

    weight_load.wait()

    @pl.loop(0, rows)
    def _(b):
        value = own[line.z, b]
        for k in line.far:
            along(k, b).wait_recv()
            value += from_line[line.frm(k), b].astype(jnp.float32)
        attended[b] = value.astype(attended.dtype)

    @pl.loop(0, rows)
    def _(b):
        for k in line.far:
            along(k, b).wait_send()


def project_kernel(attended, weight, scores, out, scores_out, sem):
    copy = pltpu.make_async_copy(scores, scores_out, sem.at[0])
    copy.start()
    rows, heads, latent = attended.shape
    flat = attended[...]
    if heads % 16:
        flat = flat.astype(jnp.float32)
    flat = flat.reshape(rows * heads, latent).astype(jnp.bfloat16)
    which = lax.broadcasted_iota(jnp.int32, (rows * heads, 1), 0) % heads

    def project(h, y):
        part = jnp.dot(flat, weight[h], preferred_element_type=jnp.float32)
        return jnp.where(which == h, part, y)

    y = jnp.zeros((rows * heads, weight.shape[2]), jnp.float32)
    y = lax.fori_loop(0, heads, project, y, unroll=8)
    out[...] = y.reshape(rows, heads, weight.shape[2]).astype(out.dtype)
    copy.wait()


def on_device(
    n,
    latent_cache,
    index_keys,
    latent_query,
    index_query,
    index_weight,
    value_up_weight,
    selected,
    lengths,
):
    cache, keys, lq = latent_cache[0], index_keys[0], latent_query[0]
    iq, iw, weight, sel = index_query[0], index_weight[0], value_up_weight[0], selected[0]
    rows, span, width = cache.shape
    heads = lq.shape[1]
    half = n // 2
    extra = -iq.shape[1] % 8
    if extra:
        iq = jnp.pad(iq, ((0, 0), (0, extra), (0, 0)))
    vmem = pl.BlockSpec(memory_space=pltpu.VMEM)
    smem = pl.BlockSpec(memory_space=pltpu.SMEM)
    hbm = pl.BlockSpec(memory_space=pl.ANY)
    dma = pltpu.SemaphoreType.DMA

    def far(x):
        return pltpu.with_memory_space_constraint(x, pltpu.HBM)

    def near(x):
        return pltpu.with_memory_space_constraint(x, pltpu.VMEM)

    params = functools.partial(pltpu.CompilerParams, vmem_limit_bytes=16 * MIB)
    gq, giw, cbuf, table = pl.pallas_call(
        functools.partial(gather_kernel, n),
        out_shape=(
            pltpu.VMEM((n, rows, heads, PACKED), lq.dtype),
            pltpu.VMEM((n,) + iw.shape, iw.dtype),
            pltpu.VMEM((rows, span // STRIP, width, STRIP), cache.dtype),
            pltpu.VMEM((2, rows, HEAD_GROUPS, LANES), jnp.int32),
        ),
        in_specs=[hbm] * 6,
        out_specs=(vmem,) * 4,
        scratch_shapes=[
            pltpu.VMEM(lq.shape, lq.dtype),
            pltpu.VMEM(iq.shape, iq.dtype),
            pltpu.VMEM(sel.shape, sel.dtype),
            pltpu.SMEM(lengths.shape, lengths.dtype),
            dma((5 + rows * (span // STRIP),)),
            dma((half, rows + 1)), dma((half, rows + 1)),
            dma((half, rows + 1)), dma((half, rows + 1)),
        ],
        compiler_params=params(collective_id=0, has_side_effects=True),
        name="gather",
    )(
        far(lq), far(iq), far(iw), far(sel), far(lengths),
        far(jnp.swapaxes(cache, 1, 2)),
    )

    pairs = rows * HEAD_GROUPS
    wide = n // HEAD_GROUPS * heads
    accs, norms = pl.pallas_call(
        surplus_kernel,
        out_shape=(
            pltpu.VMEM((pairs, wide, LATENT_WIDTH), jnp.float32),
            pltpu.VMEM((pairs, 2, wide, LANES), jnp.float32),
        ),
        in_specs=[smem, vmem, vmem],
        out_specs=(vmem,) * 2,
        compiler_params=params(),
        name="surplus",
    )(table, near(gq), near(cbuf))

    parts = (half, rows, heads, LATENT_WIDTH)
    attended, scores, wbuf = pl.pallas_call(
        functools.partial(attend_kernel, n),
        out_shape=(
            pltpu.VMEM((rows, heads, LATENT_WIDTH), jnp.bfloat16),
            pltpu.VMEM((rows, span), jnp.float32),
            pltpu.VMEM(weight.shape, weight.dtype),
        ),
        in_specs=[vmem] * 6 + [hbm] * 2,
        out_specs=(vmem,) * 3,
        scratch_shapes=[
            pltpu.VMEM(keys.shape, keys.dtype),
            pltpu.SMEM(table.shape, table.dtype),
            pltpu.VMEM(parts, jnp.float32),
            pltpu.VMEM(parts, jnp.bfloat16),
            pltpu.VMEM(parts, jnp.bfloat16),
            pltpu.VMEM(parts, jnp.bfloat16),
            pltpu.VMEM(parts, jnp.bfloat16),
            pltpu.VMEM((rows, 1, n * heads), jnp.float32),
            pltpu.VMEM((n, rows, 1, n * heads), jnp.float32),
            pltpu.VMEM((n * heads, 8), jnp.float32),
            dma((3,)),
            dma((half, rows)), dma((half, rows)), dma((half, rows)), dma((half, rows)),
            dma((n, rows)), dma((n, rows)),
        ],
        compiler_params=params(collective_id=1, has_side_effects=True),
        name="attend",
    )(
        near(table), near(gq), near(giw), near(cbuf), near(accs), near(norms),
        far(keys), far(weight),
    )

    head_out, index_scores = pl.pallas_call(
        project_kernel,
        out_shape=(
            jax.ShapeDtypeStruct((rows, heads, weight.shape[2]), jnp.bfloat16),
            jax.ShapeDtypeStruct((rows, span), jnp.float32),
        ),
        in_specs=[vmem, vmem, vmem],
        out_specs=(vmem, hbm),
        scratch_shapes=[dma((1,))],
        compiler_params=pltpu.CompilerParams(vmem_limit_bytes=16 * MIB),
        name="project",
    )(near(attended), near(wbuf), near(scores))
    return (index_scores[None], head_out[None])


def solution(mesh):
    return jax.shard_map(
        functools.partial(on_device, mesh.shape["seq"]),
        mesh=mesh,
        in_specs=(
            P("section", "groups", "seq", None),
            P("section", "groups", "seq", None),
            P("section", "groups", "seq", None),
            P("section", "groups", "seq", None),
            P("section", "groups", "seq"),
            P("section", "seq", None, None),
            P("section", "groups", None, None),
            P("groups"),
        ),
        out_specs=(P("section", "groups", "seq"), P("section", "groups", "seq", None)),
        check_vma=False,
    )
```
